256 devices in a mesh: dp: 64 (over z, y, core), tp: 4 (over x).
Axes of the slice: x: 4, y: 4, z: 8, core: 2. Of those that a mesh axis runs over, the one named last changes fastest.
Arguments:
- irreps: bfloat16 [131072, 9, 128], P('dp', None, 'tp')
- norm_gain: float32 [3, 128], P(None, 'tp')
- w_up: bfloat16 [3, 128, 512], P(None, None, 'tp')
- w_gate: bfloat16 [128, 512], P(None, 'tp')
- w_down: bfloat16 [3, 512, 128], P(None, 'tp')
- to_grid: float32 [9, 36], replicated
- from_grid: float32 [36, 8], replicated
- grad_out: bfloat16 [131072, 9, 128], P('dp', None, 'tp')
Outputs:
- output 1: bfloat16 [131072, 9, 128], P('dp', None, 'tp')
- output 2: bfloat16 [131072, 9, 128], P('dp', None, 'tp')
- output 3: bfloat16 [3, 128, 512], P(None, None, 'tp')
- output 4: bfloat16 [128, 512], P(None, 'tp')
- output 5: bfloat16 [3, 512, 128], P(None, 'tp')
All inputs are finite; a program needn't handle non-finite values.
Results may differ from the reference program's by a relative error of at most 0.0120943.
Values are sent between devices in bfloat16 or wider.
A program may use at most 768 MiB of HBM per device.

```python
import math
import jax
import jax.numpy as jnp
from jax import lax

N_NODES = 131072
CHANNELS = 128
HIDDEN = 512
DEG_MAX = 2
GRID_PTS = 36

DEGREES = DEG_MAX + 1
COEFS = DEGREES * DEGREES
ROW_BLOCK = math.gcd(N_NODES, 128)
NORM_EPS = 1e-5


def setup_inputs(seed: int = 0) -> dict:
    key_list = jax.random.split(jax.random.key(seed), 11)
    chan_pos = jnp.arange(CHANNELS, dtype=jnp.float32) / CHANNELS
    chan_scale = jnp.exp(2.4 * (chan_pos - 0.5) + 0.3 * jax.random.normal(key_list[0], (CHANNELS,)))
    node_scale = jnp.exp(0.4 * jax.random.normal(key_list[1], (N_NODES, 1, 1)))
    scalar_row = (jnp.arange(COEFS) == 0).astype(jnp.float32)[:, None]
    offsets = 0.8 * jax.random.normal(key_list[2], (CHANNELS,))
    noise_draw = jax.random.normal(key_list[3], (N_NODES, COEFS, CHANNELS))
    irreps = node_scale * chan_scale * (noise_draw + scalar_row * offsets)
    norm_gain = 0.6 + 0.8 * jax.random.uniform(key_list[4], (DEGREES, CHANNELS))
    w_up = jax.random.normal(key_list[5], (DEGREES, CHANNELS, HIDDEN)) * CHANNELS ** -0.5
    w_gate = jax.random.normal(key_list[6], (CHANNELS, HIDDEN)) * CHANNELS ** -0.5
    w_down = jax.random.normal(key_list[7], (DEGREES, HIDDEN, CHANNELS)) * HIDDEN ** -0.5
    to_grid = jax.random.normal(key_list[8], (COEFS, GRID_PTS)) * COEFS ** -0.5
    from_grid = jax.random.normal(key_list[9], (GRID_PTS, COEFS - 1)) * GRID_PTS ** -0.5
    grad_out = jax.random.normal(key_list[10], (N_NODES, COEFS, CHANNELS))
    return {'irreps': irreps.astype(jnp.bfloat16), 'norm_gain': norm_gain, 'w_up': w_up.astype(jnp.bfloat16), 'w_gate': w_gate.astype(jnp.bfloat16), 'w_down': w_down.astype(jnp.bfloat16), 'to_grid': to_grid, 'from_grid': from_grid, 'grad_out': grad_out.astype(jnp.bfloat16)}


def expand_rows(per_degree):
    return jnp.concatenate([jnp.broadcast_to(per_degree[degree:degree + 1], (2 * degree + 1,) + per_degree.shape[1:]) for degree in range(per_degree.shape[0])], axis=0)


def block_forward(x_blk, norm_gain, up_f, gate_f, down_f, grid_in, grid_back):
    x_f = x_blk.astype(jnp.float32)
    scalar = x_f[:, 0, :]
    mean_s = jnp.mean(scalar, axis=-1, keepdims=True)
    centered = scalar - mean_s
    var_s = jnp.mean(centered * centered, axis=-1, keepdims=True)
    vector = x_f[:, 1:, :]
    mean_sq = jnp.mean(vector * vector, axis=(1, 2), keepdims=True)
    normed = jnp.concatenate([(centered * lax.rsqrt(var_s + NORM_EPS))[:, None, :], vector * lax.rsqrt(mean_sq + NORM_EPS)], axis=1)
    normed = (normed * expand_rows(norm_gain)).astype(jnp.bfloat16).astype(jnp.float32)
    hidden_act = jnp.einsum('nkc,kch->nkh', normed, expand_rows(up_f)).astype(jnp.bfloat16).astype(jnp.float32)
    pre_gate = jnp.einsum('nc,ch->nh', normed[:, 0, :], gate_f).astype(jnp.bfloat16).astype(jnp.float32)
    gate_val = jax.nn.silu(pre_gate).astype(jnp.bfloat16)
    pre_grid = jnp.einsum('nkh,kg->ngh', hidden_act, grid_in).astype(jnp.bfloat16).astype(jnp.float32)
    grid_val = jax.nn.silu(pre_grid).astype(jnp.bfloat16).astype(jnp.float32)
    back_proj = jnp.einsum('ngh,gk->nkh', grid_val, grid_back).astype(jnp.bfloat16)
    mixed_act = jnp.concatenate([gate_val[:, None, :], back_proj], axis=1).astype(jnp.float32)
    ffn_delta = jnp.einsum('nkh,khc->nkc', mixed_act, expand_rows(down_f))
    return (x_f + ffn_delta).astype(jnp.bfloat16)


def reference(irreps, norm_gain, w_up, w_gate, w_down, to_grid, from_grid, grad_out):
    up_f = w_up.astype(jnp.float32)
    gate_f = w_gate.astype(jnp.float32)
    down_f = w_down.astype(jnp.float32)
    grid_in = to_grid.astype(jnp.bfloat16).astype(jnp.float32)
    grid_back = from_grid.astype(jnp.bfloat16).astype(jnp.float32)
    blk_count = N_NODES // ROW_BLOCK
    x_blocks = irreps.reshape(blk_count, ROW_BLOCK, COEFS, CHANNELS)
    g_blocks = grad_out.reshape(blk_count, ROW_BLOCK, COEFS, CHANNELS)

    def scan_step(grad_sums, blk_pair):
        def local_fn(x_in, up_in, gate_in, down_in):
            return block_forward(x_in, norm_gain, up_in, gate_in, down_in, grid_in, grid_back)
        out_blk, pull_back = jax.vjp(local_fn, blk_pair[0], up_f, gate_f, down_f)
        dx_blk, d_up, d_gate, d_down = pull_back(blk_pair[1])
        new_sums = (grad_sums[0] + d_up, grad_sums[1] + d_gate, grad_sums[2] + d_down)
        return new_sums, (out_blk, dx_blk)

    init_sums = (jnp.zeros_like(up_f), jnp.zeros_like(gate_f), jnp.zeros_like(down_f))
    total_sums, (out_blocks, dx_blocks) = lax.scan(scan_step, init_sums, (x_blocks, g_blocks))
    out_irreps = out_blocks.reshape(N_NODES, COEFS, CHANNELS)
    d_irreps = dx_blocks.reshape(N_NODES, COEFS, CHANNELS)
    return (out_irreps, d_irreps, total_sums[0].astype(jnp.bfloat16), total_sums[1].astype(jnp.bfloat16), total_sums[2].astype(jnp.bfloat16))
```

```python
import functools
import jax
import jax.numpy as jnp
from jax import lax
from jax.experimental import pallas as pl
from jax.experimental.pallas import tpu as pltpu
from jax.sharding import PartitionSpec as P

NORM_EPS = 1e-5
COEFS = 9
CH = 128
HID = 512
SUB = 16
BLK = 256
GRID_ROWS = 576
GRID_PAD = 640
SLAB = 56
ROWS = 896
DEGS = 3
TP = 4
VMEM_LIMIT = 60 * 2**20
F32 = jnp.float32
BF16 = jnp.bfloat16


def iota(shape, axis):
    return lax.broadcasted_iota(jnp.int32, shape, axis)


def mm(a, b):
    return jnp.dot(a, b, preferred_element_type=F32)


def mm_nt(a, b):
    return lax.dot_general(a, b, (((1,), (1,)), ((), ())), preferred_element_type=F32)


def one_hot(shape, row_div, col_div):
    return jnp.where(iota(shape, 0) // row_div == iota(shape, 1) // col_div, 1.0, 0.0).astype(BF16)


def spread(table, rows, row_div, cols, col_div):
    left = mm(one_hot((rows, CH), row_div, 1), table).astype(BF16)
    full = mm(left, one_hot((CH, cols), 1, col_div))
    same = iota((rows, cols), 0) % SUB == iota((rows, cols), 1) % SUB
    return jnp.where(same, full, 0.0)


def degree_of(coef):
    return jnp.where(coef >= 4, 2, jnp.where(coef >= 1, 1, 0))


def setup_tables(tog_ref, frg_ref, kg, kf, kft, kgt):
    tog = tog_ref[...].astype(BF16)
    frg = frg_ref[...].astype(BF16)
    tog_t = tog_ref[...].T.astype(BF16)
    frg_t = frg_ref[...].T.astype(BF16)
    kg[...] = (0.5 * spread(tog_t, GRID_ROWS, SUB, BLK, SUB)).astype(BF16)
    kf[...] = (0.5 * spread(frg, GRID_ROWS, SUB, CH, SUB)).astype(BF16)
    kft[...] = spread(frg_t, CH, SUB, GRID_PAD, SUB).astype(BF16)
    kgt[...] = spread(tog, 144, SUB, GRID_PAD, SUB).astype(BF16)


def compute_block(lanes, x_ref, g_ref, gain_ref, wup, wgate, wdown, out_ref, dx_ref, grad_ref,
                  wup_t, wgate_t, wdown_t, kg, kf, kft, kgt, n_s, y_s, dm_s, m_s, dy_s, da_s, dn_s, s_bufs, du_bufs):
    gain = [jnp.concatenate([gain_ref[degree]] * 2, axis=1) for degree in range(DEGS)]
    x0 = x_ref[0, :, lanes].astype(F32)
    mean_s = jnp.sum(x0, axis=0, keepdims=True) * (1.0 / CH)
    cen = x0 - mean_s
    inv_s = lax.rsqrt(jnp.sum(cen * cen, axis=0, keepdims=True) * (1.0 / CH) + NORM_EPS)
    n_s[0] = ((cen * inv_s) * gain[0]).astype(BF16)
    acc = jnp.zeros((CH, BLK), F32)
    for coef in range(1, COEFS):
        xk = x_ref[coef, :, lanes].astype(F32)
        acc = acc + xk * xk
    inv_v = lax.rsqrt(jnp.sum(acc, axis=0, keepdims=True) * (1.0 / 1024) + NORM_EPS)
    for coef in range(1, COEFS):
        xk = x_ref[coef, :, lanes].astype(F32)
        n_s[coef] = ((xk * inv_v) * gain[1 if coef < 4 else 2]).astype(BF16)

    def up_step(coef, carry):
        degree = degree_of(coef)
        y_s[coef] = mm(wup_t[degree], n_s[coef]).astype(BF16)
        dm_s[coef] = mm(wdown[degree], g_ref[coef, :, lanes]).astype(BF16)
        return carry
    lax.fori_loop(0, COEFS, up_step, 0)

    def gate_step(i, carry):
        rows = pl.ds(pl.multiple_of(i * CH, CH), CH)
        half = (0.5 * mm(wgate_t[rows, :], n_s[0])).astype(BF16).astype(F32)
        th = jnp.tanh(half)
        plus = 1.0 + th
        val = half * plus
        m_s[0, rows, :] = val.astype(BF16)
        slope = 0.5 * (plus + val * (1.0 - th))
        da_s[rows, :] = (dm_s[0, rows, :].astype(F32) * slope).astype(BF16)
        return carry
    lax.fori_loop(0, 4, gate_step, 0)

    def expand(j, s_buf, du_buf):
        rows = pl.ds(pl.multiple_of(j * SUB, SUB), SUB)
        yj = y_s[:, rows, :].reshape(144, BLK)
        dzj = dm_s[1:, rows, :].reshape(CH, BLK)
        for r0 in range(0, GRID_ROWS, CHUNK):
            half = mm(kg[r0:r0 + CHUNK, 0:144], yj).astype(BF16).astype(F32)
            dval = mm(kf[r0:r0 + CHUNK, :], dzj).astype(BF16).astype(F32)
            th = jnp.tanh(half)
            plus = 1.0 + th
            val = half * plus
            s_buf[r0:r0 + CHUNK, :] = val.astype(BF16)
            du_buf[r0:r0 + CHUNK, :] = (dval * (plus + val * (1.0 - th))).astype(BF16)

    def contract(j, s_buf, du_buf):
        rows = pl.ds(pl.multiple_of(j * SUB, SUB), SUB)
        m_s[1:, rows, :] = mm(kft[...], s_buf[...]).astype(BF16).reshape(8, SUB, BLK)
        dy_s[:, rows, :] = mm(kgt[...], du_buf[...]).astype(BF16).reshape(9, SUB, BLK)

    expand(0, s_bufs[0], du_bufs[0])

    def grid_step(i, carry):
        expand(2 * i + 1, s_bufs[1], du_bufs[1])
        contract(2 * i, s_bufs[0], du_bufs[0])
        expand(jnp.minimum(2 * i + 2, 31), s_bufs[0], du_bufs[0])
        contract(2 * i + 1, s_bufs[1], du_bufs[1])
        return carry
    lax.fori_loop(0, 16, grid_step, 0)

    def down_step(coef, carry):
        degree = degree_of(coef)
        mk = m_s[coef]
        dyk = dy_s[coef]
        gk = g_ref[coef, :, lanes]
        nk = n_s[coef]
        xk = x_ref[coef, :, lanes].astype(F32)
        out_ref[coef, :, lanes] = (xk + mm(wdown_t[degree], mk)).astype(BF16)
        dn_s[coef] = mm(wup[degree], dyk)
        base = pl.multiple_of(degree * CH, CH)
        g_up = mm_nt(nk, dyk)
        for t in range(TP):
            grad_ref[t, pl.ds(base, CH), :] += g_up[:, t * CH:(t + 1) * CH]
            grad_ref[t, pl.ds(base + HID, CH), :] += mm_nt(mk[t * CH:(t + 1) * CH, :], gk)
        return carry
    lax.fori_loop(0, COEFS, down_step, 0)
    dn_s[0] += mm(wgate[...], da_s[...])
    g_gate = mm_nt(n_s[0], da_s[...])
    for t in range(TP):
        grad_ref[t, 384:HID, :] += g_gate[:, t * CH:(t + 1) * CH]

    x0 = x_ref[0, :, lanes].astype(F32)
    hat = (x0 - mean_s) * inv_s
    dh = dn_s[0].astype(BF16).astype(F32) * gain[0]
    m1 = jnp.sum(dh, axis=0, keepdims=True) * (1.0 / CH)
    m2 = jnp.sum(dh * hat, axis=0, keepdims=True) * (1.0 / CH)
    dx_ref[0, :, lanes] = (inv_s * (dh - m1 - hat * m2) + g_ref[0, :, lanes].astype(F32)).astype(BF16)
    acc = jnp.zeros((CH, BLK), F32)
    for coef in range(1, COEFS):
        xk = x_ref[coef, :, lanes].astype(F32)
        acc = acc + (dn_s[coef].astype(BF16).astype(F32) * gain[1 if coef < 4 else 2]) * (xk * inv_v)
    mv = jnp.sum(acc, axis=0, keepdims=True) * (1.0 / 1024)
    for coef in range(1, COEFS):
        xk = x_ref[coef, :, lanes].astype(F32)
        dh = dn_s[coef].astype(BF16).astype(F32) * gain[1 if coef < 4 else 2]
        dx_ref[coef, :, lanes] = (inv_v * (dh - (xk * inv_v) * mv) + g_ref[coef, :, lanes].astype(F32)).astype(BF16)


CHUNK = 144


def compute_kernel(x_ref, g_ref, gain_ref, wup, wgate, wdown, tog_ref, frg_ref, out_ref, dx_ref, grad_ref,
                   wup_t, wgate_t, wdown_t, kg, kf, kft, kgt, n_s, y_s, dm_s, m_s, dy_s, da_s, dn_s, sb0, sb1, db0, db1):
    setup_tables(tog_ref, frg_ref, kg, kf, kft, kgt)
    for degree in range(DEGS):
        wup_t[degree] = wup[degree].T
        wdown_t[degree] = wdown[degree].T
    wgate_t[...] = wgate[...].T
    for buf in (sb0, sb1, db0, db1):
        buf[GRID_ROWS:GRID_PAD, :] = jnp.zeros((64, BLK), BF16)
    grad_ref[...] = jnp.zeros(grad_ref.shape, F32)

    def block_step(b, carry):
        lanes = pl.ds(pl.multiple_of(b * BLK, BLK), BLK)
        compute_block(lanes, x_ref, g_ref, gain_ref, wup, wgate, wdown, out_ref, dx_ref, grad_ref,
                      wup_t, wgate_t, wdown_t, kg, kf, kft, kgt, n_s, y_s, dm_s, m_s, dy_s, da_s, dn_s, (sb0, sb1), (db0, db1))
        return carry
    lax.fori_loop(0, x_ref.shape[2] // BLK, block_step, 0)


def scratch_list():
    v = pltpu.VMEM
    return [v((DEGS, HID, CH), BF16), v((HID, CH), BF16), v((DEGS, CH, HID), BF16),
            v((GRID_ROWS, BLK), BF16), v((GRID_ROWS, CH), BF16), v((CH, GRID_PAD), BF16), v((144, GRID_PAD), BF16),
            v((COEFS, CH, BLK), BF16), v((COEFS, HID, BLK), BF16), v((COEFS, HID, BLK), BF16), v((COEFS, HID, BLK), BF16),
            v((COEFS, HID, BLK), BF16), v((HID, BLK), BF16), v((COEFS, CH, BLK), F32),
            v((GRID_PAD, BLK), BF16), v((GRID_PAD, BLK), BF16), v((GRID_PAD, BLK), BF16), v((GRID_PAD, BLK), BF16)]


def compute_call(x, g, gain, wup, wgate, wdown, tog, frg):
    vm = pl.BlockSpec(memory_space=pltpu.VMEM)
    return pl.pallas_call(
        compute_kernel,
        out_shape=[jax.ShapeDtypeStruct(x.shape, BF16), jax.ShapeDtypeStruct(x.shape, BF16), jax.ShapeDtypeStruct((4, ROWS, CH), F32)],
        in_specs=[vm] * 8, out_specs=[vm] * 3, scratch_shapes=scratch_list(),
        compiler_params=pltpu.CompilerParams(vmem_limit_bytes=VMEM_LIMIT), name="ffn",
    )(x, g, gain, wup, wgate, wdown, tog, frg)


MESH = pl.DeviceIdType.MESH


def places():
    dp = lax.axis_index("dp")
    return lax.axis_index("tp"), dp // 8, (dp // 2) % 4, dp % 2


def dp_index(z, y, core):
    return (z * 4 + y) * 2 + core


def meet(peers):
    barrier = pltpu.get_barrier_semaphore()
    for peer in peers:
        pl.semaphore_signal(barrier, inc=1, device_id=peer, device_id_type=MESH)
    pl.semaphore_wait(barrier, len(peers))


def remote(src, dst, send_sem, recv_sem, peer):
    return pltpu.make_async_remote_copy(src_ref=src, dst_ref=dst, send_sem=send_sem, recv_sem=recv_sem,
                                        device_id=peer, device_id_type=MESH)


def part(i, size):
    return pl.ds(pl.multiple_of(i * size, size), size)


def gather_kernel(x_loc, g_loc, gain_loc, up_loc, gate_loc, down_loc, x_all, g_all, gain_all, up_all, gate_all, down_all,
                  act_send, act_recv, w_send, w_recv, pair_send, pair_recv, loc_sem):
    me, z, y, core = places()
    atoms = x_all.shape[2]
    pair = {"dp": dp_index(z, y, 1 - core)}
    meet([{"tp": lax.rem(me + d, TP)} for d in range(1, TP)] + [pair])
    half = part(core, 64)
    mine = part(me, CH)

    pieces = [
        (up_loc.at[:, half, :], up_all.at[:, half, mine]),
        (gate_loc.at[half, :], gate_all.at[half, mine]),
        (down_loc.at[:, half, :], down_all.at[:, part(2 * me + core, 64), :]),
    ]
    copies = []
    for d in range(1, TP):
        peer = {"tp": lax.rem(me + d, TP)}
        for i, (src, dst) in enumerate(pieces):
            copies.append(remote(src, dst, w_send.at[d - 1, i], w_recv.at[d - 1, i], peer))
        copies.append(remote(gain_loc, gain_all.at[:, part(me, 32), :], w_send.at[d - 1, 3], w_recv.at[d - 1, 3], peer))
    acts = []
    for d in range(1, TP):
        tgt = lax.rem(me + d, TP)
        peer = {"tp": tgt}
        for i, (src, dst) in enumerate(((x_loc, x_all), (g_loc, g_all))):
            acts.append(remote(src.at[:, :, part(tgt, atoms)], dst.at[:, part(me, 32), :], act_send.at[d - 1, i], act_recv.at[d - 1, i], peer))
    for c in copies + acts:
        c.start()
    local = [pltpu.make_async_copy(src, dst, loc_sem.at[i]) for i, (src, dst) in enumerate(
        pieces + [(gain_loc, gain_all.at[:, part(me, 32), :]), (x_loc.at[:, :, part(me, atoms)], x_all.at[:, part(me, 32), :]),
                  (g_loc.at[:, :, part(me, atoms)], g_all.at[:, part(me, 32), :])])]
    for c in local:
        c.start()
    for c in local:
        c.wait()
    for c in copies:
        c.wait_recv()
    pairs = [remote(up_all.at[:, half, :], up_all.at[:, half, :], pair_send.at[0], pair_recv.at[0], pair),
             remote(gate_all.at[half, :], gate_all.at[half, :], pair_send.at[1], pair_recv.at[1], pair)]
    for t in range(TP):
        rows = pl.ds(pl.multiple_of(t * CH + core * 64, 64), 64)
        pairs.append(remote(down_all.at[:, rows, :], down_all.at[:, rows, :], pair_send.at[2 + t], pair_recv.at[2 + t], pair))
    for c in pairs:
        c.start()
    for c in pairs:
        c.wait_recv()
    for c in acts:
        c.wait_recv()
    for c in copies + acts + pairs:
        c.wait_send()


def gather_call(x, g, gain, up, gate, down):
    vm = pl.BlockSpec(memory_space=pltpu.VMEM)
    hbm = pl.BlockSpec(memory_space=pl.ANY)
    dma = pltpu.SemaphoreType.DMA
    atoms = x.shape[2] // 4
    sds = jax.ShapeDtypeStruct
    return pl.pallas_call(
        gather_kernel,
        out_shape=[sds((COEFS, CH, atoms), BF16), sds((COEFS, CH, atoms), BF16), sds((DEGS, CH, CH), F32),
                   sds((DEGS, CH, HID), BF16), sds((CH, HID), BF16), sds((DEGS, HID, CH), BF16)],
        in_specs=[hbm] * 2 + [vm] * 4, out_specs=[vm] * 6,
        scratch_shapes=[dma((DEGS, 2)), dma((DEGS, 2)), dma((DEGS, 4)), dma((DEGS, 4)), dma((6,)), dma((6,)), dma((6,))],
        compiler_params=pltpu.CompilerParams(collective_id=0, has_side_effects=True, vmem_limit_bytes=VMEM_LIMIT), name="gather",
    )(x, g, gain, up, gate, down)


def scatter_kernel(out_all, dx_all, wg, out_loc, dx_loc, d_up, d_gate, d_down,
                   r1, a1, r2, a2, r3, a3, r4, fin, r5, r7, full,
                   act_send, act_recv, loc_sem, s1, q1, s2, q2, s3, q3, s4, q4, s5, q5, s6, q6):
    me, z, y, core = places()
    atoms = out_all.shape[2]
    pair = {"dp": dp_index(z, y, 1 - core)}
    x_peers = [{"tp": lax.rem(me + d, TP)} for d in range(1, TP)]
    z_peers = [{"dp": dp_index(lax.rem(z + d, 8), y, core)} for d in range(1, 8)]
    group = [(dy, dc) for dc in range(2) for dy in range(TP) if (dy, dc) != (0, 0)]
    yc_peers = [{"dp": dp_index(z, lax.rem(y + dy, 4), lax.rem(core + dc, 2))} for dy, dc in group]
    meet(x_peers + z_peers + yc_peers)
    sent = []
    c1 = remote(wg.at[:, part(1 - core, 8)], r1, s1, q1, pair)
    c1.start()
    sent.append(c1)
    acts = []
    for d in range(1, TP):
        tgt = lax.rem(me + d, TP)
        for i, (src, dst) in enumerate(((out_all, out_loc), (dx_all, dx_loc))):
            acts.append(remote(src.at[:, part(tgt, 32), :], dst.at[:, :, part(me, atoms)], act_send.at[d - 1, i], act_recv.at[d - 1, i], {"tp": tgt}))
    local = [pltpu.make_async_copy(src.at[:, part(me, 32), :], dst.at[:, :, part(me, atoms)], loc_sem.at[i])
             for i, (src, dst) in enumerate(((out_all, out_loc), (dx_all, dx_loc)))]
    for c in acts + local:
        c.start()
    c1.wait_recv()

    def sum1(i, carry):
        t, s = i // 8, i % 8
        a1[t, s] = wg[t, core * 8 + s] + r1[t, s]
        return carry
    lax.fori_loop(0, 32, sum1, 0)
    c2 = []
    for d in range(1, TP):
        ty = lax.rem(y + d, TP)
        c2.append(remote(a1.at[:, part(ty, 2)], r2.at[d - 1], s2.at[d - 1], q2.at[d - 1], {"dp": dp_index(z, ty, core)}))
    for c in c2:
        c.start()
    for c in c2:
        c.wait_recv()

    def sum2(i, carry):
        t, s = i // 2, i % 2
        a2[i] = (a1[t, y * 2 + s] + r2[0, t, s]) + (r2[1, t, s] + r2[2, t, s])
        return carry
    lax.fori_loop(0, 8, sum2, 0)
    c3 = []
    for d in range(1, 8):
        tz = lax.rem(z + d, 8)
        c3.append(remote(a2.at[tz], r3.at[d - 1], s3.at[d - 1], q3.at[d - 1], {"dp": dp_index(tz, y, core)}))
    for c in c3:
        c.start()
    for c in c3:
        c.wait_recv()
    a3[...] = ((a2[z] + r3[0]) + (r3[1] + r3[2])) + ((r3[3] + r3[4]) + (r3[5] + r3[6]))
    c4 = [remote(a3, r4.at[d - 1], s4.at[d - 1], q4.at[d - 1], x_peers[d - 1]) for d in range(1, TP)]
    for c in c4:
        c.start()
    for c in c4:
        c.wait_recv()
    half = lax.rem(z, 2)
    owner = me == z // 2
    fin[...] = ((a3[...] + r4[0]) + (r4[1] + r4[2])).astype(BF16)
    c5 = [remote(fin, r5.at[half], s5.at[d - 1], q5.at[half], z_peers[d - 1]) for d in range(1, 8)]

    @pl.when(owner)
    def _():
        for c in c5:
            c.start()
        r5[half] = fin[...]
    for h in range(2):
        @pl.when(z != 2 * me + h)
        def _():
            remote(fin, r5.at[h], s5.at[0], q5.at[h], z_peers[0]).wait_recv()
    slot = core * 4 + y
    c6 = [remote(r5, r7.at[slot], s6.at[i], q6.at[i], yc_peers[i]) for i in range(7)]
    for c in c6:
        c.start()
    r7[slot] = r5[...]
    for c in c6:
        c.wait_recv()
    for s in range(16):
        full[s * SLAB:(s + 1) * SLAB, :] = r7[s // 2, s % 2].astype(F32)
    for degree in range(DEGS):
        d_up[degree] = full[degree * CH:(degree + 1) * CH, :].astype(BF16)
        d_down[degree] = full[HID + degree * CH:GRID_PAD + degree * CH, :].astype(BF16)
    d_gate[...] = full[384:HID, :].astype(BF16)
    for c in acts:
        c.wait_recv()
    for c in local:
        c.wait()
    for c in acts + sent + c2 + c3 + c4 + c6:
        c.wait_send()

    @pl.when(owner)
    def _():
        for c in c5:
            c.wait_send()


def scatter_call(out, dx, wg):
    vm = pl.BlockSpec(memory_space=pltpu.VMEM)
    hbm = pl.BlockSpec(memory_space=pl.ANY)
    dma = pltpu.SemaphoreType.DMA
    v = pltpu.VMEM
    sds = jax.ShapeDtypeStruct
    atoms = out.shape[2]
    return pl.pallas_call(
        scatter_kernel,
        out_shape=[sds((COEFS, 32, atoms * 4), BF16), sds((COEFS, 32, atoms * 4), BF16), sds((DEGS, CH, CH), BF16), sds((CH, CH), BF16), sds((DEGS, CH, CH), BF16)],
        in_specs=[vm] * 3, out_specs=[hbm] * 2 + [vm] * 3,
        scratch_shapes=[v((TP, 8, SLAB, CH), F32), v((TP, 8, SLAB, CH), F32), v((DEGS, 4, 2, SLAB, CH), F32), v((8, SLAB, CH), F32),
                        v((7, SLAB, CH), F32), v((SLAB, CH), F32), v((DEGS, SLAB, CH), F32), v((SLAB, CH), BF16), v((2, SLAB, CH), BF16),
                        v((8, 2, SLAB, CH), BF16), v((ROWS, CH), F32),
                        dma((DEGS, 2)), dma((DEGS, 2)), dma((2,)), dma, dma, dma((3,)), dma((3,)), dma((7,)), dma((7,)), dma((3,)), dma((3,)),
                        dma((7,)), dma((2,)), dma((7,)), dma((7,))],
        compiler_params=pltpu.CompilerParams(collective_id=1, has_side_effects=True, vmem_limit_bytes=VMEM_LIMIT), name="scatter",
    )(out, dx, wg.reshape(4, 16, SLAB, CH))


def solution(mesh):
    act = P('dp', None, 'tp')
    in_specs = (act, P(None, 'tp'), P(None, None, 'tp'), P(None, 'tp'), P(None, 'tp', None), P(None, None), P(None, None), act)
    out_specs = (act, act, P(None, None, 'tp'), P(None, 'tp'), P(None, 'tp', None))

    def local_step(x, gain, up, gate, down, tog, frg, g):
        gain_b = jnp.broadcast_to(gain[:, :, None], (3, 32, CH))
        tog_p = jnp.pad(tog, ((0, 119), (0, 92)))
        frg_p = jnp.pad(frg, ((0, 92), (0, 120)))
        x_all, g_all, gain_all, up_all, gate_all, down_all = gather_call(x.transpose(1, 2, 0), g.transpose(1, 2, 0), gain_b, up, gate, down)
        out_all, dx_all, wg = compute_call(x_all, g_all, gain_all, up_all, gate_all, down_all, tog_p, frg_p)
        out, dx, d_up, d_gate, d_down = scatter_call(out_all, dx_all, wg)
        return out.transpose(2, 0, 1), dx.transpose(2, 0, 1), d_up, d_gate, d_down

    return jax.shard_map(local_step, mesh=mesh, in_specs=in_specs, out_specs=out_specs, check_vma=False)
```

```python
import functools
import jax
import jax.numpy as jnp
from jax import lax
from jax.experimental import pallas as pl
from jax.experimental.pallas import tpu as pltpu
from jax.sharding import PartitionSpec as P

NORM_EPS = 1e-5
COEFS = 9
CH = 128
HID = 512
SUB = 16
BLK = 256
GRID_ROWS = 576
GRID_PAD = 640
SLAB = 56
ROWS = 896
TILE = 16
EIGHTH = 112
NZ = 8
DEGS = 3
TP = 4
SLICE = 32
PTS = 36
VEC_SCALE = 1.0 / 1024
VMEM_LIMIT = 60 * 2**20
F32 = jnp.float32
BF16 = jnp.bfloat16


def iota(shape, axis):
    return lax.broadcasted_iota(jnp.int32, shape, axis)


def mm(a, b):
    return jnp.dot(a, b, preferred_element_type=F32)


def mm_nt(a, b):
    return lax.dot_general(a, b, (((1,), (1,)), ((), ())), preferred_element_type=F32)


def one_hot(shape, row_div, col_div):
    return jnp.where(iota(shape, 0) // row_div == iota(shape, 1) // col_div, 1.0, 0.0).astype(BF16)


def spread(table, rows, row_div, cols, col_div):
    left = mm(one_hot((rows, CH), row_div, 1), table).astype(BF16)
    full = mm(left, one_hot((CH, cols), 1, col_div))
    same = iota((rows, cols), 0) % SUB == iota((rows, cols), 1) % SUB
    return jnp.where(same, full, 0.0)


def degree_of(coef):
    return jnp.where(coef >= 4, 2, jnp.where(coef >= 1, 1, 0))


MESH = pl.DeviceIdType.MESH


def places():
    dp = lax.axis_index("dp")
    return lax.axis_index("tp"), dp // NZ, (dp // 2) % TP, dp % 2


def dp_index(z, y, core):
    return (z * TP + y) * 2 + core


def remote(src, dst, send_sem, recv_sem, peer):
    return pltpu.make_async_remote_copy(src_ref=src, dst_ref=dst, send_sem=send_sem, recv_sem=recv_sem,
                                        device_id=peer, device_id_type=MESH)


def part(i, size):
    return pl.ds(pl.multiple_of(i * size, size), size)


def start(copies):
    for c in copies:
        c.start()


def arrive(copies):
    for c in copies:
        c.wait_recv()


CHUNK = 144
GROUPS = HID // SUB
BLOCKS = 2


def step_kernel(x_loc, g_loc, gain_loc, up_loc, gate_loc, down_loc, tog_ref, frg_ref,
                out_loc, dx_loc, d_up, d_gate, d_down,
                x_all, g_all, gain_x, up_all, gate_all, down_all, out_all, dx_all, wg, pad_s, gain_b,
                wup_t, wgate_t, wdown_t, kg, kf, kft, kgt, n_s, y_s, dm_s, m_s, dy_s, da_s, dn_s, sb0, sb1, db0, db1,
                r1, a1, r2, a2, r3, a3, r4, fin, r5, r7,
                act_send, act_recv, wx_send, wx_recv, wy_send, wy_recv, wc_send, wc_recv, gain_send, gain_recv, loc_sem,
                o_send, o_recv, oloc_sem, s1, q1, s2, q2, s3, q3, s4, q4, s5, q5, s6, q6):
    me, z, y, core = places()
    atoms = x_all.shape[2]
    pair = {"dp": dp_index(z, y, 1 - core)}
    x_dist = list(range(1, TP))
    x_peers = [{"tp": lax.rem(me + d, TP)} for d in x_dist]
    y_peers = [{"dp": dp_index(z, lax.rem(y + d, TP), core)} for d in x_dist]
    z_peers = [{"dp": dp_index(lax.rem(z + d, NZ), y, core)} for d in range(1, NZ)]
    group = [(dy, dc) for dc in range(2) for dy in range(TP) if dy + dc > 0]
    yc_peers = [{"dp": dp_index(z, lax.rem(y + dy, TP), lax.rem(core + dc, 2))} for dy, dc in group]
    barrier = pltpu.get_barrier_semaphore()
    meeting = x_peers + z_peers + yc_peers
    for peer in meeting:
        pl.semaphore_signal(barrier, inc=1, device_id=peer, device_id_type=MESH)
    pl.semaphore_wait(barrier, len(meeting))

    eighth = part(core * TP + y, TILE)
    mine = part(me, CH)
    pieces = [(up_loc.at[:, eighth, :], up_all.at[:, eighth, mine]),
              (gate_loc.at[eighth, :], gate_all.at[eighth, mine]),
              (down_loc.at[:, eighth, :], down_all.at[:, me, eighth, :])]
    wx = [remote(src, dst, wx_send.at[d, i], wx_recv.at[d, i], peer)
          for d, peer in enumerate(x_peers) for i, (src, dst) in enumerate(pieces)]
    gx = [remote(gain_loc, gain_x.at[me], gain_send.at[d], gain_recv.at[d], peer) for d, peer in enumerate(x_peers)]
    start(wx + gx)
    acts = []
    for b in range(BLOCKS):
        acts.append([])
        for d, peer in enumerate(x_peers):
            tgt = lax.rem(me + d + 1, TP)
            cols = part(tgt * BLOCKS + b, BLK)
            for i, (src, dst) in enumerate(((x_loc, x_all), (g_loc, g_all))):
                acts[b].append(remote(src.at[:, :, cols], dst.at[:, part(me, SLICE), part(b, BLK)], act_send.at[b, d, i], act_recv.at[b, d, i], peer))
        start(acts[b])
    local = [pltpu.make_async_copy(src, dst, loc_sem.at[i]) for i, (src, dst) in enumerate(
        pieces + [(x_loc.at[:, :, part(me, atoms)], x_all.at[:, part(me, SLICE), :]), (g_loc.at[:, :, part(me, atoms)], g_all.at[:, part(me, SLICE), :])])]
    start(local)

    pad_s[...] = jnp.zeros(pad_s.shape, F32)
    pad_s[0, 0:COEFS, 0:PTS] = tog_ref[...]
    pad_s[1, 0:COEFS - 1, 0:PTS] = frg_ref[...]
    tog, tog_t = pad_s[0].astype(BF16), pad_s[0].T.astype(BF16)
    frg_t, frg = pad_s[1].astype(BF16), pad_s[1].T.astype(BF16)
    kg[...] = (0.5 * spread(tog_t, GRID_ROWS, SUB, BLK, SUB)).astype(BF16)
    kf[...] = (0.5 * spread(frg, GRID_ROWS, SUB, CH, SUB)).astype(BF16)
    kft[...] = spread(frg_t, CH, SUB, GRID_PAD, SUB).astype(BF16)
    kgt[...] = spread(tog, CHUNK, SUB, GRID_PAD, SUB).astype(BF16)
    for buf in (sb0, sb1, db0, db1):
        buf[GRID_ROWS:GRID_PAD, :] = jnp.zeros((GRID_PAD - GRID_ROWS, BLK), BF16)
    wg[...] = jnp.zeros(wg.shape, F32)
    gain_x[me] = gain_loc[...]
    for c in local:
        c.wait()
    arrive(wx)
    wholes = [lambda rows: up_all.at[:, rows, :], lambda rows: gate_all.at[rows, :], lambda rows: down_all.at[:, :, rows, :]]
    wy = [remote(whole(eighth), whole(eighth), wy_send.at[d, i], wy_recv.at[d, i], peer)
          for d, peer in enumerate(y_peers) for i, whole in enumerate(wholes)]
    start(wy)
    arrive(gx)
    for t in range(TP):
        pad_s[2, t * NZ:t * NZ + DEGS, 0:SLICE] = gain_x[t]
    cols = pad_s[2].T
    for t in range(TP):
        for degree in range(DEGS):
            col = t * NZ + degree
            gain_b[degree, t * SLICE:(t + 1) * SLICE, :] = jnp.broadcast_to(cols[0:SLICE, col:col + 1], (SLICE, BLK))
    arrive(wy)
    side = part(core, CH // 2)
    wc = [remote(whole(side), whole(side), wc_send.at[i], wc_recv.at[i], pair) for i, whole in enumerate(wholes)]
    start(wc)
    arrive(wc)
    for degree in range(DEGS):
        wup_t[degree] = up_all[degree].T
        wdown_t[degree] = down_all[degree].reshape(HID, CH).T
    wgate_t[...] = gate_all[...].T

    def gain_of(coef):
        return gain_b[0 if coef == 0 else (1 if coef < TP else 2)]

    def norm(lanes):
        x0 = x_all[0, :, lanes].astype(F32)
        mean_s = jnp.sum(x0, axis=0, keepdims=True) * (1.0 / CH)
        cen = x0 - mean_s
        inv_s = lax.rsqrt(jnp.sum(cen * cen, axis=0, keepdims=True) * (1.0 / CH) + NORM_EPS)
        n_s[0] = ((cen * inv_s) * gain_of(0)).astype(BF16)
        acc = jnp.zeros((CH, BLK), F32)
        for coef in range(1, COEFS):
            xk = x_all[coef, :, lanes].astype(F32)
            acc = acc + xk * xk
        inv_v = lax.rsqrt(jnp.sum(acc, axis=0, keepdims=True) * VEC_SCALE + NORM_EPS)
        for coef in range(1, COEFS):
            xk = x_all[coef, :, lanes].astype(F32)
            n_s[coef] = ((xk * inv_v) * gain_of(coef)).astype(BF16)
        return mean_s, inv_s, inv_v

    def up(lanes):
        def up_step(coef, carry):
            degree = degree_of(coef)
            y_s[coef] = mm(wup_t[degree], n_s[coef]).astype(BF16)
            dm_s[coef] = mm(down_all[degree].reshape(HID, CH), g_all[coef, :, lanes]).astype(BF16)
            return carry
        lax.fori_loop(0, COEFS, up_step, 0)

        def gate_step(i, carry):
            rows = part(i, CH)
            half = (0.5 * mm(wgate_t[rows, :], n_s[0])).astype(BF16).astype(F32)
            th = jnp.tanh(half)
            plus = 1.0 + th
            val = half * plus
            m_s[0, rows, :] = val.astype(BF16)
            slope = 0.5 * (plus + val * (1.0 - th))
            da_s[rows, :] = (dm_s[0, rows, :].astype(F32) * slope).astype(BF16)
            return carry
        lax.fori_loop(0, TP, gate_step, 0)

    def expand(j, s_buf, du_buf):
        rows = part(j, SUB)
        yj = y_s[:, rows, :].reshape(CHUNK, BLK)
        dzj = dm_s[1:, rows, :].reshape(CH, BLK)
        for r0 in range(0, GRID_ROWS, CHUNK):
            half = mm(kg[r0:r0 + CHUNK, 0:CHUNK], yj).astype(BF16).astype(F32)
            dval = mm(kf[r0:r0 + CHUNK, :], dzj).astype(BF16).astype(F32)
            th = jnp.tanh(half)
            plus = 1.0 + th
            val = half * plus
            s_buf[r0:r0 + CHUNK, :] = val.astype(BF16)
            du_buf[r0:r0 + CHUNK, :] = (dval * (plus + val * (1.0 - th))).astype(BF16)

    def contract(j, s_buf, du_buf):
        rows = part(j, SUB)
        m_s[1:, rows, :] = mm(kft[...], s_buf[...]).astype(BF16).reshape(COEFS - 1, SUB, BLK)
        dy_s[:, rows, :] = mm(kgt[...], du_buf[...]).astype(BF16).reshape(COEFS, SUB, BLK)

    def grid_step(i, carry):
        expand(2 * i + 1, sb1, db1)
        contract(2 * i, sb0, db0)
        expand(jnp.minimum(2 * i + 2, GROUPS - 1), sb0, db0)
        contract(2 * i + 1, sb1, db1)
        return carry

    def weight_grads(t, lanes):
        rows = part(t, CH)

        def coef_step(coef, carry):
            base = degree_of(coef) * CH
            wg[t, part(degree_of(coef), CH), :] += mm_nt(n_s[coef], dy_s[coef, rows, :])
            wg[t, part(degree_of(coef) + TP, CH), :] += mm_nt(m_s[coef, rows, :], g_all[coef, :, lanes])
            return carry
        lax.fori_loop(0, COEFS, coef_step, 0)
        wg[t, part(DEGS, CH), :] += mm_nt(n_s[0], da_s[rows, :])

    def down(lanes):
        def down_step(coef, carry):
            degree = degree_of(coef)
            xk = x_all[coef, :, lanes].astype(F32)
            out_all[coef, :, lanes] = (xk + mm(wdown_t[degree], m_s[coef])).astype(BF16)
            dn_s[coef] = mm(up_all[degree], dy_s[coef])
            return carry
        lax.fori_loop(0, COEFS, down_step, 0)
        dn_s[0] += mm(gate_all[...], da_s[...])

    def norm_back(lanes, mean_s, inv_s, inv_v):
        hat = (x_all[0, :, lanes].astype(F32) - mean_s) * inv_s
        dh = dn_s[0].astype(BF16).astype(F32) * gain_of(0)
        m1 = jnp.sum(dh, axis=0, keepdims=True) * (1.0 / CH)
        m2 = jnp.sum(dh * hat, axis=0, keepdims=True) * (1.0 / CH)
        dx_all[0, :, lanes] = (inv_s * (dh - m1 - hat * m2) + g_all[0, :, lanes].astype(F32)).astype(BF16)
        acc = jnp.zeros((CH, BLK), F32)
        for coef in range(1, COEFS):
            xk = x_all[coef, :, lanes].astype(F32)
            acc = acc + (dn_s[coef].astype(BF16).astype(F32) * gain_of(coef)) * (xk * inv_v)
        mv = jnp.sum(acc, axis=0, keepdims=True) * VEC_SCALE
        for coef in range(1, COEFS):
            xk = x_all[coef, :, lanes].astype(F32)
            dh = dn_s[coef].astype(BF16).astype(F32) * gain_of(coef)
            dx_all[coef, :, lanes] = (inv_v * (dh - (xk * inv_v) * mv) + g_all[coef, :, lanes].astype(F32)).astype(BF16)

    outs = ((out_all, out_loc), (dx_all, dx_loc))

    def out_copies(b, i):
        src, dst = outs[i]
        cols = part(me * BLOCKS + b, BLK)
        return [remote(src.at[:, part(lax.rem(me + d, TP), SLICE), part(b, BLK)], dst.at[:, :, cols],
                       o_send.at[b, i, d - 1], o_recv.at[b, i, d - 1], x_peers[d - 1]) for d in x_dist]

    def out_local(b, i):
        src, dst = outs[i]
        return pltpu.make_async_copy(src.at[:, part(me, SLICE), part(b, BLK)], dst.at[:, :, part(me * BLOCKS + b, BLK)], oloc_sem.at[b, i])

    sent = [[out_copies(b, i) for i in range(2)] for b in range(BLOCKS)]
    kept = [[out_local(b, i) for i in range(2)] for b in range(BLOCKS)]

    def send_out(b, i):
        start(sent[b][i])
        kept[b][i].start()

    half_rows = ROWS // 2
    c1 = [remote(wg.at[t, part(1 - core, half_rows), :], r1.at[t], s1.at[t], q1.at[t], pair) for t in range(TP)]
    c2 = [[remote(a1.at[t, part(lax.rem(y + d, TP), EIGHTH), :], r2.at[t, d - 1], s2.at[t, d - 1], q2.at[t, d - 1], y_peers[d - 1]) for d in x_dist]
          for t in range(TP)]
    c3 = [[remote(a2.at[t, part(lax.rem(lax.rem(z + d, NZ), NZ - 1), TILE), :], r3.at[t, d - 1], s3.at[t, d - 1], q3.at[t, d - 1], z_peers[d - 1])
           for d in range(1, NZ)] for t in range(TP)]
    c4 = [[remote(a3.at[t], r4.at[t, d - 1], s4.at[t, d - 1], q4.at[t, d - 1], x_peers[d - 1]) for d in x_dist] for t in range(TP)]
    c5 = [remote(fin, r5.at[part(z, TILE), :], s5.at[d - 1], q5.at[d - 1], z_peers[d - 1]) for d in range(1, NZ)]

    def sum_core(t):
        arrive([c1[t]])
        a1[t] = wg[t, part(core, half_rows), :] + r1[t]
        start(c2[t])

    def sum_y(t):
        arrive(c2[t])
        a2[t] = (a1[t, part(y, EIGHTH), :] + r2[t, 0]) + (r2[t, 1] + r2[t, 2])
        start(c3[t])

    def sum_z(t):
        arrive(c3[t])
        own = a2[t, part(lax.rem(z, NZ - 1), TILE), :]
        a3[t] = ((own + r3[t, 0]) + (r3[t, 1] + r3[t, 2])) + ((r3[t, 3] + r3[t, 4]) + (r3[t, 5] + r3[t, 6]))
        start(c4[t])

    def sum_x(t):
        arrive(c4[t])

        @pl.when(me == t)
        def _():
            fin[...] = ((a3[t] + r4[t, 0]) + (r4[t, 1] + r4[t, 2])).astype(BF16)
            start(c5)
            r5[part(z, TILE), :] = fin[...]

    first, second = pl.ds(0, BLK), pl.ds(BLK, BLK)
    arrive(acts[0])
    stats = norm(first)
    up(first)
    expand(0, sb0, db0)
    lax.fori_loop(0, GROUPS // 2, grid_step, 0)
    down(first)
    send_out(0, 0)
    norm_back(first, *stats)
    send_out(0, 1)

    def grads_step(t, carry):
        weight_grads(t, first)
        return carry
    lax.fori_loop(0, TP, grads_step, 0)

    arrive(acts[1])
    stats = norm(second)
    up(second)
    expand(0, sb0, db0)
    per = GROUPS // 2 // TP
    for t in range(TP):
        lax.fori_loop(t * per, (t + 1) * per, grid_step, 0)
        if t > 0:
            sum_core(t - 1)
        if t == TP - 1:
            sum_y(0)
        weight_grads(t, second)
        start([c1[t]])
    down(second)
    send_out(1, 0)
    sum_core(TP - 1)
    sum_y(1)
    norm_back(second, *stats)
    sum_z(0)
    sum_y(2)
    sum_z(1)
    sum_x(0)
    sum_y(3)
    sum_z(2)
    sum_x(1)
    sum_z(3)
    send_out(1, 1)
    sum_x(2)
    sum_x(3)
    arrive(c5)
    slot = part(core * TP + y, EIGHTH)
    c6 = [remote(r5.at[0:EIGHTH, :], r7.at[slot, :], s6.at[i], q6.at[i], yc_peers[i]) for i in range(len(group))]
    start(c6)
    r7[slot, :] = r5[0:EIGHTH, :]
    arrive(c6)
    for degree in range(DEGS):
        d_up[degree] = r7[degree * CH:(degree + 1) * CH, :]
        d_down[degree] = r7[(TP + degree) * CH:(TP + degree + 1) * CH, :]
    d_gate[...] = r7[DEGS * CH:TP * CH, :]
    finished = wx + gx + wy + wc + c1 + c5 + c6
    for group_of in acts + c2 + c3 + c4:
        finished = finished + group_of
    for b in range(BLOCKS):
        for i in range(2):
            arrive(sent[b][i])
            kept[b][i].wait()
            finished = finished + sent[b][i]
    for c in finished:
        c.wait_send()


def step_call(x, g, gain, up, gate, down, tog, frg):
    vm = pl.BlockSpec(memory_space=pltpu.VMEM)
    hbm = pl.BlockSpec(memory_space=pl.ANY)
    dma = pltpu.SemaphoreType.DMA
    v = pltpu.VMEM
    sds = jax.ShapeDtypeStruct
    atoms = x.shape[2] // TP
    act = (COEFS, CH, atoms)
    hid = (COEFS, HID, BLK)
    peers = TP - 1
    zs = NZ - 1
    return pl.pallas_call(
        step_kernel,
        out_shape=[sds(x.shape, BF16), sds(x.shape, BF16), sds((DEGS, CH, CH), BF16), sds((CH, CH), BF16), sds((DEGS, CH, CH), BF16)],
        in_specs=[hbm] * 2 + [vm] * 6, out_specs=[hbm] * 2 + [vm] * 3,
        scratch_shapes=[
            v(act, BF16), v(act, BF16), v((TP, DEGS, SLICE), F32), v((DEGS, CH, HID), BF16), v((CH, HID), BF16), v((DEGS, TP, CH, CH), BF16),
            v(act, BF16), v(act, BF16), v((TP, ROWS, CH), F32), v((DEGS, CH, CH), F32), v((DEGS, CH, BLK), F32),
            v((DEGS, HID, CH), BF16), v((HID, CH), BF16), v((DEGS, CH, HID), BF16),
            v((GRID_ROWS, BLK), BF16), v((GRID_ROWS, CH), BF16), v((CH, GRID_PAD), BF16), v((CHUNK, GRID_PAD), BF16),
            v((COEFS, CH, BLK), BF16), v(hid, BF16), v(hid, BF16), v(hid, BF16), v(hid, BF16), v((HID, BLK), BF16), v((COEFS, CH, BLK), F32),
            v((GRID_PAD, BLK), BF16), v((GRID_PAD, BLK), BF16), v((GRID_PAD, BLK), BF16), v((GRID_PAD, BLK), BF16),
            v((TP, ROWS // 2, CH), F32), v((TP, ROWS // 2, CH), F32), v((TP, peers, EIGHTH, CH), F32), v((TP, EIGHTH, CH), F32),
            v((TP, zs, TILE, CH), F32), v((TP, TILE, CH), F32), v((TP, peers, TILE, CH), F32), v((TILE, CH), BF16),
            v((NZ * TILE, CH), BF16), v((ROWS, CH), BF16),
            dma((BLOCKS, peers, 2)), dma((BLOCKS, peers, 2)), dma((peers, 3)), dma((peers, 3)), dma((peers, 3)), dma((peers, 3)), dma((3,)), dma((3,)),
            dma((peers,)), dma((peers,)), dma((5,)),
            dma((BLOCKS, 2, peers)), dma((BLOCKS, 2, peers)), dma((BLOCKS, 2)),
            dma((TP,)), dma((TP,)), dma((TP, peers)), dma((TP, peers)), dma((TP, zs)), dma((TP, zs)), dma((TP, peers)), dma((TP, peers)),
            dma((zs,)), dma((zs,)), dma((zs,)), dma((zs,))],
        compiler_params=pltpu.CompilerParams(collective_id=0, has_side_effects=True, vmem_limit_bytes=VMEM_LIMIT), name="step",
    )(x, g, gain, up, gate, down, tog, frg)


def solution(mesh):
    act = P('dp', None, 'tp')
    in_specs = (act, P(None, 'tp'), P(None, None, 'tp'), P(None, 'tp'), P(None, 'tp', None), P(None, None), P(None, None), act)
    out_specs = (act, act, P(None, None, 'tp'), P(None, 'tp'), P(None, 'tp', None))

    def local_step(x, gain, up, gate, down, tog, frg, g):
        out, dx, d_up, d_gate, d_down = step_call(x.transpose(1, 2, 0), g.transpose(1, 2, 0), gain, up, gate, down, tog, frg.T)
        return out.transpose(2, 0, 1), dx.transpose(2, 0, 1), d_up, d_gate, d_down

    return jax.shard_map(local_step, mesh=mesh, in_specs=in_specs, out_specs=out_specs, check_vma=False)
```

```python
import jax
import jax.numpy as jnp
from jax import lax
from jax.experimental import pallas as pl
from jax.experimental.pallas import tpu as pltpu
from jax.sharding import PartitionSpec as P

NORM_EPS = 1e-5
COEFS = 9
CH = 128
HID = 512
SUB = 16
BLK = 256
GRID_ROWS = 576
GRID_PAD = 640
SLAB = 56
ROWS = 896
TILE = 16
EIGHTH = 112
NZ = 8
DEGS = 3
TP = 4
SLICE = 32
PTS = 36
VEC_SCALE = 1.0 / 1024
VMEM_LIMIT = 60 * 2**20
F32 = jnp.float32
BF16 = jnp.bfloat16


def iota(shape, axis):
    return lax.broadcasted_iota(jnp.int32, shape, axis)


def mm(a, b):
    return jnp.dot(a, b, preferred_element_type=F32)


def mm_nt(a, b):
    return lax.dot_general(a, b, (((1,), (1,)), ((), ())), preferred_element_type=F32)


def one_hot(shape, row_div, col_div):
    return jnp.where(iota(shape, 0) // row_div == iota(shape, 1) // col_div, 1.0, 0.0).astype(BF16)


def spread(table, rows, row_div, cols, col_div):
    left = mm(one_hot((rows, CH), row_div, 1), table).astype(BF16)
    full = mm(left, one_hot((CH, cols), 1, col_div))
    same = iota((rows, cols), 0) % SUB == iota((rows, cols), 1) % SUB
    return jnp.where(same, full, 0.0)


def degree_of(coef):
    return jnp.where(coef >= 4, 2, jnp.where(coef >= 1, 1, 0))


MESH = pl.DeviceIdType.MESH


def places():
    dp = lax.axis_index("dp")
    return lax.axis_index("tp"), dp // NZ, (dp // 2) % TP, dp % 2


def dp_index(z, y, core):
    return (z * TP + y) * 2 + core


def remote(src, dst, send_sem, recv_sem, peer):
    return pltpu.make_async_remote_copy(src_ref=src, dst_ref=dst, send_sem=send_sem, recv_sem=recv_sem,
                                        device_id=peer, device_id_type=MESH)


def part(i, size):
    return pl.ds(pl.multiple_of(i * size, size), size)


def start(copies):
    for c in copies:
        c.start()


def arrive(copies):
    for c in copies:
        c.wait_recv()


CHUNK = 144
GROUPS = HID // SUB
BLOCKS = 2


def step_kernel(x_loc, g_loc, gain_loc, up_loc, gate_loc, down_loc, tog_ref, frg_ref,
                out_loc, dx_loc, d_up, d_gate, d_down,
                x_all, g_all, gain_x, up_all, gate_all, down_all, out_all, dx_all, wg, pad_s, gain_b,
                wup_t, wgate_t, wdown_t, kg, kf, kft, kgt, n_s, y_s, dm_s, m_s, dy_s, da_s, dn_s, sb0, sb1, db0, db1,
                r1, a1, r2, a2, r3, a3, r4, fin, r5, r7,
                act_send, act_recv, wx_send, wx_recv, wy_send, wy_recv, wc_send, wc_recv, gain_send, gain_recv, loc_sem,
                o_send, o_recv, oloc_sem, s1, q1, s2, q2, s3, q3, s4, q4, s5, q5, s6, q6):
    me, z, y, core = places()
    atoms = x_all.shape[2]
    pair = {"dp": dp_index(z, y, 1 - core)}
    x_dist = list(range(1, TP))
    x_peers = [{"tp": lax.rem(me + d, TP)} for d in x_dist]
    y_peers = [{"dp": dp_index(z, lax.rem(y + d, TP), core)} for d in x_dist]
    z_peers = [{"dp": dp_index(lax.rem(z + d, NZ), y, core)} for d in range(1, NZ)]
    group = [(dy, dc) for dc in range(2) for dy in range(TP) if dy + dc > 0]
    yc_peers = [{"dp": dp_index(z, lax.rem(y + dy, TP), lax.rem(core + dc, 2))} for dy, dc in group]
    barrier = pltpu.get_barrier_semaphore()
    meeting = x_peers + z_peers + yc_peers
    for peer in meeting:
        pl.semaphore_signal(barrier, inc=1, device_id=peer, device_id_type=MESH)
    pl.semaphore_wait(barrier, len(meeting))

    eighth = part(core * TP + y, TILE)
    mine = part(me, CH)
    pieces = [(up_loc.at[:, eighth, :], up_all.at[:, eighth, mine]),
              (gate_loc.at[eighth, :], gate_all.at[eighth, mine]),
              (down_loc.at[:, eighth, :], down_all.at[:, me, eighth, :])]
    wx = [remote(src, dst, wx_send.at[d, i], wx_recv.at[d, i], peer)
          for d, peer in enumerate(x_peers) for i, (src, dst) in enumerate(pieces)]
    gx = [remote(gain_loc, gain_x.at[me], gain_send.at[d], gain_recv.at[d], peer) for d, peer in enumerate(x_peers)]
    start(wx + gx)
    acts = []
    for b in range(BLOCKS):
        acts.append([])
        for d, peer in enumerate(x_peers):
            tgt = lax.rem(me + d + 1, TP)
            cols = part(tgt * BLOCKS + b, BLK)
            for i, (src, dst) in enumerate(((x_loc, x_all), (g_loc, g_all))):
                acts[b].append(remote(src.at[:, :, cols], dst.at[:, part(me, SLICE), part(b, BLK)], act_send.at[b, d, i], act_recv.at[b, d, i], peer))
    start(acts[0])
    local = [pltpu.make_async_copy(src, dst, loc_sem.at[i]) for i, (src, dst) in enumerate(
        pieces + [(x_loc.at[:, :, part(me, atoms)], x_all.at[:, part(me, SLICE), :]), (g_loc.at[:, :, part(me, atoms)], g_all.at[:, part(me, SLICE), :])])]
    start(local)

    pad_s[...] = jnp.zeros(pad_s.shape, F32)
    pad_s[0, 0:COEFS, 0:PTS] = tog_ref[...]
    pad_s[1, 0:COEFS - 1, 0:PTS] = frg_ref[...]
    tog, tog_t = pad_s[0].astype(BF16), pad_s[0].T.astype(BF16)
    frg_t, frg = pad_s[1].astype(BF16), pad_s[1].T.astype(BF16)
    kg[...] = (0.5 * spread(tog_t, GRID_ROWS, SUB, BLK, SUB)).astype(BF16)
    kf[...] = (0.5 * spread(frg, GRID_ROWS, SUB, CH, SUB)).astype(BF16)
    kft[...] = spread(frg_t, CH, SUB, GRID_PAD, SUB).astype(BF16)
    kgt[...] = spread(tog, CHUNK, SUB, GRID_PAD, SUB).astype(BF16)
    for buf in (sb0, sb1, db0, db1):
        buf[GRID_ROWS:GRID_PAD, :] = jnp.zeros((GRID_PAD - GRID_ROWS, BLK), BF16)
    wg[...] = jnp.zeros(wg.shape, F32)
    gain_x[me] = gain_loc[...]
    for c in local:
        c.wait()
    arrive(wx)
    wholes = [lambda rows: up_all.at[:, rows, :], lambda rows: gate_all.at[rows, :], lambda rows: down_all.at[:, :, rows, :]]
    wy = [remote(whole(eighth), whole(eighth), wy_send.at[d, i], wy_recv.at[d, i], peer)
          for d, peer in enumerate(y_peers) for i, whole in enumerate(wholes)]
    start(wy)
    arrive(gx)
    for t in range(TP):
        pad_s[2, t * NZ:t * NZ + DEGS, 0:SLICE] = gain_x[t]
    cols = pad_s[2].T
    for t in range(TP):
        for degree in range(DEGS):
            col = t * NZ + degree
            gain_b[degree, t * SLICE:(t + 1) * SLICE, :] = jnp.broadcast_to(cols[0:SLICE, col:col + 1], (SLICE, BLK))
    arrive(wy)
    side = part(core, CH // 2)
    wc = [remote(whole(side), whole(side), wc_send.at[i], wc_recv.at[i], pair) for i, whole in enumerate(wholes)]
    start(wc)
    arrive(wc)
    for degree in range(DEGS):
        wup_t[degree] = up_all[degree].T
        wdown_t[degree] = down_all[degree].reshape(HID, CH).T
    wgate_t[...] = gate_all[...].T

    def gain_of(coef):
        return gain_b[0 if coef == 0 else (1 if coef < TP else 2)]

    def norm(lanes):
        x0 = x_all[0, :, lanes].astype(F32)
        mean_s = jnp.sum(x0, axis=0, keepdims=True) * (1.0 / CH)
        cen = x0 - mean_s
        inv_s = lax.rsqrt(jnp.sum(cen * cen, axis=0, keepdims=True) * (1.0 / CH) + NORM_EPS)
        n_s[0] = ((cen * inv_s) * gain_of(0)).astype(BF16)
        acc = jnp.zeros((CH, BLK), F32)
        for coef in range(1, COEFS):
            xk = x_all[coef, :, lanes].astype(F32)
            acc = acc + xk * xk
        inv_v = lax.rsqrt(jnp.sum(acc, axis=0, keepdims=True) * VEC_SCALE + NORM_EPS)
        for coef in range(1, COEFS):
            xk = x_all[coef, :, lanes].astype(F32)
            n_s[coef] = ((xk * inv_v) * gain_of(coef)).astype(BF16)
        return mean_s, inv_s, inv_v

    def up(lanes):
        def up_step(coef, carry):
            degree = degree_of(coef)
            y_s[coef] = mm(wup_t[degree], n_s[coef]).astype(BF16)
            dm_s[coef] = mm(down_all[degree].reshape(HID, CH), g_all[coef, :, lanes]).astype(BF16)
            return carry
        lax.fori_loop(0, COEFS, up_step, 0)

        def gate_step(i, carry):
            rows = part(i, CH)
            half = (0.5 * mm(wgate_t[rows, :], n_s[0])).astype(BF16).astype(F32)
            th = jnp.tanh(half)
            plus = 1.0 + th
            val = half * plus
            m_s[0, rows, :] = val.astype(BF16)
            slope = 0.5 * (plus + val * (1.0 - th))
            da_s[rows, :] = (dm_s[0, rows, :].astype(F32) * slope).astype(BF16)
            return carry
        lax.fori_loop(0, TP, gate_step, 0)

    def expand(j, s_buf, du_buf):
        rows = part(j, SUB)
        yj = y_s[:, rows, :].reshape(CHUNK, BLK)
        dzj = dm_s[1:, rows, :].reshape(CH, BLK)
        for r0 in range(0, GRID_ROWS, CHUNK):
            half = mm(kg[r0:r0 + CHUNK, 0:CHUNK], yj).astype(BF16).astype(F32)
            dval = mm(kf[r0:r0 + CHUNK, :], dzj).astype(BF16).astype(F32)
            th = jnp.tanh(half)
            plus = 1.0 + th
            val = half * plus
            s_buf[r0:r0 + CHUNK, :] = val.astype(BF16)
            du_buf[r0:r0 + CHUNK, :] = (dval * (plus + val * (1.0 - th))).astype(BF16)

    def contract(j, s_buf, du_buf):
        rows = part(j, SUB)
        m_s[1:, rows, :] = mm(kft[...], s_buf[...]).astype(BF16).reshape(COEFS - 1, SUB, BLK)
        dy_s[:, rows, :] = mm(kgt[...], du_buf[...]).astype(BF16).reshape(COEFS, SUB, BLK)

    def grid_step(i, carry):
        expand(2 * i + 1, sb1, db1)
        contract(2 * i, sb0, db0)
        expand(jnp.minimum(2 * i + 2, GROUPS - 1), sb0, db0)
        contract(2 * i + 1, sb1, db1)
        return carry

    def weight_grads(t, lanes):
        rows = part(t, CH)

        def coef_step(coef, carry):
            base = degree_of(coef) * CH
            wg[t, part(degree_of(coef), CH), :] += mm_nt(n_s[coef], dy_s[coef, rows, :])
            wg[t, part(degree_of(coef) + TP, CH), :] += mm_nt(m_s[coef, rows, :], g_all[coef, :, lanes])
            return carry
        lax.fori_loop(0, COEFS, coef_step, 0)
        wg[t, part(DEGS, CH), :] += mm_nt(n_s[0], da_s[rows, :])

    def down(lanes):
        def down_step(coef, carry):
            degree = degree_of(coef)
            xk = x_all[coef, :, lanes].astype(F32)
            out_all[coef, :, lanes] = (xk + mm(wdown_t[degree], m_s[coef])).astype(BF16)
            dn_s[coef] = mm(up_all[degree], dy_s[coef])
            return carry
        lax.fori_loop(0, COEFS, down_step, 0)
        dn_s[0] += mm(gate_all[...], da_s[...])

    def norm_back(lanes, mean_s, inv_s, inv_v):
        hat = (x_all[0, :, lanes].astype(F32) - mean_s) * inv_s
        dh = dn_s[0].astype(BF16).astype(F32) * gain_of(0)
        m1 = jnp.sum(dh, axis=0, keepdims=True) * (1.0 / CH)
        m2 = jnp.sum(dh * hat, axis=0, keepdims=True) * (1.0 / CH)
        dx_all[0, :, lanes] = (inv_s * (dh - m1 - hat * m2) + g_all[0, :, lanes].astype(F32)).astype(BF16)
        acc = jnp.zeros((CH, BLK), F32)
        for coef in range(1, COEFS):
            xk = x_all[coef, :, lanes].astype(F32)
            acc = acc + (dn_s[coef].astype(BF16).astype(F32) * gain_of(coef)) * (xk * inv_v)
        mv = jnp.sum(acc, axis=0, keepdims=True) * VEC_SCALE
        for coef in range(1, COEFS):
            xk = x_all[coef, :, lanes].astype(F32)
            dh = dn_s[coef].astype(BF16).astype(F32) * gain_of(coef)
            dx_all[coef, :, lanes] = (inv_v * (dh - (xk * inv_v) * mv) + g_all[coef, :, lanes].astype(F32)).astype(BF16)

    outs = ((out_all, out_loc), (dx_all, dx_loc))

    def out_copies(b, i):
        src, dst = outs[i]
        cols = part(me * BLOCKS + b, BLK)
        return [remote(src.at[:, part(lax.rem(me + d, TP), SLICE), part(b, BLK)], dst.at[:, :, cols],
                       o_send.at[b, i, d - 1], o_recv.at[b, i, d - 1], x_peers[d - 1]) for d in x_dist]

    def out_local(b, i):
        src, dst = outs[i]
        return pltpu.make_async_copy(src.at[:, part(me, SLICE), part(b, BLK)], dst.at[:, :, part(me * BLOCKS + b, BLK)], oloc_sem.at[b, i])

    sent = [[out_copies(b, i) for i in range(2)] for b in range(BLOCKS)]
    kept = [[out_local(b, i) for i in range(2)] for b in range(BLOCKS)]

    def send_out(b, i):
        start(sent[b][i])
        kept[b][i].start()

    half_rows = ROWS // 2
    c1 = [remote(wg.at[t, part(1 - core, half_rows), :], r1.at[t], s1.at[t], q1.at[t], pair) for t in range(TP)]
    c2 = [[remote(a1.at[t, part(lax.rem(y + d, TP), EIGHTH), :], r2.at[t, d - 1], s2.at[t, d - 1], q2.at[t, d - 1], y_peers[d - 1]) for d in x_dist]
          for t in range(TP)]
    c3 = [[remote(a2.at[t, part(lax.rem(lax.rem(z + d, NZ), NZ - 1), TILE), :], r3.at[t, d - 1], s3.at[t, d - 1], q3.at[t, d - 1], z_peers[d - 1])
           for d in range(1, NZ)] for t in range(TP)]
    c4 = [[remote(a3.at[t], r4.at[t, d - 1], s4.at[t, d - 1], q4.at[t, d - 1], x_peers[d - 1]) for d in x_dist] for t in range(TP)]
    c5 = [remote(fin, r5.at[part(z, TILE), :], s5.at[d - 1], q5.at[d - 1], z_peers[d - 1]) for d in range(1, NZ)]

    def sum_core(t):
        arrive([c1[t]])
        a1[t] = wg[t, part(core, half_rows), :] + r1[t]
        start(c2[t])

    def sum_y(t):
        arrive(c2[t])
        a2[t] = (a1[t, part(y, EIGHTH), :] + r2[t, 0]) + (r2[t, 1] + r2[t, 2])
        start(c3[t])

    def sum_z(t):
        arrive(c3[t])
        own = a2[t, part(lax.rem(z, NZ - 1), TILE), :]
        a3[t] = ((own + r3[t, 0]) + (r3[t, 1] + r3[t, 2])) + ((r3[t, 3] + r3[t, 4]) + (r3[t, 5] + r3[t, 6]))
        start(c4[t])

    def sum_x(t):
        arrive(c4[t])

        @pl.when(me == t)
        def _():
            fin[...] = ((a3[t] + r4[t, 0]) + (r4[t, 1] + r4[t, 2])).astype(BF16)
            start(c5)
            r5[part(z, TILE), :] = fin[...]

    first, second = pl.ds(0, BLK), pl.ds(BLK, BLK)
    for c in acts[0]:
        c.wait_send()
    start(acts[1])
    arrive(acts[0])
    stats = norm(first)
    up(first)
    expand(0, sb0, db0)
    lax.fori_loop(0, GROUPS // 2, grid_step, 0)
    down(first)
    send_out(0, 0)
    norm_back(first, *stats)
    send_out(0, 1)

    def grads_step(t, carry):
        weight_grads(t, first)
        return carry
    lax.fori_loop(0, TP, grads_step, 0)

    arrive(acts[1])
    stats = norm(second)
    up(second)
    expand(0, sb0, db0)
    per = GROUPS // 2 // TP
    for t in range(TP):
        lax.fori_loop(t * per, (t + 1) * per, grid_step, 0)
        if t > 0:
            sum_core(t - 1)
        if t == TP - 1:
            sum_y(0)
        weight_grads(t, second)
        start([c1[t]])
    down(second)
    send_out(1, 0)
    sum_core(TP - 1)
    sum_y(1)
    norm_back(second, *stats)
    sum_z(0)
    sum_y(2)
    sum_z(1)
    sum_x(0)
    sum_y(3)
    sum_z(2)
    sum_x(1)
    sum_z(3)
    send_out(1, 1)
    sum_x(2)
    sum_x(3)
    arrive(c5)
    slot = part(core * TP + y, EIGHTH)
    c6 = [remote(r5.at[0:EIGHTH, :], r7.at[slot, :], s6.at[i], q6.at[i], yc_peers[i]) for i in range(len(group))]
    start(c6)
    r7[slot, :] = r5[0:EIGHTH, :]
    arrive(c6)
    for degree in range(DEGS):
        d_up[degree] = r7[degree * CH:(degree + 1) * CH, :]
        d_down[degree] = r7[(TP + degree) * CH:(TP + degree + 1) * CH, :]
    d_gate[...] = r7[DEGS * CH:TP * CH, :]
    finished = wx + gx + wy + wc + c1 + c5 + c6
    for group_of in [acts[1]] + c2 + c3 + c4:
        finished = finished + group_of
    for b in range(BLOCKS):
        for i in range(2):
            arrive(sent[b][i])
            kept[b][i].wait()
            finished = finished + sent[b][i]
    for c in finished:
        c.wait_send()


def step_call(x, g, gain, up, gate, down, tog, frg):
    vm = pl.BlockSpec(memory_space=pltpu.VMEM)
    hbm = pl.BlockSpec(memory_space=pl.ANY)
    dma = pltpu.SemaphoreType.DMA
    v = pltpu.VMEM
    sds = jax.ShapeDtypeStruct
    atoms = x.shape[2] // TP
    act = (COEFS, CH, atoms)
    hid = (COEFS, HID, BLK)
    peers = TP - 1
    zs = NZ - 1
    return pl.pallas_call(
        step_kernel,
        out_shape=[sds(x.shape, BF16), sds(x.shape, BF16), sds((DEGS, CH, CH), BF16), sds((CH, CH), BF16), sds((DEGS, CH, CH), BF16)],
        in_specs=[hbm] * 2 + [vm] * 6, out_specs=[hbm] * 2 + [vm] * 3,
        scratch_shapes=[
            v(act, BF16), v(act, BF16), v((TP, DEGS, SLICE), F32), v((DEGS, CH, HID), BF16), v((CH, HID), BF16), v((DEGS, TP, CH, CH), BF16),
            v(act, BF16), v(act, BF16), v((TP, ROWS, CH), F32), v((DEGS, CH, CH), F32), v((DEGS, CH, BLK), F32),
            v((DEGS, HID, CH), BF16), v((HID, CH), BF16), v((DEGS, CH, HID), BF16),
            v((GRID_ROWS, BLK), BF16), v((GRID_ROWS, CH), BF16), v((CH, GRID_PAD), BF16), v((CHUNK, GRID_PAD), BF16),
            v((COEFS, CH, BLK), BF16), v(hid, BF16), v(hid, BF16), v(hid, BF16), v(hid, BF16), v((HID, BLK), BF16), v((COEFS, CH, BLK), F32),
            v((GRID_PAD, BLK), BF16), v((GRID_PAD, BLK), BF16), v((GRID_PAD, BLK), BF16), v((GRID_PAD, BLK), BF16),
            v((TP, ROWS // 2, CH), F32), v((TP, ROWS // 2, CH), F32), v((TP, peers, EIGHTH, CH), F32), v((TP, EIGHTH, CH), F32),
            v((TP, zs, TILE, CH), F32), v((TP, TILE, CH), F32), v((TP, peers, TILE, CH), F32), v((TILE, CH), BF16),
            v((NZ * TILE, CH), BF16), v((ROWS, CH), BF16),
            dma((BLOCKS, peers, 2)), dma((BLOCKS, peers, 2)), dma((peers, 3)), dma((peers, 3)), dma((peers, 3)), dma((peers, 3)), dma((3,)), dma((3,)),
            dma((peers,)), dma((peers,)), dma((5,)),
            dma((BLOCKS, 2, peers)), dma((BLOCKS, 2, peers)), dma((BLOCKS, 2)),
            dma((TP,)), dma((TP,)), dma((TP, peers)), dma((TP, peers)), dma((TP, zs)), dma((TP, zs)), dma((TP, peers)), dma((TP, peers)),
            dma((zs,)), dma((zs,)), dma((zs,)), dma((zs,))],
        compiler_params=pltpu.CompilerParams(collective_id=0, has_side_effects=True, vmem_limit_bytes=VMEM_LIMIT), name="step",
    )(x, g, gain, up, gate, down, tog, frg)


def solution(mesh):
    act = P('dp', None, 'tp')
    in_specs = (act, P(None, 'tp'), P(None, None, 'tp'), P(None, 'tp'), P(None, 'tp', None), P(None, None), P(None, None), act)
    out_specs = (act, act, P(None, None, 'tp'), P(None, 'tp'), P(None, 'tp', None))

    def local_step(x, gain, up, gate, down, tog, frg, g):
        out, dx, d_up, d_gate, d_down = step_call(x.transpose(1, 2, 0), g.transpose(1, 2, 0), gain, up, gate, down, tog, frg.T)
        return out.transpose(2, 0, 1), dx.transpose(2, 0, 1), d_up, d_gate, d_down

    return jax.shard_map(local_step, mesh=mesh, in_specs=in_specs, out_specs=out_specs, check_vma=False)
```

```python
import jax
import jax.numpy as jnp
from jax import lax
from jax.experimental import pallas as pl
from jax.experimental.pallas import tpu as pltpu
from jax.sharding import PartitionSpec as P

NORM_EPS = 1e-5
COEFS = 9
CH = 128
HID = 512
SUB = 16
BLK = 256
GRID_ROWS = 576
GRID_PAD = 640
SLAB = 56
ROWS = 896
TILE = 16
EIGHTH = 112
NZ = 8
DEGS = 3
TP = 4
SLICE = 32
PTS = 36
VEC_SCALE = 1.0 / 1024
VMEM_LIMIT = 60 * 2**20
F32 = jnp.float32
BF16 = jnp.bfloat16


def iota(shape, axis):
    return lax.broadcasted_iota(jnp.int32, shape, axis)


def mm(a, b):
    return jnp.dot(a, b, preferred_element_type=F32)


def mm_nt(a, b):
    return lax.dot_general(a, b, (((1,), (1,)), ((), ())), preferred_element_type=F32)


def one_hot(shape, row_div, col_div):
    return jnp.where(iota(shape, 0) // row_div == iota(shape, 1) // col_div, 1.0, 0.0).astype(BF16)


def spread(table, rows, row_div, cols, col_div):
    left = mm(one_hot((rows, CH), row_div, 1), table).astype(BF16)
    full = mm(left, one_hot((CH, cols), 1, col_div))
    same = iota((rows, cols), 0) % SUB == iota((rows, cols), 1) % SUB
    return jnp.where(same, full, 0.0)


def degree_of(coef):
    return jnp.where(coef >= 4, 2, jnp.where(coef >= 1, 1, 0))


MESH = pl.DeviceIdType.MESH


def places():
    dp = lax.axis_index("dp")
    return lax.axis_index("tp"), dp // NZ, (dp // 2) % TP, dp % 2


def dp_index(z, y, core):
    return (z * TP + y) * 2 + core


def remote(src, dst, send_sem, recv_sem, peer):
    return pltpu.make_async_remote_copy(src_ref=src, dst_ref=dst, send_sem=send_sem, recv_sem=recv_sem,
                                        device_id=peer, device_id_type=MESH)


def part(i, size):
    return pl.ds(pl.multiple_of(i * size, size), size)


def start(copies):
    for c in copies:
        c.start()


def arrive(copies):
    for c in copies:
        c.wait_recv()


CHUNK = 144
GROUPS = HID // SUB
BLOCKS = 2


def step_kernel(x_loc, g_loc, gain_loc, up_loc, gate_loc, down_loc, tog_ref, frg_ref,
                out_loc, dx_loc, d_up, d_gate, d_down,
                x_all, g_all, gain_x, up_all, gate_all, down_all, out_all, dx_all, wg, pad_s, gain_b,
                wup_t, wgate_t, wdown_t, kg, kf, kft, kgt, n_s, y_s, dm_s, m_s, dy_s, da_s, dn_s, sb0, sb1, db0, db1,
                r1, a1, r2, a2, r3, a3, r4, fin, r5, r7,
                act_send, act_recv, wx_send, wx_recv, wy_send, wy_recv, wc_send, wc_recv, gain_send, gain_recv, loc_sem,
                o_send, o_recv, oloc_sem, s1, q1, s2, q2, s3, q3, s4, q4, s5, q5, s6, q6):
    me, z, y, core = places()
    atoms = x_all.shape[2]
    pair = {"dp": dp_index(z, y, 1 - core)}
    x_dist = list(range(1, TP))
    x_peers = [{"tp": lax.rem(me + d, TP)} for d in x_dist]
    y_peers = [{"dp": dp_index(z, lax.rem(y + d, TP), core)} for d in x_dist]
    z_peers = [{"dp": dp_index(lax.rem(z + d, NZ), y, core)} for d in range(1, NZ)]
    group = [(dy, dc) for dc in range(2) for dy in range(TP) if dy + dc > 0]
    yc_peers = [{"dp": dp_index(z, lax.rem(y + dy, TP), lax.rem(core + dc, 2))} for dy, dc in group]
    barrier = pltpu.get_barrier_semaphore()
    meeting = x_peers + z_peers + yc_peers
    for peer in meeting:
        pl.semaphore_signal(barrier, inc=1, device_id=peer, device_id_type=MESH)
    pl.semaphore_wait(barrier, len(meeting))

    eighth = part(core * TP + y, TILE)
    mine = part(me, CH)
    pieces = [(up_loc.at[:, eighth, :], up_all.at[:, eighth, mine]),
              (gate_loc.at[eighth, :], gate_all.at[eighth, mine]),
              (down_loc.at[:, eighth, :], down_all.at[:, me, eighth, :])]
    wx = [remote(src, dst, wx_send.at[d, i], wx_recv.at[d, i], peer)
          for d, peer in enumerate(x_peers) for i, (src, dst) in enumerate(pieces)]
    gx = [remote(gain_loc, gain_x.at[me], gain_send.at[d], gain_recv.at[d], peer) for d, peer in enumerate(x_peers)]
    start(wx + gx)
    acts = []
    for b in range(BLOCKS):
        acts.append([])
        for d, peer in enumerate(x_peers):
            tgt = lax.rem(me + d + 1, TP)
            cols = part(tgt * BLOCKS + b, BLK)
            for i, (src, dst) in enumerate(((x_loc, x_all), (g_loc, g_all))):
                acts[b].append(remote(src.at[:, :, cols], dst.at[:, part(me, SLICE), part(b, BLK)], act_send.at[b, d, i], act_recv.at[b, d, i], peer))
    start(acts[0][0::2])
    local = [pltpu.make_async_copy(src, dst, loc_sem.at[i]) for i, (src, dst) in enumerate(
        pieces + [(x_loc.at[:, :, part(me, atoms)], x_all.at[:, part(me, SLICE), :]), (g_loc.at[:, :, part(me, atoms)], g_all.at[:, part(me, SLICE), :])])]
    start(local)

    pad_s[...] = jnp.zeros(pad_s.shape, F32)
    pad_s[0, 0:COEFS, 0:PTS] = tog_ref[...]
    pad_s[1, 0:COEFS - 1, 0:PTS] = frg_ref[...]
    tog, tog_t = pad_s[0].astype(BF16), pad_s[0].T.astype(BF16)
    frg_t, frg = pad_s[1].astype(BF16), pad_s[1].T.astype(BF16)
    kg[...] = (0.5 * spread(tog_t, GRID_ROWS, SUB, BLK, SUB)).astype(BF16)
    kf[...] = (0.5 * spread(frg, GRID_ROWS, SUB, CH, SUB)).astype(BF16)
    kft[...] = spread(frg_t, CH, SUB, GRID_PAD, SUB).astype(BF16)
    kgt[...] = spread(tog, CHUNK, SUB, GRID_PAD, SUB).astype(BF16)
    for buf in (sb0, sb1, db0, db1):
        buf[GRID_ROWS:GRID_PAD, :] = jnp.zeros((GRID_PAD - GRID_ROWS, BLK), BF16)
    wg[...] = jnp.zeros(wg.shape, F32)
    gain_x[me] = gain_loc[...]
    for c in local:
        c.wait()
    arrive(wx)
    wholes = [lambda rows: up_all.at[:, rows, :], lambda rows: gate_all.at[rows, :], lambda rows: down_all.at[:, :, rows, :]]
    wy = [remote(whole(eighth), whole(eighth), wy_send.at[d, i], wy_recv.at[d, i], peer)
          for d, peer in enumerate(y_peers) for i, whole in enumerate(wholes)]
    start(wy)
    start(acts[0][1::2])
    arrive(gx)
    for t in range(TP):
        pad_s[2, t * NZ:t * NZ + DEGS, 0:SLICE] = gain_x[t]
    cols = pad_s[2].T
    for t in range(TP):
        for degree in range(DEGS):
            col = t * NZ + degree
            gain_b[degree, t * SLICE:(t + 1) * SLICE, :] = jnp.broadcast_to(cols[0:SLICE, col:col + 1], (SLICE, BLK))
    arrive(wy)
    side = part(core, CH // 2)
    wc = [remote(whole(side), whole(side), wc_send.at[i], wc_recv.at[i], pair) for i, whole in enumerate(wholes)]
    start(wc)
    arrive(wc)
    for degree in range(DEGS):
        wup_t[degree] = up_all[degree].T
        wdown_t[degree] = down_all[degree].reshape(HID, CH).T
    wgate_t[...] = gate_all[...].T

    def gain_of(coef):
        return gain_b[0 if coef == 0 else (1 if coef < TP else 2)]

    def norm(lanes):
        x0 = x_all[0, :, lanes].astype(F32)
        mean_s = jnp.sum(x0, axis=0, keepdims=True) * (1.0 / CH)
        cen = x0 - mean_s
        inv_s = lax.rsqrt(jnp.sum(cen * cen, axis=0, keepdims=True) * (1.0 / CH) + NORM_EPS)
        n_s[0] = ((cen * inv_s) * gain_of(0)).astype(BF16)
        acc = jnp.zeros((CH, BLK), F32)
        for coef in range(1, COEFS):
            xk = x_all[coef, :, lanes].astype(F32)
            acc = acc + xk * xk
        inv_v = lax.rsqrt(jnp.sum(acc, axis=0, keepdims=True) * VEC_SCALE + NORM_EPS)
        for coef in range(1, COEFS):
            xk = x_all[coef, :, lanes].astype(F32)
            n_s[coef] = ((xk * inv_v) * gain_of(coef)).astype(BF16)
        return mean_s, inv_s, inv_v

    def up(lanes):
        def up_step(coef, carry):
            degree = degree_of(coef)
            y_s[coef] = mm(wup_t[degree], n_s[coef]).astype(BF16)
            dm_s[coef] = mm(down_all[degree].reshape(HID, CH), g_all[coef, :, lanes]).astype(BF16)
            return carry
        lax.fori_loop(0, COEFS, up_step, 0)

        def gate_step(i, carry):
            rows = part(i, CH)
            half = (0.5 * mm(wgate_t[rows, :], n_s[0])).astype(BF16).astype(F32)
            th = jnp.tanh(half)
            plus = 1.0 + th
            val = half * plus
            m_s[0, rows, :] = val.astype(BF16)
            slope = 0.5 * (plus + val * (1.0 - th))
            da_s[rows, :] = (dm_s[0, rows, :].astype(F32) * slope).astype(BF16)
            return carry
        lax.fori_loop(0, TP, gate_step, 0)

    def expand(j, s_buf, du_buf):
        rows = part(j, SUB)
        yj = y_s[:, rows, :].reshape(CHUNK, BLK)
        dzj = dm_s[1:, rows, :].reshape(CH, BLK)
        for r0 in range(0, GRID_ROWS, CHUNK):
            half = mm(kg[r0:r0 + CHUNK, 0:CHUNK], yj).astype(BF16).astype(F32)
            dval = mm(kf[r0:r0 + CHUNK, :], dzj).astype(BF16).astype(F32)
            th = jnp.tanh(half)
            plus = 1.0 + th
            val = half * plus
            s_buf[r0:r0 + CHUNK, :] = val.astype(BF16)
            du_buf[r0:r0 + CHUNK, :] = (dval * (plus + val * (1.0 - th))).astype(BF16)

    def contract(j, s_buf, du_buf):
        rows = part(j, SUB)
        m_s[1:, rows, :] = mm(kft[...], s_buf[...]).astype(BF16).reshape(COEFS - 1, SUB, BLK)
        dy_s[:, rows, :] = mm(kgt[...], du_buf[...]).astype(BF16).reshape(COEFS, SUB, BLK)

    def grid_step(i, carry):
        expand(2 * i + 1, sb1, db1)
        contract(2 * i, sb0, db0)
        expand(jnp.minimum(2 * i + 2, GROUPS - 1), sb0, db0)
        contract(2 * i + 1, sb1, db1)
        return carry

    def weight_grads(t, lanes):
        rows = part(t, CH)

        def coef_step(coef, carry):
            base = degree_of(coef) * CH
            wg[t, part(degree_of(coef), CH), :] += mm_nt(n_s[coef], dy_s[coef, rows, :])
            wg[t, part(degree_of(coef) + TP, CH), :] += mm_nt(m_s[coef, rows, :], g_all[coef, :, lanes])
            return carry
        lax.fori_loop(0, COEFS, coef_step, 0)
        wg[t, part(DEGS, CH), :] += mm_nt(n_s[0], da_s[rows, :])

    def down(lanes):
        def down_step(coef, carry):
            degree = degree_of(coef)
            xk = x_all[coef, :, lanes].astype(F32)
            out_all[coef, :, lanes] = (xk + mm(wdown_t[degree], m_s[coef])).astype(BF16)
            dn_s[coef] = mm(up_all[degree], dy_s[coef])
            return carry
        lax.fori_loop(0, COEFS, down_step, 0)
        dn_s[0] += mm(gate_all[...], da_s[...])

    def norm_back(lanes, mean_s, inv_s, inv_v):
        hat = (x_all[0, :, lanes].astype(F32) - mean_s) * inv_s
        dh = dn_s[0].astype(BF16).astype(F32) * gain_of(0)
        m1 = jnp.sum(dh, axis=0, keepdims=True) * (1.0 / CH)
        m2 = jnp.sum(dh * hat, axis=0, keepdims=True) * (1.0 / CH)
        dx_all[0, :, lanes] = (inv_s * (dh - m1 - hat * m2) + g_all[0, :, lanes].astype(F32)).astype(BF16)
        acc = jnp.zeros((CH, BLK), F32)
        for coef in range(1, COEFS):
            xk = x_all[coef, :, lanes].astype(F32)
            acc = acc + (dn_s[coef].astype(BF16).astype(F32) * gain_of(coef)) * (xk * inv_v)
        mv = jnp.sum(acc, axis=0, keepdims=True) * VEC_SCALE
        for coef in range(1, COEFS):
            xk = x_all[coef, :, lanes].astype(F32)
            dh = dn_s[coef].astype(BF16).astype(F32) * gain_of(coef)
            dx_all[coef, :, lanes] = (inv_v * (dh - (xk * inv_v) * mv) + g_all[coef, :, lanes].astype(F32)).astype(BF16)

    outs = ((out_all, out_loc), (dx_all, dx_loc))

    def out_copies(b, i, third):
        src, dst = outs[i]
        coefs = slice(third * DEGS, (third + 1) * DEGS)
        cols = part(me * BLOCKS + b, BLK)
        return [remote(src.at[coefs, part(lax.rem(me + d, TP), SLICE), part(b, BLK)], dst.at[coefs, :, cols],
                       o_send.at[b, i, third, d - 1], o_recv.at[b, i, third, d - 1], x_peers[d - 1]) for d in x_dist]

    def out_local(b, i):
        src, dst = outs[i]
        return pltpu.make_async_copy(src.at[:, part(me, SLICE), part(b, BLK)], dst.at[:, :, part(me * BLOCKS + b, BLK)], oloc_sem.at[b, i])

    sent = [[[out_copies(b, i, third) for third in range(DEGS)] for i in range(2)] for b in range(BLOCKS)]
    kept = [[out_local(b, i) for i in range(2)] for b in range(BLOCKS)]

    def send_out(b, i):
        for third in range(DEGS):
            start(sent[b][i][third])
        kept[b][i].start()

    half_rows = ROWS // 2
    c1 = [remote(wg.at[t, part(1 - core, half_rows), :], r1.at[t], s1.at[t], q1.at[t], pair) for t in range(TP)]
    c2 = [[remote(a1.at[t, part(lax.rem(y + d, TP), EIGHTH), :], r2.at[t, d - 1], s2.at[t, d - 1], q2.at[t, d - 1], y_peers[d - 1]) for d in x_dist]
          for t in range(TP)]
    c3 = [[remote(a2.at[t, part(lax.rem(lax.rem(z + d, NZ), NZ - 1), TILE), :], r3.at[t, d - 1], s3.at[t, d - 1], q3.at[t, d - 1], z_peers[d - 1])
           for d in range(1, NZ)] for t in range(TP)]
    c4 = [[remote(a3.at[t], r4.at[t, d - 1], s4.at[t, d - 1], q4.at[t, d - 1], x_peers[d - 1]) for d in x_dist] for t in range(TP)]
    c5 = [remote(fin, r5.at[part(z, TILE), :], s5.at[d - 1], q5.at[d - 1], z_peers[d - 1]) for d in range(1, NZ)]

    def sum_core(t):
        arrive([c1[t]])
        a1[t] = wg[t, part(core, half_rows), :] + r1[t]
        start(c2[t])

    def sum_y(t):
        arrive(c2[t])
        a2[t] = (a1[t, part(y, EIGHTH), :] + r2[t, 0]) + (r2[t, 1] + r2[t, 2])
        start(c3[t])

    def sum_z(t):
        arrive(c3[t])
        own = a2[t, part(lax.rem(z, NZ - 1), TILE), :]
        a3[t] = ((own + r3[t, 0]) + (r3[t, 1] + r3[t, 2])) + ((r3[t, 3] + r3[t, 4]) + (r3[t, 5] + r3[t, 6]))
        start(c4[t])

    def sum_x(t):
        arrive(c4[t])

        @pl.when(me == t)
        def _():
            fin[...] = ((a3[t] + r4[t, 0]) + (r4[t, 1] + r4[t, 2])).astype(BF16)
            start(c5)
            r5[part(z, TILE), :] = fin[...]

    first, second = pl.ds(0, BLK), pl.ds(BLK, BLK)
    for c in acts[0]:
        c.wait_send()
    start(acts[1])
    arrive(acts[0])
    stats = norm(first)
    up(first)
    expand(0, sb0, db0)
    lax.fori_loop(0, GROUPS // 2, grid_step, 0)
    down(first)
    send_out(0, 0)
    norm_back(first, *stats)
    send_out(0, 1)

    def grads_step(t, carry):
        weight_grads(t, first)
        return carry
    lax.fori_loop(0, TP, grads_step, 0)

    arrive(acts[1])
    stats = norm(second)
    up(second)
    expand(0, sb0, db0)
    per = GROUPS // 2 // TP
    for t in range(TP):
        lax.fori_loop(t * per, (t + 1) * per, grid_step, 0)
        if t > 0:
            sum_core(t - 1)
        if t == TP - 1:
            sum_y(0)
        weight_grads(t, second)
        start([c1[t]])
    sum_y(1)
    down(second)
    sum_core(TP - 1)
    start(sent[1][0][0])
    kept[1][0].start()
    norm_back(second, *stats)
    kept[1][1].start()
    sum_y(2)
    sum_z(0)
    start(sent[1][0][1])
    sum_z(1)
    sum_y(3)
    start(sent[1][0][2])
    start(sent[1][1][0])
    sum_z(2)
    sum_x(0)
    sum_x(1)
    sum_z(3)
    start(sent[1][1][1])
    sum_x(2)
    sum_x(3)
    start(sent[1][1][2])
    arrive(c5)
    slot = part(core * TP + y, EIGHTH)
    c6 = [remote(r5.at[0:EIGHTH, :], r7.at[slot, :], s6.at[i], q6.at[i], yc_peers[i]) for i in range(len(group))]
    start(c6)
    r7[slot, :] = r5[0:EIGHTH, :]
    arrive(c6)
    for degree in range(DEGS):
        d_up[degree] = r7[degree * CH:(degree + 1) * CH, :]
        d_down[degree] = r7[(TP + degree) * CH:(TP + degree + 1) * CH, :]
    d_gate[...] = r7[DEGS * CH:TP * CH, :]
    finished = wx + gx + wy + wc + c1 + c5 + c6
    for group_of in [acts[1]] + c2 + c3 + c4:
        finished = finished + group_of
    for b in range(BLOCKS):
        for i in range(2):
            kept[b][i].wait()
            for third in range(DEGS):
                arrive(sent[b][i][third])
                finished = finished + sent[b][i][third]
    for c in finished:
        c.wait_send()


def step_call(x, g, gain, up, gate, down, tog, frg):
    vm = pl.BlockSpec(memory_space=pltpu.VMEM)
    hbm = pl.BlockSpec(memory_space=pl.ANY)
    dma = pltpu.SemaphoreType.DMA
    v = pltpu.VMEM
    sds = jax.ShapeDtypeStruct
    atoms = x.shape[2] // TP
    act = (COEFS, CH, atoms)
    hid = (COEFS, HID, BLK)
    peers = TP - 1
    zs = NZ - 1
    return pl.pallas_call(
        step_kernel,
        out_shape=[sds(x.shape, BF16), sds(x.shape, BF16), sds((DEGS, CH, CH), BF16), sds((CH, CH), BF16), sds((DEGS, CH, CH), BF16)],
        in_specs=[hbm] * 2 + [vm] * 6, out_specs=[hbm] * 2 + [vm] * 3,
        scratch_shapes=[
            v(act, BF16), v(act, BF16), v((TP, DEGS, SLICE), F32), v((DEGS, CH, HID), BF16), v((CH, HID), BF16), v((DEGS, TP, CH, CH), BF16),
            v(act, BF16), v(act, BF16), v((TP, ROWS, CH), F32), v((DEGS, CH, CH), F32), v((DEGS, CH, BLK), F32),
            v((DEGS, HID, CH), BF16), v((HID, CH), BF16), v((DEGS, CH, HID), BF16),
            v((GRID_ROWS, BLK), BF16), v((GRID_ROWS, CH), BF16), v((CH, GRID_PAD), BF16), v((CHUNK, GRID_PAD), BF16),
            v((COEFS, CH, BLK), BF16), v(hid, BF16), v(hid, BF16), v(hid, BF16), v(hid, BF16), v((HID, BLK), BF16), v((COEFS, CH, BLK), F32),
            v((GRID_PAD, BLK), BF16), v((GRID_PAD, BLK), BF16), v((GRID_PAD, BLK), BF16), v((GRID_PAD, BLK), BF16),
            v((TP, ROWS // 2, CH), F32), v((TP, ROWS // 2, CH), F32), v((TP, peers, EIGHTH, CH), F32), v((TP, EIGHTH, CH), F32),
            v((TP, zs, TILE, CH), F32), v((TP, TILE, CH), F32), v((TP, peers, TILE, CH), F32), v((TILE, CH), BF16),
            v((NZ * TILE, CH), BF16), v((ROWS, CH), BF16),
            dma((BLOCKS, peers, 2)), dma((BLOCKS, peers, 2)), dma((peers, 3)), dma((peers, 3)), dma((peers, 3)), dma((peers, 3)), dma((3,)), dma((3,)),
            dma((peers,)), dma((peers,)), dma((5,)),
            dma((BLOCKS, 2, DEGS, peers)), dma((BLOCKS, 2, DEGS, peers)), dma((BLOCKS, 2)),
            dma((TP,)), dma((TP,)), dma((TP, peers)), dma((TP, peers)), dma((TP, zs)), dma((TP, zs)), dma((TP, peers)), dma((TP, peers)),
            dma((zs,)), dma((zs,)), dma((zs,)), dma((zs,))],
        compiler_params=pltpu.CompilerParams(collective_id=0, has_side_effects=True, vmem_limit_bytes=VMEM_LIMIT), name="step",
    )(x, g, gain, up, gate, down, tog, frg)


def store_kernel(*refs):
    count = (len(refs) - 2) // 3
    sources, results, bufs = refs[:count], refs[count:2 * count], refs[2 * count:3 * count]
    in_sem, out_sem = refs[3 * count:]
    loads = [pltpu.make_async_copy(src, buf, in_sem.at[i]) for i, (src, buf) in enumerate(zip(sources, bufs))]
    stores = [pltpu.make_async_copy(buf, dst, out_sem.at[i]) for i, (buf, dst) in enumerate(zip(bufs, results))]
    start(loads)
    for load, store in zip(loads, stores):
        load.wait()
        store.start()
    for store in stores:
        store.wait()


def store_call(*arrays):
    hbm = pl.BlockSpec(memory_space=pl.ANY)
    count = len(arrays)
    return pl.pallas_call(
        store_kernel, out_shape=[jax.ShapeDtypeStruct(a.shape, a.dtype) for a in arrays], in_specs=[hbm] * count, out_specs=[hbm] * count,
        scratch_shapes=[pltpu.VMEM(a.shape, a.dtype) for a in arrays] + [pltpu.SemaphoreType.DMA((count,))] * 2,
        compiler_params=pltpu.CompilerParams(vmem_limit_bytes=VMEM_LIMIT), name="store",
    )(*arrays)


def solution(mesh):
    act = P('dp', None, 'tp')
    in_specs = (act, P(None, 'tp'), P(None, None, 'tp'), P(None, 'tp'), P(None, 'tp', None), P(None, None), P(None, None), act)
    out_specs = (act, act, P(None, None, 'tp'), P(None, 'tp'), P(None, 'tp', None))

    def local_step(x, gain, up, gate, down, tog, frg, g):
        out, dx, d_up, d_gate, d_down = store_call(*step_call(x.transpose(1, 2, 0), g.transpose(1, 2, 0), gain, up, gate, down, tog, frg.T))
        return out.transpose(2, 0, 1), dx.transpose(2, 0, 1), d_up, d_gate, d_down

    return jax.shard_map(local_step, mesh=mesh, in_specs=in_specs, out_specs=out_specs, check_vma=False)
```

```python
import jax
import jax.numpy as jnp
from jax import lax
from jax.experimental import pallas as pl
from jax.experimental.pallas import tpu as pltpu
from jax.sharding import PartitionSpec as P

NORM_EPS = 1e-5
COEFS = 9
CH = 128
HID = 512
SUB = 16
BLK = 256
GRID_ROWS = 576
GRID_PAD = 640
SLAB = 56
ROWS = 896
TILE = 16
EIGHTH = 112
NZ = 8
DEGS = 3
TP = 4
SLICE = 32
PTS = 36
VEC_SCALE = 1.0 / 1024
VMEM_LIMIT = 60 * 2**20
F32 = jnp.float32
BF16 = jnp.bfloat16


def iota(shape, axis):
    return lax.broadcasted_iota(jnp.int32, shape, axis)


def mm(a, b):
    return jnp.dot(a, b, preferred_element_type=F32)


def mm_nt(a, b):
    return lax.dot_general(a, b, (((1,), (1,)), ((), ())), preferred_element_type=F32)


def one_hot(shape, row_div, col_div):
    return jnp.where(iota(shape, 0) // row_div == iota(shape, 1) // col_div, 1.0, 0.0).astype(BF16)


def point_of(row):
    main = row < HID
    point = jnp.where(main, (row % BLK) // NZ, SLICE + (row % SLICE) // NZ)
    half = jnp.where(main, row // BLK, (row % 64) // SLICE)
    return point, half


def spread_out(table_t, cols):
    point, half = point_of(iota((GRID_ROWS, CH), 0))
    left = mm(jnp.where(point == iota((GRID_ROWS, CH), 1), 1.0, 0.0).astype(BF16), table_t).astype(BF16)
    full = mm(left, one_hot((CH, cols), 1, SUB))
    row = iota((GRID_ROWS, cols), 0)
    same = point_of(row)[1] * NZ + row % NZ == iota((GRID_ROWS, cols), 1) % SUB
    return jnp.where(same, 0.5 * full, 0.0).astype(BF16)


def spread_back(table, rows):
    left = mm(one_hot((rows, CH), NZ, 1), table).astype(BF16)
    full = mm(left, one_hot((CH, BLK), 1, NZ))
    return jnp.where(iota((rows, BLK), 0) % NZ == iota((rows, BLK), 1) % NZ, full, 0.0).astype(BF16)


def spread_last(table, rows):
    row, col = iota((2 * rows, CH), 0), iota((2 * rows, CH), 1)
    r2, c2 = iota((2 * rows, CH), 0), iota((2 * rows, CH), 1)
    left = mm(jnp.where((r2 % rows) // NZ == c2, 1.0, 0.0).astype(BF16), table).astype(BF16)
    pick = jnp.where(iota((CH, CH), 0) == SLICE + (iota((CH, CH), 1) % SLICE) // NZ, 1.0, 0.0).astype(BF16)
    full = mm(left, pick)
    same = (row % NZ == col % NZ) & (row // rows == col // SLICE)
    return jnp.where(same, full, 0.0).astype(BF16)


def degree_of(coef):
    return jnp.where(coef >= 4, 2, jnp.where(coef >= 1, 1, 0))


MESH = pl.DeviceIdType.MESH


def places():
    dp = lax.axis_index("dp")
    return lax.axis_index("tp"), dp // NZ, (dp // 2) % TP, dp % 2


def dp_index(z, y, core):
    return (z * TP + y) * 2 + core


def remote(src, dst, send_sem, recv_sem, peer):
    return pltpu.make_async_remote_copy(src_ref=src, dst_ref=dst, send_sem=send_sem, recv_sem=recv_sem,
                                        device_id=peer, device_id_type=MESH)


def part(i, size):
    return pl.ds(pl.multiple_of(i * size, size), size)


def start(copies):
    for c in copies:
        c.start()


def arrive(copies):
    for c in copies:
        c.wait_recv()


CHUNK = 288
KROWS = 144
ZROWS = 64
YROWS = 72
GROUPS = HID // SUB
BLOCKS = 2


def step_kernel(x_loc, g_loc, gain_loc, up_loc, gate_loc, down_loc, tog_ref, frg_ref,
                out_loc, dx_loc, d_up, d_gate, d_down,
                x_all, g_all, gain_x, up_all, gate_all, down_all, out_all, dx_all, wg, pad_s, gain_b,
                wup_t, wgate_t, wdown_t, kg, kf, kft, kgt, kftl, kgtl, n_s, y_s, dm_s, m_s, dy_s, da_s, dn0_s, dn1_s, sb0, sb1, db0, db1,
                r1, a1, r2, a2, r3, a3, r4, fin, r5, r7, gain_v, tog_v, frg_v, small_sem,
                act_send, act_recv, wx_send, wx_recv, wy_send, wy_recv, wc_send, wc_recv, gain_send, gain_recv, loc_sem,
                o_send, o_recv, oloc_sem, s1, q1, s2, q2, s3, q3, s4, q4, s5, q5, s6, q6):
    me, z, y, core = places()
    atoms = x_all.shape[2]
    small = [pltpu.make_async_copy(src, dst, small_sem.at[i]) for i, (src, dst) in enumerate(((gain_loc, gain_v), (tog_ref, tog_v), (frg_ref, frg_v)))]
    start(small)
    pair = {"dp": dp_index(z, y, 1 - core)}
    x_dist = list(range(1, TP))
    x_peers = [{"tp": lax.rem(me + d, TP)} for d in x_dist]
    y_peers = [{"dp": dp_index(z, lax.rem(y + d, TP), core)} for d in x_dist]
    z_peers = [{"dp": dp_index(lax.rem(z + d, NZ), y, core)} for d in range(1, NZ)]
    group = [(dy, dc) for dc in range(2) for dy in range(TP) if dy + dc > 0]
    yc_peers = [{"dp": dp_index(z, lax.rem(y + dy, TP), lax.rem(core + dc, 2))} for dy, dc in group]
    barrier = pltpu.get_barrier_semaphore()
    meeting = x_peers + z_peers + yc_peers
    for peer in meeting:
        pl.semaphore_signal(barrier, inc=1, device_id=peer, device_id_type=MESH)
    pl.semaphore_wait(barrier, len(meeting))

    eighth = part(core * TP + y, TILE)
    mine = part(me, CH)
    pieces = [(up_loc.at[:, eighth, :], up_all.at[:, eighth, mine]),
              (gate_loc.at[eighth, :], gate_all.at[eighth, mine]),
              (down_loc.at[:, eighth, :], down_all.at[:, me, eighth, :])]
    wx = [remote(src, dst, wx_send.at[d, i], wx_recv.at[d, i], peer)
          for d, peer in enumerate(x_peers) for i, (src, dst) in enumerate(pieces)]
    gx = [remote(gain_loc, gain_x.at[me], gain_send.at[d], gain_recv.at[d], peer) for d, peer in enumerate(x_peers)]
    start(wx + gx)
    acts = []
    for b in range(BLOCKS):
        acts.append([])
        for d, peer in enumerate(x_peers):
            tgt = lax.rem(me + d + 1, TP)
            cols = part(tgt * BLOCKS + b, BLK)
            for i, (src, dst) in enumerate(((x_loc, x_all), (g_loc, g_all))):
                acts[b].append(remote(src.at[:, :, cols], dst.at[:, part(me, SLICE), part(b, BLK)], act_send.at[b, d, i], act_recv.at[b, d, i], peer))
    start(acts[0][0::2])
    local = [pltpu.make_async_copy(src, dst, loc_sem.at[i]) for i, (src, dst) in enumerate(
        pieces + [(x_loc.at[:, :, part(me, atoms)], x_all.at[:, part(me, SLICE), :]), (g_loc.at[:, :, part(me, atoms)], g_all.at[:, part(me, SLICE), :])])]
    start(local)

    pad_s[...] = jnp.zeros(pad_s.shape, F32)
    for c in small:
        c.wait()
    pad_s[0, 0:COEFS, 0:PTS] = tog_v[...]
    pad_s[1, 0:COEFS - 1, 0:PTS] = frg_v[...]
    tog, tog_t = pad_s[0].astype(BF16), pad_s[0].T.astype(BF16)
    frg_t, frg = pad_s[1].astype(BF16), pad_s[1].T.astype(BF16)
    kg[...] = spread_out(tog_t, BLK)
    kf[...] = spread_out(frg, CH)
    kft[...] = spread_back(frg_t, ZROWS)
    kgt[...] = spread_back(tog, YROWS)
    kftl[...] = spread_last(frg_t, ZROWS)
    kgtl[...] = spread_last(tog, YROWS)
    for buf in (sb0, sb1, db0, db1):
        buf[GRID_ROWS:GRID_PAD, :] = jnp.zeros((GRID_PAD - GRID_ROWS, BLK), BF16)
    wg[...] = jnp.zeros(wg.shape, F32)
    gain_x[me] = gain_v[...]
    for c in local:
        c.wait()
    arrive(wx)
    wholes = [lambda rows: up_all.at[:, rows, :], lambda rows: gate_all.at[rows, :], lambda rows: down_all.at[:, :, rows, :]]
    wy = [remote(whole(eighth), whole(eighth), wy_send.at[d, i], wy_recv.at[d, i], peer)
          for d, peer in enumerate(y_peers) for i, whole in enumerate(wholes)]
    start(wy)
    start(acts[0][1::2])
    arrive(gx)
    for t in range(TP):
        pad_s[2, t * NZ:t * NZ + DEGS, 0:SLICE] = gain_x[t]
    cols = pad_s[2].T
    for t in range(TP):
        for degree in range(DEGS):
            col = t * NZ + degree
            gain_b[degree, t * SLICE:(t + 1) * SLICE, :] = jnp.broadcast_to(cols[0:SLICE, col:col + 1], (SLICE, BLK))
    arrive(wy)
    side = part(core, CH // 2)
    wc = [remote(whole(side), whole(side), wc_send.at[i], wc_recv.at[i], pair) for i, whole in enumerate(wholes)]
    start(wc)
    arrive(wc)
    for degree in range(DEGS):
        wup_t[degree] = up_all[degree].T
        wdown_t[degree] = down_all[degree].reshape(HID, CH).T
    wgate_t[...] = gate_all[...].T

    def gain_of(coef):
        return gain_b[0 if coef == 0 else (1 if coef < TP else 2)]

    def norm(lanes):
        x0 = x_all[0, :, lanes].astype(F32)
        mean_s = jnp.sum(x0, axis=0, keepdims=True) * (1.0 / CH)
        cen = x0 - mean_s
        inv_s = lax.rsqrt(jnp.sum(cen * cen, axis=0, keepdims=True) * (1.0 / CH) + NORM_EPS)
        n_s[0] = ((cen * inv_s) * gain_of(0)).astype(BF16)
        acc = jnp.zeros((CH, BLK), F32)
        for coef in range(1, COEFS):
            xk = x_all[coef, :, lanes].astype(F32)
            acc = acc + xk * xk
        inv_v = lax.rsqrt(jnp.sum(acc, axis=0, keepdims=True) * VEC_SCALE + NORM_EPS)
        for coef in range(1, COEFS):
            xk = x_all[coef, :, lanes].astype(F32)
            n_s[coef] = ((xk * inv_v) * gain_of(coef)).astype(BF16)
        return mean_s, inv_s, inv_v

    def up(lanes):
        def up_step(i, carry):
            for k in range(DEGS):
                coef = i * DEGS + k
                degree = degree_of(coef)
                y_s[coef] = mm(wup_t[degree], n_s[coef]).astype(BF16)
                dm_s[coef] = mm(down_all[degree].reshape(HID, CH), g_all[coef, :, lanes]).astype(BF16)
            return carry
        lax.fori_loop(0, DEGS, up_step, 0)

        def gate_step(i, carry):
            rows = part(i, CH)
            half = (0.5 * mm(wgate_t[rows, :], n_s[0])).astype(BF16).astype(F32)
            th = jnp.tanh(half)
            plus = 1.0 + th
            val = half * plus
            m_s[0, rows, :] = val.astype(BF16)
            slope = 0.5 * (plus + val * (1.0 - th))
            da_s[rows, :] = (dm_s[0, rows, :].astype(F32) * slope).astype(BF16)
            return carry
        lax.fori_loop(0, TP, gate_step, 0)

    def expand(j, s_buf, du_buf):
        rows = part(j, SUB)
        yj = y_s[:, rows, :].reshape(KROWS, BLK)
        dzj = dm_s[1:, rows, :].reshape(CH, BLK)
        for r0 in range(0, GRID_ROWS, CHUNK):
            half = mm(kg[r0:r0 + CHUNK, 0:KROWS], yj).astype(BF16).astype(F32)
            dval = mm(kf[r0:r0 + CHUNK, :], dzj).astype(BF16).astype(F32)
            th = jnp.tanh(half)
            plus = 1.0 + th
            val = half * plus
            s_buf[r0:r0 + CHUNK, :] = val.astype(BF16)
            du_buf[r0:r0 + CHUNK, :] = (dval * (plus + val * (1.0 - th))).astype(BF16)

    def halves(back, last, buf, rows):
        low = mm(last[...], buf[HID:GRID_PAD, :])
        sums = [mm(back[...], buf[h * BLK:(h + 1) * BLK, :]) + low[h * rows:(h + 1) * rows, :] for h in range(2)]
        return jnp.concatenate([v.reshape(rows // NZ, NZ, BLK) for v in sums], axis=1).astype(BF16)

    def contract(j, s_buf, du_buf):
        rows = part(j, SUB)
        m_s[1:, rows, :] = halves(kft, kftl, s_buf, ZROWS)
        dy_s[:, rows, :] = halves(kgt, kgtl, du_buf, YROWS)

    def grid_step(i, carry):
        expand(2 * i + 1, sb1, db1)
        contract(2 * i, sb0, db0)
        expand(jnp.minimum(2 * i + 2, GROUPS - 1), sb0, db0)
        contract(2 * i + 1, sb1, db1)
        return carry

    def weight_grads(t, lanes):
        rows = part(t, CH)

        for degree in range(DEGS):
            coefs = range(degree * degree, (degree + 1) * (degree + 1))
            wg[t, degree * CH:(degree + 1) * CH, :] += sum(mm_nt(n_s[c], dy_s[c, rows, :]) for c in coefs)
            wg[t, (degree + TP) * CH:(degree + TP + 1) * CH, :] += sum(mm_nt(m_s[c, rows, :], g_all[c, :, lanes]) for c in coefs)
        wg[t, DEGS * CH:TP * CH, :] += mm_nt(n_s[0], da_s[rows, :])

    def down(lanes, dn_s):
        def down_step(i, carry):
            for k in range(DEGS):
                coef = i * DEGS + k
                degree = degree_of(coef)
                xk = x_all[coef, :, lanes].astype(F32)
                out_all[coef, :, lanes] = (xk + mm(wdown_t[degree], m_s[coef])).astype(BF16)
                dn_s[coef] = mm(up_all[degree], dy_s[coef])
            return carry
        lax.fori_loop(0, DEGS, down_step, 0)
        dn_s[0] += mm(gate_all[...], da_s[...])

    def norm_back(lanes, dn_s, mean_s, inv_s, inv_v):
        hat = (x_all[0, :, lanes].astype(F32) - mean_s) * inv_s
        dh = dn_s[0].astype(BF16).astype(F32) * gain_of(0)
        m1 = jnp.sum(dh, axis=0, keepdims=True) * (1.0 / CH)
        m2 = jnp.sum(dh * hat, axis=0, keepdims=True) * (1.0 / CH)
        dx_all[0, :, lanes] = (inv_s * (dh - m1 - hat * m2) + g_all[0, :, lanes].astype(F32)).astype(BF16)
        acc = jnp.zeros((CH, BLK), F32)
        for coef in range(1, COEFS):
            xk = x_all[coef, :, lanes].astype(F32)
            acc = acc + (dn_s[coef].astype(BF16).astype(F32) * gain_of(coef)) * (xk * inv_v)
        mv = jnp.sum(acc, axis=0, keepdims=True) * VEC_SCALE
        for coef in range(1, COEFS):
            xk = x_all[coef, :, lanes].astype(F32)
            dh = dn_s[coef].astype(BF16).astype(F32) * gain_of(coef)
            dx_all[coef, :, lanes] = (inv_v * (dh - (xk * inv_v) * mv) + g_all[coef, :, lanes].astype(F32)).astype(BF16)

    outs = ((out_all, out_loc), (dx_all, dx_loc))

    def out_copies(b, i, third):
        src, dst = outs[i]
        coefs = slice(third * DEGS, (third + 1) * DEGS)
        cols = part(me * BLOCKS + b, BLK)
        return [remote(src.at[coefs, part(lax.rem(me + d, TP), SLICE), part(b, BLK)], dst.at[coefs, :, cols],
                       o_send.at[b, i, third, d - 1], o_recv.at[b, i, third, d - 1], x_peers[d - 1]) for d in x_dist]

    def out_local(b, i):
        src, dst = outs[i]
        return pltpu.make_async_copy(src.at[:, part(me, SLICE), part(b, BLK)], dst.at[:, :, part(me * BLOCKS + b, BLK)], oloc_sem.at[b, i])

    sent = [[[out_copies(b, i, third) for third in range(DEGS)] for i in range(2)] for b in range(BLOCKS)]
    kept = [[out_local(b, i) for i in range(2)] for b in range(BLOCKS)]

    def send_out(b, i):
        for third in range(DEGS):
            start(sent[b][i][third])
        kept[b][i].start()

    half_rows = ROWS // 2
    c1 = [remote(wg.at[t, part(1 - core, half_rows), :], r1.at[t], s1.at[t], q1.at[t], pair) for t in range(TP)]
    c2 = [[remote(a1.at[t, part(lax.rem(y + d, TP), EIGHTH), :], r2.at[t, d - 1], s2.at[t, d - 1], q2.at[t, d - 1], y_peers[d - 1]) for d in x_dist]
          for t in range(TP)]
    c3 = [[remote(a2.at[t, part(lax.rem(lax.rem(z + d, NZ), NZ - 1), TILE), :], r3.at[t, d - 1], s3.at[t, d - 1], q3.at[t, d - 1], z_peers[d - 1])
           for d in range(1, NZ)] for t in range(TP)]
    c4 = [[remote(a3.at[t], r4.at[t, d - 1], s4.at[t, d - 1], q4.at[t, d - 1], x_peers[d - 1]) for d in x_dist] for t in range(TP)]
    c5 = [remote(fin, r5.at[part(z, TILE), :], s5.at[d - 1], q5.at[d - 1], z_peers[d - 1]) for d in range(1, NZ)]

    def sum_core(t):
        arrive([c1[t]])
        a1[t] = wg[t, part(core, half_rows), :] + r1[t]
        start(c2[t])

    def sum_y(t):
        arrive(c2[t])
        a2[t] = (a1[t, part(y, EIGHTH), :] + r2[t, 0]) + (r2[t, 1] + r2[t, 2])
        start(c3[t])

    def sum_z(t):
        arrive(c3[t])
        own = a2[t, part(lax.rem(z, NZ - 1), TILE), :]
        a3[t] = ((own + r3[t, 0]) + (r3[t, 1] + r3[t, 2])) + ((r3[t, 3] + r3[t, 4]) + (r3[t, 5] + r3[t, 6]))
        start(c4[t])

    def sum_x(t):
        arrive(c4[t])

        @pl.when(me == t)
        def _():
            fin[...] = ((a3[t] + r4[t, 0]) + (r4[t, 1] + r4[t, 2])).astype(BF16)
            start(c5)
            r5[part(z, TILE), :] = fin[...]

    first, second = pl.ds(0, BLK), pl.ds(BLK, BLK)
    for c in acts[0]:
        c.wait_send()
    start(acts[1])
    arrive(acts[0])
    stats0 = norm(first)
    up(first)
    expand(0, sb0, db0)
    lax.fori_loop(0, GROUPS // 2, grid_step, 0)
    down(first, dn0_s)
    send_out(0, 0)

    def grads_step(t, carry):
        weight_grads(t, first)
        return carry
    lax.fori_loop(0, TP, grads_step, 0)

    arrive(acts[1])
    stats = norm(second)
    up(second)
    expand(0, sb0, db0)
    per = GROUPS // 2 // TP
    for t in range(TP):
        lax.fori_loop(t * per, (t + 1) * per, grid_step, 0)
        if t > 0:
            sum_core(t - 1)
        if t == TP - 1:
            sum_y(0)
        weight_grads(t, second)
        start([c1[t]])
    sum_y(1)
    down(second, dn1_s)
    sum_core(TP - 1)
    send_out(1, 0)
    sum_y(2)
    norm_back(second, dn1_s, *stats)
    sum_z(0)
    norm_back(first, dn0_s, *stats0)
    sum_z(1)
    sum_y(3)
    send_out(1, 1)
    sum_z(2)
    sum_z(3)
    send_out(0, 1)
    for t in range(TP):
        sum_x(t)
    arrive(c5)
    slot = part(core * TP + y, EIGHTH)
    c6 = [remote(r5.at[0:EIGHTH, :], r7.at[slot, :], s6.at[i], q6.at[i], yc_peers[i]) for i in range(len(group))]
    start(c6)
    r7[slot, :] = r5[0:EIGHTH, :]
    arrive(c6)
    for degree in range(DEGS):
        d_up[degree] = r7[degree * CH:(degree + 1) * CH, :]
        d_down[degree] = r7[(TP + degree) * CH:(TP + degree + 1) * CH, :]
    d_gate[...] = r7[DEGS * CH:TP * CH, :]
    finished = wx + gx + wy + wc + c1 + c5 + c6
    for group_of in [acts[1]] + c2 + c3 + c4:
        finished = finished + group_of
    for b in range(BLOCKS):
        for i in range(2):
            kept[b][i].wait()
            for third in range(DEGS):
                arrive(sent[b][i][third])
                finished = finished + sent[b][i][third]
    for c in finished:
        c.wait_send()


def step_call(x, g, gain, up, gate, down, tog, frg):
    vm = pl.BlockSpec(memory_space=pltpu.VMEM)
    hbm = pl.BlockSpec(memory_space=pl.ANY)
    dma = pltpu.SemaphoreType.DMA
    v = pltpu.VMEM
    sds = jax.ShapeDtypeStruct
    atoms = x.shape[2] // TP
    act = (COEFS, CH, atoms)
    hid = (COEFS, HID, BLK)
    peers = TP - 1
    zs = NZ - 1
    return pl.pallas_call(
        step_kernel,
        out_shape=[sds(x.shape, BF16), sds(x.shape, BF16), sds((DEGS, CH, CH), BF16), sds((CH, CH), BF16), sds((DEGS, CH, CH), BF16)],
        in_specs=[hbm] * 8, out_specs=[hbm] * 2 + [vm] * 3,
        scratch_shapes=[
            v(act, BF16), v(act, BF16), v((TP, DEGS, SLICE), F32), v((DEGS, CH, HID), BF16), v((CH, HID), BF16), v((DEGS, TP, CH, CH), BF16),
            v(act, BF16), v(act, BF16), v((TP, ROWS, CH), F32), v((DEGS, CH, CH), F32), v((DEGS, CH, BLK), F32),
            v((DEGS, HID, CH), BF16), v((HID, CH), BF16), v((DEGS, CH, HID), BF16),
            v((GRID_ROWS, BLK), BF16), v((GRID_ROWS, CH), BF16), v((ZROWS, BLK), BF16), v((YROWS, BLK), BF16), v((2 * ZROWS, CH), BF16), v((2 * YROWS, CH), BF16),
            v((COEFS, CH, BLK), BF16), v(hid, BF16), v(hid, BF16), v(hid, BF16), v(hid, BF16), v((HID, BLK), BF16), v((COEFS, CH, BLK), F32), v((COEFS, CH, BLK), F32),
            v((GRID_PAD, BLK), BF16), v((GRID_PAD, BLK), BF16), v((GRID_PAD, BLK), BF16), v((GRID_PAD, BLK), BF16),
            v((TP, ROWS // 2, CH), F32), v((TP, ROWS // 2, CH), F32), v((TP, peers, EIGHTH, CH), F32), v((TP, EIGHTH, CH), F32),
            v((TP, zs, TILE, CH), F32), v((TP, TILE, CH), F32), v((TP, peers, TILE, CH), F32), v((TILE, CH), BF16),
            v((NZ * TILE, CH), BF16), v((ROWS, CH), BF16), v((DEGS, SLICE), F32), v((COEFS, PTS), F32), v((COEFS - 1, PTS), F32), dma((3,)),
            dma((BLOCKS, peers, 2)), dma((BLOCKS, peers, 2)), dma((peers, 3)), dma((peers, 3)), dma((peers, 3)), dma((peers, 3)), dma((3,)), dma((3,)),
            dma((peers,)), dma((peers,)), dma((5,)),
            dma((BLOCKS, 2, DEGS, peers)), dma((BLOCKS, 2, DEGS, peers)), dma((BLOCKS, 2)),
            dma((TP,)), dma((TP,)), dma((TP, peers)), dma((TP, peers)), dma((TP, zs)), dma((TP, zs)), dma((TP, peers)), dma((TP, peers)),
            dma((zs,)), dma((zs,)), dma((zs,)), dma((zs,))],
        compiler_params=pltpu.CompilerParams(collective_id=0, has_side_effects=True, vmem_limit_bytes=VMEM_LIMIT), name="step",
    )(x, g, gain, up, gate, down, tog, frg)


def store_kernel(*refs):
    count = (len(refs) - 2) // 3
    sources, results, bufs = refs[:count], refs[count:2 * count], refs[2 * count:3 * count]
    in_sem, out_sem = refs[3 * count:]
    loads = [pltpu.make_async_copy(src, buf, in_sem.at[i]) for i, (src, buf) in enumerate(zip(sources, bufs))]
    stores = [pltpu.make_async_copy(buf, dst, out_sem.at[i]) for i, (buf, dst) in enumerate(zip(bufs, results))]
    start(loads)
    for load, store in zip(loads, stores):
        load.wait()
        store.start()
    for store in stores:
        store.wait()


def store_call(*arrays):
    hbm = pl.BlockSpec(memory_space=pl.ANY)
    count = len(arrays)
    return pl.pallas_call(
        store_kernel, out_shape=[jax.ShapeDtypeStruct(a.shape, a.dtype) for a in arrays], in_specs=[hbm] * count, out_specs=[hbm] * count,
        scratch_shapes=[pltpu.VMEM(a.shape, a.dtype) for a in arrays] + [pltpu.SemaphoreType.DMA((count,))] * 2,
        compiler_params=pltpu.CompilerParams(vmem_limit_bytes=VMEM_LIMIT), name="store",
    )(*arrays)


def solution(mesh):
    act = P('dp', None, 'tp')
    in_specs = (act, P(None, 'tp'), P(None, None, 'tp'), P(None, 'tp'), P(None, 'tp', None), P(None, None), P(None, None), act)
    out_specs = (act, act, P(None, None, 'tp'), P(None, 'tp'), P(None, 'tp', None))

    def local_step(x, gain, up, gate, down, tog, frg, g):
        out, dx, d_up, d_gate, d_down = store_call(*step_call(x.transpose(1, 2, 0), g.transpose(1, 2, 0), gain, up, gate, down, tog, frg.T))
        return out.transpose(2, 0, 1), dx.transpose(2, 0, 1), d_up, d_gate, d_down

    return jax.shard_map(local_step, mesh=mesh, in_specs=in_specs, out_specs=out_specs, check_vma=False)
```

```python
import jax
import jax.numpy as jnp
from jax import lax
from jax.experimental import pallas as pl
from jax.experimental.pallas import tpu as pltpu
from jax.sharding import PartitionSpec as P

NORM_EPS = 1e-5
COEFS = 9
CH = 128
HID = 512
SUB = 16
BLK = 256
GRID_ROWS = 576
GRID_PAD = 640
SLAB = 56
ROWS = 896
TILE = 16
EIGHTH = 112
NZ = 8
DEGS = 3
TP = 4
SLICE = 32
PTS = 36
VEC_SCALE = 1.0 / 1024
VMEM_LIMIT = 60 * 2**20
F32 = jnp.float32
BF16 = jnp.bfloat16


def iota(shape, axis):
    return lax.broadcasted_iota(jnp.int32, shape, axis)


def mm(a, b):
    return jnp.dot(a, b, preferred_element_type=F32)


def mm_nt(a, b):
    return lax.dot_general(a, b, (((1,), (1,)), ((), ())), preferred_element_type=F32)


def one_hot(shape, row_div, col_div):
    return jnp.where(iota(shape, 0) // row_div == iota(shape, 1) // col_div, 1.0, 0.0).astype(BF16)


def point_of(row):
    main = row < HID
    point = jnp.where(main, (row % BLK) // NZ, SLICE + (row % SLICE) // NZ)
    half = jnp.where(main, row // BLK, (row % 64) // SLICE)
    return point, half


def spread_out(table_t, cols):
    point, half = point_of(iota((GRID_ROWS, CH), 0))
    left = mm(jnp.where(point == iota((GRID_ROWS, CH), 1), 1.0, 0.0).astype(BF16), table_t).astype(BF16)
    full = mm(left, one_hot((CH, cols), 1, SUB))
    row = iota((GRID_ROWS, cols), 0)
    same = point_of(row)[1] * NZ + row % NZ == iota((GRID_ROWS, cols), 1) % SUB
    return jnp.where(same, 0.5 * full, 0.0).astype(BF16)


def spread_back(table, rows):
    left = mm(one_hot((rows, CH), NZ, 1), table).astype(BF16)
    full = mm(left, one_hot((CH, BLK), 1, NZ))
    return jnp.where(iota((rows, BLK), 0) % NZ == iota((rows, BLK), 1) % NZ, full, 0.0).astype(BF16)


def spread_last(table, rows):
    row, col = iota((2 * rows, CH), 0), iota((2 * rows, CH), 1)
    r2, c2 = iota((2 * rows, CH), 0), iota((2 * rows, CH), 1)
    left = mm(jnp.where((r2 % rows) // NZ == c2, 1.0, 0.0).astype(BF16), table).astype(BF16)
    pick = jnp.where(iota((CH, CH), 0) == SLICE + (iota((CH, CH), 1) % SLICE) // NZ, 1.0, 0.0).astype(BF16)
    full = mm(left, pick)
    same = (row % NZ == col % NZ) & (row // rows == col // SLICE)
    return jnp.where(same, full, 0.0).astype(BF16)


def degree_of(coef):
    return jnp.where(coef >= 4, 2, jnp.where(coef >= 1, 1, 0))


MESH = pl.DeviceIdType.MESH


def places():
    dp = lax.axis_index("dp")
    return lax.axis_index("tp"), dp // NZ, (dp // 2) % TP, dp % 2


def dp_index(z, y, core):
    return (z * TP + y) * 2 + core


def remote(src, dst, send_sem, recv_sem, peer):
    return pltpu.make_async_remote_copy(src_ref=src, dst_ref=dst, send_sem=send_sem, recv_sem=recv_sem,
                                        device_id=peer, device_id_type=MESH)


def part(i, size):
    return pl.ds(pl.multiple_of(i * size, size), size)


def start(copies):
    for c in copies:
        c.start()


def arrive(copies):
    for c in copies:
        c.wait_recv()


CHUNK = 288
KROWS = 144
ZROWS = 64
YROWS = 72
GROUPS = HID // SUB
BLOCKS = 2


def step_kernel(x_loc, g_loc, gain_loc, up_loc, gate_loc, down_loc, tog_ref, frg_ref,
                out_loc, dx_loc, d_up, d_gate, d_down,
                x_all, g_all, gain_x, up_all, gate_all, down_all, out_all, dx_all, wg, pad_s, gain_b,
                wup_t, wgate_t, wdown_t, kg, kf, kft, kgt, kftl, kgtl, n_s, y_s, dm_s, m_s, dy_s, da_s, dn_s, stat_s, sb0, sb1, db0, db1,
                r1, a1, r2, a2, r3, a3, r4, fin, r5, r7, gain_v, tog_v, frg_v, small_sem,
                act_send, act_recv, wx_send, wx_recv, wy_send, wy_recv, wc_send, wc_recv, gain_send, gain_recv, loc_sem,
                o_send, o_recv, oloc_sem, s1, q1, s2, q2, s3, q3, s4, q4, s5, q5, s6, q6):
    me, z, y, core = places()
    atoms = x_all.shape[2]
    small = [pltpu.make_async_copy(src, dst, small_sem.at[i]) for i, (src, dst) in enumerate(((gain_loc, gain_v), (tog_ref, tog_v), (frg_ref, frg_v)))]
    start(small)
    pair = {"dp": dp_index(z, y, 1 - core)}
    x_dist = list(range(1, TP))
    x_peers = [{"tp": lax.rem(me + d, TP)} for d in x_dist]
    y_peers = [{"dp": dp_index(z, lax.rem(y + d, TP), core)} for d in x_dist]
    z_peers = [{"dp": dp_index(lax.rem(z + d, NZ), y, core)} for d in range(1, NZ)]
    group = [(dy, dc) for dc in range(2) for dy in range(TP) if dy + dc > 0]
    yc_peers = [{"dp": dp_index(z, lax.rem(y + dy, TP), lax.rem(core + dc, 2))} for dy, dc in group]
    barrier = pltpu.get_barrier_semaphore()
    meeting = x_peers + z_peers + yc_peers
    for peer in meeting:
        pl.semaphore_signal(barrier, inc=1, device_id=peer, device_id_type=MESH)
    pl.semaphore_wait(barrier, len(meeting))

    eighth = part(core * TP + y, TILE)
    mine = part(me, CH)
    pieces = [(up_loc.at[:, eighth, :], up_all.at[:, eighth, mine]),
              (gate_loc.at[eighth, :], gate_all.at[eighth, mine]),
              (down_loc.at[:, eighth, :], down_all.at[:, me, eighth, :])]
    wx = [remote(src, dst, wx_send.at[d, i], wx_recv.at[d, i], peer)
          for d, peer in enumerate(x_peers) for i, (src, dst) in enumerate(pieces)]
    gx = [remote(gain_loc, gain_x.at[me], gain_send.at[d], gain_recv.at[d], peer) for d, peer in enumerate(x_peers)]
    start(wx + gx)
    def acts(b):
        copies = []
        for d, peer in enumerate(x_peers):
            cols = part(lax.rem(me + d + 1, TP) * BLOCKS + b, BLK)
            for i, (src, dst) in enumerate(((x_loc, x_all), (g_loc, g_all))):
                copies.append(remote(src.at[:, :, cols], dst.at[:, part(me, SLICE), part(b, BLK)], act_send.at[b, d, i], act_recv.at[b, d, i], peer))
        return copies

    start(acts(0)[0::2])
    local = [pltpu.make_async_copy(src, dst, loc_sem.at[i]) for i, (src, dst) in enumerate(
        pieces + [(x_loc.at[:, :, part(me, atoms)], x_all.at[:, part(me, SLICE), :]), (g_loc.at[:, :, part(me, atoms)], g_all.at[:, part(me, SLICE), :])])]
    start(local)

    pad_s[...] = jnp.zeros(pad_s.shape, F32)
    for c in small:
        c.wait()
    pad_s[0, 0:COEFS, 0:PTS] = tog_v[...]
    pad_s[1, 0:COEFS - 1, 0:PTS] = frg_v[...]
    tog, tog_t = pad_s[0].astype(BF16), pad_s[0].T.astype(BF16)
    frg_t, frg = pad_s[1].astype(BF16), pad_s[1].T.astype(BF16)
    kg[...] = spread_out(tog_t, BLK)
    kf[...] = spread_out(frg, CH)
    kft[...] = spread_back(frg_t, ZROWS)
    kgt[...] = spread_back(tog, YROWS)
    kftl[...] = spread_last(frg_t, ZROWS)
    kgtl[...] = spread_last(tog, YROWS)
    for buf in (sb0, sb1, db0, db1):
        buf[GRID_ROWS:GRID_PAD, :] = jnp.zeros((GRID_PAD - GRID_ROWS, BLK), BF16)
    wg[...] = jnp.zeros(wg.shape, F32)
    gain_x[me] = gain_v[...]
    for c in local:
        c.wait()
    arrive(wx)
    wholes = [lambda rows: up_all.at[:, rows, :], lambda rows: gate_all.at[rows, :], lambda rows: down_all.at[:, :, rows, :]]
    wy = [remote(whole(eighth), whole(eighth), wy_send.at[d, i], wy_recv.at[d, i], peer)
          for d, peer in enumerate(y_peers) for i, whole in enumerate(wholes)]
    start(wy)
    start(acts(0)[1::2])
    arrive(gx)
    for t in range(TP):
        pad_s[2, t * NZ:t * NZ + DEGS, 0:SLICE] = gain_x[t]
    cols = pad_s[2].T
    for t in range(TP):
        for degree in range(DEGS):
            col = t * NZ + degree
            gain_b[degree, t * SLICE:(t + 1) * SLICE, :] = jnp.broadcast_to(cols[0:SLICE, col:col + 1], (SLICE, BLK))
    arrive(wy)
    side = part(core, CH // 2)
    wc = [remote(whole(side), whole(side), wc_send.at[i], wc_recv.at[i], pair) for i, whole in enumerate(wholes)]
    start(wc)
    arrive(wc)
    for degree in range(DEGS):
        wup_t[degree] = up_all[degree].T
        wdown_t[degree] = down_all[degree].reshape(HID, CH).T
    wgate_t[...] = gate_all[...].T

    def gain_of(coef):
        return gain_b[0 if coef == 0 else (1 if coef < TP else 2)]

    def norm(b, lanes):
        x0 = x_all[0, :, lanes].astype(F32)
        mean_s = jnp.sum(x0, axis=0, keepdims=True) * (1.0 / CH)
        cen = x0 - mean_s
        inv_s = lax.rsqrt(jnp.sum(cen * cen, axis=0, keepdims=True) * (1.0 / CH) + NORM_EPS)
        n_s[0] = ((cen * inv_s) * gain_of(0)).astype(BF16)
        acc = jnp.zeros((CH, BLK), F32)
        for coef in range(1, COEFS):
            xk = x_all[coef, :, lanes].astype(F32)
            acc = acc + xk * xk
        inv_v = lax.rsqrt(jnp.sum(acc, axis=0, keepdims=True) * VEC_SCALE + NORM_EPS)
        for coef in range(1, COEFS):
            xk = x_all[coef, :, lanes].astype(F32)
            n_s[coef] = ((xk * inv_v) * gain_of(coef)).astype(BF16)
        for i, stat in enumerate((mean_s, inv_s, inv_v)):
            stat_s[b, i:i + 1, :] = stat

    def up(lanes):
        def up_step(i, carry):
            for k in range(DEGS):
                coef = i * DEGS + k
                degree = degree_of(coef)
                y_s[coef] = mm(wup_t[degree], n_s[coef]).astype(BF16)
                dm_s[coef] = mm(down_all[degree].reshape(HID, CH), g_all[coef, :, lanes]).astype(BF16)
            return carry
        lax.fori_loop(0, DEGS, up_step, 0)

        def gate_step(i, carry):
            rows = part(i, CH)
            half = (0.5 * mm(wgate_t[rows, :], n_s[0])).astype(BF16).astype(F32)
            th = jnp.tanh(half)
            plus = 1.0 + th
            val = half * plus
            m_s[0, rows, :] = val.astype(BF16)
            slope = 0.5 * (plus + val * (1.0 - th))
            da_s[rows, :] = (dm_s[0, rows, :].astype(F32) * slope).astype(BF16)
            return carry
        lax.fori_loop(0, TP, gate_step, 0)

    def expand(j, s_buf, du_buf):
        rows = part(j, SUB)
        yj = y_s[:, rows, :].reshape(KROWS, BLK)
        dzj = dm_s[1:, rows, :].reshape(CH, BLK)
        for r0 in range(0, GRID_ROWS, CHUNK):
            half = mm(kg[r0:r0 + CHUNK, 0:KROWS], yj).astype(BF16).astype(F32)
            dval = mm(kf[r0:r0 + CHUNK, :], dzj).astype(BF16).astype(F32)
            th = jnp.tanh(half)
            plus = 1.0 + th
            val = half * plus
            s_buf[r0:r0 + CHUNK, :] = val.astype(BF16)
            du_buf[r0:r0 + CHUNK, :] = (dval * (plus + val * (1.0 - th))).astype(BF16)

    def halves(back, last, buf, rows):
        low = mm(last[...], buf[HID:GRID_PAD, :])
        sums = [mm(back[...], buf[h * BLK:(h + 1) * BLK, :]) + low[h * rows:(h + 1) * rows, :] for h in range(2)]
        return jnp.concatenate([v.reshape(rows // NZ, NZ, BLK) for v in sums], axis=1).astype(BF16)

    def contract(j, s_buf, du_buf):
        rows = part(j, SUB)
        m_s[1:, rows, :] = halves(kft, kftl, s_buf, ZROWS)
        dy_s[:, rows, :] = halves(kgt, kgtl, du_buf, YROWS)

    def grid_step(i, carry):
        expand(2 * i + 1, sb1, db1)
        contract(2 * i, sb0, db0)
        expand(jnp.minimum(2 * i + 2, GROUPS - 1), sb0, db0)
        contract(2 * i + 1, sb1, db1)
        return carry

    def weight_grads(t, lanes):
        rows = part(t, CH)

        for degree in range(DEGS):
            coefs = range(degree * degree, (degree + 1) * (degree + 1))
            wg[t, degree * CH:(degree + 1) * CH, :] += sum(mm_nt(n_s[c], dy_s[c, rows, :]) for c in coefs)
            wg[t, (degree + TP) * CH:(degree + TP + 1) * CH, :] += sum(mm_nt(m_s[c, rows, :], g_all[c, :, lanes]) for c in coefs)
        wg[t, DEGS * CH:TP * CH, :] += mm_nt(n_s[0], da_s[rows, :])

    def down(b, lanes):
        def down_step(i, carry):
            for k in range(DEGS):
                coef = i * DEGS + k
                degree = degree_of(coef)
                xk = x_all[coef, :, lanes].astype(F32)
                out_all[coef, :, lanes] = (xk + mm(wdown_t[degree], m_s[coef])).astype(BF16)
                dn_s[b, coef] = mm(up_all[degree], dy_s[coef])
            return carry
        lax.fori_loop(0, DEGS, down_step, 0)
        dn_s[b, 0] += mm(gate_all[...], da_s[...])

    def norm_back(i, carry):
        b = 1 - i
        lanes = part(b, BLK)
        mean_s, inv_s, inv_v = [stat_s[b, k:k + 1, :] for k in range(DEGS)]
        hat = (x_all[0, :, lanes].astype(F32) - mean_s) * inv_s
        dh = dn_s[b, 0].astype(BF16).astype(F32) * gain_of(0)
        m1 = jnp.sum(dh, axis=0, keepdims=True) * (1.0 / CH)
        m2 = jnp.sum(dh * hat, axis=0, keepdims=True) * (1.0 / CH)
        dx_all[0, :, lanes] = (inv_s * (dh - m1 - hat * m2) + g_all[0, :, lanes].astype(F32)).astype(BF16)
        acc = jnp.zeros((CH, BLK), F32)
        for coef in range(1, COEFS):
            xk = x_all[coef, :, lanes].astype(F32)
            acc = acc + (dn_s[b, coef].astype(BF16).astype(F32) * gain_of(coef)) * (xk * inv_v)
        mv = jnp.sum(acc, axis=0, keepdims=True) * VEC_SCALE
        for coef in range(1, COEFS):
            xk = x_all[coef, :, lanes].astype(F32)
            dh = dn_s[b, coef].astype(BF16).astype(F32) * gain_of(coef)
            dx_all[coef, :, lanes] = (inv_v * (dh - (xk * inv_v) * mv) + g_all[coef, :, lanes].astype(F32)).astype(BF16)
        return carry

    outs = ((out_all, out_loc), (dx_all, dx_loc))

    def out_copies(b, i, third):
        src, dst = outs[i]
        coefs = slice(third * DEGS, (third + 1) * DEGS)
        cols = part(me * BLOCKS + b, BLK)
        return [remote(src.at[coefs, part(lax.rem(me + d, TP), SLICE), part(b, BLK)], dst.at[coefs, :, cols],
                       o_send.at[b, i, third, d - 1], o_recv.at[b, i, third, d - 1], x_peers[d - 1]) for d in x_dist]

    def out_local(b, i):
        src, dst = outs[i]
        return pltpu.make_async_copy(src.at[:, part(me, SLICE), part(b, BLK)], dst.at[:, :, part(me * BLOCKS + b, BLK)], oloc_sem.at[b, i])

    sent = [[[out_copies(b, i, third) for third in range(DEGS)] for i in range(2)] for b in range(BLOCKS)]
    kept = [[out_local(b, i) for i in range(2)] for b in range(BLOCKS)]

    def send_out(b, i):
        for third in range(DEGS):
            start(sent[b][i][third])
        kept[b][i].start()

    half_rows = ROWS // 2

    def c1(t):
        return remote(wg.at[t, part(1 - core, half_rows), :], r1.at[t], s1.at[t], q1.at[t], pair)

    def c2(t):
        return [remote(a1.at[t, part(lax.rem(y + d, TP), EIGHTH), :], r2.at[t, d - 1], s2.at[t, d - 1], q2.at[t, d - 1], y_peers[d - 1]) for d in x_dist]

    def c3(t):
        return [remote(a2.at[t, part(lax.rem(lax.rem(z + d, NZ), NZ - 1), TILE), :], r3.at[t, d - 1], s3.at[t, d - 1], q3.at[t, d - 1], z_peers[d - 1])
                for d in range(1, NZ)]

    def c4(t):
        return [remote(a3.at[t], r4.at[t, d - 1], s4.at[t, d - 1], q4.at[t, d - 1], x_peers[d - 1]) for d in x_dist]

    c5 = [remote(fin, r5.at[part(z, TILE), :], s5.at[d - 1], q5.at[d - 1], z_peers[d - 1]) for d in range(1, NZ)]

    def sum_core(t):
        c1(t).wait_recv()
        a1[t] = wg[t, part(core, half_rows), :] + r1[t]
        start(c2(t))

    def sum_y(t):
        arrive(c2(t))
        a2[t] = (a1[t, part(y, EIGHTH), :] + r2[t, 0]) + (r2[t, 1] + r2[t, 2])
        start(c3(t))

    def sum_z(t):
        arrive(c3(t))
        own = a2[t, part(lax.rem(z, NZ - 1), TILE), :]
        a3[t] = ((own + r3[t, 0]) + (r3[t, 1] + r3[t, 2])) + ((r3[t, 3] + r3[t, 4]) + (r3[t, 5] + r3[t, 6]))
        start(c4(t))

    def sum_x(t):
        arrive(c4(t))

        @pl.when(me == t)
        def _():
            fin[...] = ((a3[t] + r4[t, 0]) + (r4[t, 1] + r4[t, 2])).astype(BF16)
            start(c5)
            r5[part(z, TILE), :] = fin[...]

    for c in acts(0):
        c.wait_send()
    start(acts(1))
    per = GROUPS // 2 // TP

    def block_step(b, carry):
        lanes = part(b, BLK)
        arrive(acts(b))
        norm(b, lanes)
        up(lanes)
        expand(0, sb0, db0)

        def quarter_step(t, inner):
            lax.fori_loop(t * per, (t + 1) * per, grid_step, 0)

            @pl.when((b == 1) & (t > 0))
            def _():
                sum_core(t - 1)

            @pl.when((b == 1) & (t == TP - 1))
            def _():
                sum_y(0)
            weight_grads(t, lanes)

            @pl.when(b == 1)
            def _():
                c1(t).start()
            return inner
        lax.fori_loop(0, TP, quarter_step, 0)
        down(b, lanes)

        @pl.when(b == 0)
        def _():
            send_out(0, 0)
        return carry
    lax.fori_loop(0, BLOCKS, block_step, 0)
    sum_core(TP - 1)
    send_out(1, 0)
    sum_y(1)
    sum_y(2)
    lax.fori_loop(0, BLOCKS, norm_back, 0)
    sum_z(0)
    sum_z(1)
    sum_y(3)
    send_out(1, 1)
    sum_z(2)
    sum_z(3)
    send_out(0, 1)
    for t in range(TP):
        sum_x(t)
    arrive(c5)
    slot = part(core * TP + y, EIGHTH)
    c6 = [remote(r5.at[0:EIGHTH, :], r7.at[slot, :], s6.at[i], q6.at[i], yc_peers[i]) for i in range(len(group))]
    start(c6)
    r7[slot, :] = r5[0:EIGHTH, :]
    arrive(c6)
    for degree in range(DEGS):
        d_up[degree] = r7[degree * CH:(degree + 1) * CH, :]
        d_down[degree] = r7[(TP + degree) * CH:(TP + degree + 1) * CH, :]
    d_gate[...] = r7[DEGS * CH:TP * CH, :]
    finished = wx + gx + wy + wc + c5 + c6 + acts(1)
    for t in range(TP):
        finished = finished + [c1(t)] + c2(t) + c3(t) + c4(t)
    for b in range(BLOCKS):
        for i in range(2):
            kept[b][i].wait()
            for third in range(DEGS):
                arrive(sent[b][i][third])
                finished = finished + sent[b][i][third]
    for c in finished:
        c.wait_send()


def step_call(x, g, gain, up, gate, down, tog, frg):
    vm = pl.BlockSpec(memory_space=pltpu.VMEM)
    hbm = pl.BlockSpec(memory_space=pl.ANY)
    dma = pltpu.SemaphoreType.DMA
    v = pltpu.VMEM
    sds = jax.ShapeDtypeStruct
    atoms = x.shape[2] // TP
    act = (COEFS, CH, atoms)
    hid = (COEFS, HID, BLK)
    peers = TP - 1
    zs = NZ - 1
    return pl.pallas_call(
        step_kernel,
        out_shape=[sds(x.shape, BF16), sds(x.shape, BF16), sds((DEGS, CH, CH), BF16), sds((CH, CH), BF16), sds((DEGS, CH, CH), BF16)],
        in_specs=[hbm] * 8, out_specs=[hbm] * 2 + [vm] * 3,
        scratch_shapes=[
            v(act, BF16), v(act, BF16), v((TP, DEGS, SLICE), F32), v((DEGS, CH, HID), BF16), v((CH, HID), BF16), v((DEGS, TP, CH, CH), BF16),
            v(act, BF16), v(act, BF16), v((TP, ROWS, CH), F32), v((DEGS, CH, CH), F32), v((DEGS, CH, BLK), F32),
            v((DEGS, HID, CH), BF16), v((HID, CH), BF16), v((DEGS, CH, HID), BF16),
            v((GRID_ROWS, BLK), BF16), v((GRID_ROWS, CH), BF16), v((ZROWS, BLK), BF16), v((YROWS, BLK), BF16), v((2 * ZROWS, CH), BF16), v((2 * YROWS, CH), BF16),
            v((COEFS, CH, BLK), BF16), v(hid, BF16), v(hid, BF16), v(hid, BF16), v(hid, BF16), v((HID, BLK), BF16), v((BLOCKS, COEFS, CH, BLK), F32), v((BLOCKS, NZ, BLK), F32),
            v((GRID_PAD, BLK), BF16), v((GRID_PAD, BLK), BF16), v((GRID_PAD, BLK), BF16), v((GRID_PAD, BLK), BF16),
            v((TP, ROWS // 2, CH), F32), v((TP, ROWS // 2, CH), F32), v((TP, peers, EIGHTH, CH), F32), v((TP, EIGHTH, CH), F32),
            v((TP, zs, TILE, CH), F32), v((TP, TILE, CH), F32), v((TP, peers, TILE, CH), F32), v((TILE, CH), BF16),
            v((NZ * TILE, CH), BF16), v((ROWS, CH), BF16), v((DEGS, SLICE), F32), v((COEFS, PTS), F32), v((COEFS - 1, PTS), F32), dma((3,)),
            dma((BLOCKS, peers, 2)), dma((BLOCKS, peers, 2)), dma((peers, 3)), dma((peers, 3)), dma((peers, 3)), dma((peers, 3)), dma((3,)), dma((3,)),
            dma((peers,)), dma((peers,)), dma((5,)),
            dma((BLOCKS, 2, DEGS, peers)), dma((BLOCKS, 2, DEGS, peers)), dma((BLOCKS, 2)),
            dma((TP,)), dma((TP,)), dma((TP, peers)), dma((TP, peers)), dma((TP, zs)), dma((TP, zs)), dma((TP, peers)), dma((TP, peers)),
            dma((zs,)), dma((zs,)), dma((zs,)), dma((zs,))],
        compiler_params=pltpu.CompilerParams(collective_id=0, has_side_effects=True, vmem_limit_bytes=VMEM_LIMIT), name="step",
    )(x, g, gain, up, gate, down, tog, frg)


def store_kernel(*refs):
    count = (len(refs) - 2) // 3
    sources, results, bufs = refs[:count], refs[count:2 * count], refs[2 * count:3 * count]
    in_sem, out_sem = refs[3 * count:]
    loads = [pltpu.make_async_copy(src, buf, in_sem.at[i]) for i, (src, buf) in enumerate(zip(sources, bufs))]
    stores = [pltpu.make_async_copy(buf, dst, out_sem.at[i]) for i, (buf, dst) in enumerate(zip(bufs, results))]
    start(loads)
    for load, store in zip(loads, stores):
        load.wait()
        store.start()
    for store in stores:
        store.wait()


def store_call(*arrays):
    hbm = pl.BlockSpec(memory_space=pl.ANY)
    count = len(arrays)
    return pl.pallas_call(
        store_kernel, out_shape=[jax.ShapeDtypeStruct(a.shape, a.dtype) for a in arrays], in_specs=[hbm] * count, out_specs=[hbm] * count,
        scratch_shapes=[pltpu.VMEM(a.shape, a.dtype) for a in arrays] + [pltpu.SemaphoreType.DMA((count,))] * 2,
        compiler_params=pltpu.CompilerParams(vmem_limit_bytes=VMEM_LIMIT), name="store",
    )(*arrays)


def solution(mesh):
    act = P('dp', None, 'tp')
    in_specs = (act, P(None, 'tp'), P(None, None, 'tp'), P(None, 'tp'), P(None, 'tp', None), P(None, None), P(None, None), act)
    out_specs = (act, act, P(None, None, 'tp'), P(None, 'tp'), P(None, 'tp', None))

    def local_step(x, gain, up, gate, down, tog, frg, g):
        out, dx, d_up, d_gate, d_down = store_call(*step_call(x.transpose(1, 2, 0), g.transpose(1, 2, 0), gain, up, gate, down, tog, frg.T))
        return out.transpose(2, 0, 1), dx.transpose(2, 0, 1), d_up, d_gate, d_down

    return jax.shard_map(local_step, mesh=mesh, in_specs=in_specs, out_specs=out_specs, check_vma=False)
```

```python
import jax
import jax.numpy as jnp
from jax import lax
from jax.experimental import pallas as pl
from jax.experimental.pallas import tpu as pltpu
from jax.sharding import PartitionSpec as P

NORM_EPS = 1e-5
COEFS = 9
CH = 128
HID = 512
SUB = 16
BLK = 256
GRID_ROWS = 576
GRID_PAD = 640
SLAB = 56
ROWS = 896
TILE = 16
EIGHTH = 112
NZ = 8
DEGS = 3
TP = 4
SLICE = 32
PTS = 36
VEC_SCALE = 1.0 / 1024
VMEM_LIMIT = 60 * 2**20
F32 = jnp.float32
BF16 = jnp.bfloat16


def iota(shape, axis):
    return lax.broadcasted_iota(jnp.int32, shape, axis)


def mm(a, b):
    return jnp.dot(a, b, preferred_element_type=F32)


def mm_nt(a, b):
    return lax.dot_general(a, b, (((1,), (1,)), ((), ())), preferred_element_type=F32)


def one_hot(shape, row_div, col_div):
    return jnp.where(iota(shape, 0) // row_div == iota(shape, 1) // col_div, 1.0, 0.0).astype(BF16)


def point_of(row):
    main = row < HID
    point = jnp.where(main, (row % BLK) // NZ, SLICE + (row % SLICE) // NZ)
    half = jnp.where(main, row // BLK, (row % 64) // SLICE)
    return point, half


def spread_out(table_t, cols):
    point, half = point_of(iota((GRID_ROWS, CH), 0))
    left = mm(jnp.where(point == iota((GRID_ROWS, CH), 1), 1.0, 0.0).astype(BF16), table_t).astype(BF16)
    full = mm(left, one_hot((CH, cols), 1, SUB))
    row = iota((GRID_ROWS, cols), 0)
    same = point_of(row)[1] * NZ + row % NZ == iota((GRID_ROWS, cols), 1) % SUB
    return jnp.where(same, 0.5 * full, 0.0).astype(BF16)


def spread_back(table, rows):
    left = mm(one_hot((rows, CH), NZ, 1), table).astype(BF16)
    full = mm(left, one_hot((CH, BLK), 1, NZ))
    return jnp.where(iota((rows, BLK), 0) % NZ == iota((rows, BLK), 1) % NZ, full, 0.0).astype(BF16)


def spread_last(table, rows):
    row, col = iota((2 * rows, CH), 0), iota((2 * rows, CH), 1)
    r2, c2 = iota((2 * rows, CH), 0), iota((2 * rows, CH), 1)
    left = mm(jnp.where((r2 % rows) // NZ == c2, 1.0, 0.0).astype(BF16), table).astype(BF16)
    pick = jnp.where(iota((CH, CH), 0) == SLICE + (iota((CH, CH), 1) % SLICE) // NZ, 1.0, 0.0).astype(BF16)
    full = mm(left, pick)
    same = (row % NZ == col % NZ) & (row // rows == col // SLICE)
    return jnp.where(same, full, 0.0).astype(BF16)


def degree_of(coef):
    return jnp.where(coef >= 4, 2, jnp.where(coef >= 1, 1, 0))


MESH = pl.DeviceIdType.MESH


def places():
    dp = lax.axis_index("dp")
    return lax.axis_index("tp"), dp // NZ, (dp // 2) % TP, dp % 2


def dp_index(z, y, core):
    return (z * TP + y) * 2 + core


def remote(src, dst, send_sem, recv_sem, peer):
    return pltpu.make_async_remote_copy(src_ref=src, dst_ref=dst, send_sem=send_sem, recv_sem=recv_sem,
                                        device_id=peer, device_id_type=MESH)


def part(i, size):
    return pl.ds(pl.multiple_of(i * size, size), size)


def start(copies):
    for c in copies:
        c.start()


def arrive(copies):
    for c in copies:
        c.wait_recv()


CHUNK = 288
KROWS = 144
ZROWS = 64
YROWS = 72
GROUPS = HID // SUB
BLOCKS = 2


def step_kernel(x_loc, g_loc, gain_loc, up_loc, gate_loc, down_loc, tog_ref, frg_ref,
                out_loc, dx_loc, r7,
                x_all, g_all, gain_x, up_all, gate_all, down_all, out_all, dx_all, wg, pad_s, gain_b,
                wup_t, wgate_t, wdown_t, kg, kf, kft, kgt, kftl, kgtl, n_s, y_s, dm_s, m_s, dy_s, da_s, dn_s, stat_s, sb0, sb1, db0, db1,
                r1, a1, r2, a2, r3, a3, r4, fin, r5, gain_v, tog_v, frg_v, small_sem,
                act_send, act_recv, wx_send, wx_recv, wy_send, wy_recv, wc_send, wc_recv, gain_send, gain_recv, loc_sem,
                o_send, o_recv, oloc_sem, s1, q1, s2, q2, s3, q3, s4, q4, s5, q5, s6, q6):
    me, z, y, core = places()
    atoms = x_all.shape[2]
    small = [pltpu.make_async_copy(src, dst, small_sem.at[i]) for i, (src, dst) in enumerate(((gain_loc, gain_v), (tog_ref, tog_v), (frg_ref, frg_v)))]
    start(small)
    pair = {"dp": dp_index(z, y, 1 - core)}
    x_dist = list(range(1, TP))
    x_peers = [{"tp": lax.rem(me + d, TP)} for d in x_dist]
    y_peers = [{"dp": dp_index(z, lax.rem(y + d, TP), core)} for d in x_dist]
    z_peers = [{"dp": dp_index(lax.rem(z + d, NZ), y, core)} for d in range(1, NZ)]
    group = [(dy, dc) for dc in range(2) for dy in range(TP) if dy + dc > 0]
    yc_peers = [{"dp": dp_index(z, lax.rem(y + dy, TP), lax.rem(core + dc, 2))} for dy, dc in group]
    barrier = pltpu.get_barrier_semaphore()
    meeting = x_peers + z_peers + yc_peers
    for peer in meeting:
        pl.semaphore_signal(barrier, inc=1, device_id=peer, device_id_type=MESH)
    pl.semaphore_wait(barrier, len(meeting))

    eighth = part(core * TP + y, TILE)
    mine = part(me, CH)
    pieces = [(up_loc.at[:, eighth, :], up_all.at[:, eighth, mine]),
              (gate_loc.at[eighth, :], gate_all.at[eighth, mine]),
              (down_loc.at[:, eighth, :], down_all.at[:, me, eighth, :])]
    wx = [remote(src, dst, wx_send.at[d, i], wx_recv.at[d, i], peer)
          for d, peer in enumerate(x_peers) for i, (src, dst) in enumerate(pieces)]
    gx = [remote(gain_loc, gain_x.at[me], gain_send.at[d], gain_recv.at[d], peer) for d, peer in enumerate(x_peers)]
    start(wx + gx)
    def acts(b):
        copies = []
        for d, peer in enumerate(x_peers):
            cols = part(lax.rem(me + d + 1, TP) * BLOCKS + b, BLK)
            for i, (src, dst) in enumerate(((x_loc, x_all), (g_loc, g_all))):
                copies.append(remote(src.at[:, :, cols], dst.at[:, part(me, SLICE), part(b, BLK)], act_send.at[b, d, i], act_recv.at[b, d, i], peer))
        return copies

    start(acts(0)[0::2])
    local = [pltpu.make_async_copy(src, dst, loc_sem.at[i]) for i, (src, dst) in enumerate(
        pieces + [(x_loc.at[:, :, part(me, atoms)], x_all.at[:, part(me, SLICE), :]), (g_loc.at[:, :, part(me, atoms)], g_all.at[:, part(me, SLICE), :])])]
    start(local)

    pad_s[...] = jnp.zeros(pad_s.shape, F32)
    for c in small:
        c.wait()
    pad_s[0, 0:COEFS, 0:PTS] = tog_v[...]
    pad_s[1, 0:COEFS - 1, 0:PTS] = frg_v[...]
    tog, tog_t = pad_s[0].astype(BF16), pad_s[0].T.astype(BF16)
    frg_t, frg = pad_s[1].astype(BF16), pad_s[1].T.astype(BF16)
    kg[...] = spread_out(tog_t, BLK)
    kf[...] = spread_out(frg, CH)
    kft[...] = spread_back(frg_t, ZROWS)
    kgt[...] = spread_back(tog, YROWS)
    kftl[...] = spread_last(frg_t, ZROWS)
    kgtl[...] = spread_last(tog, YROWS)
    for buf in (sb0, sb1, db0, db1):
        buf[GRID_ROWS:GRID_PAD, :] = jnp.zeros((GRID_PAD - GRID_ROWS, BLK), BF16)
    wg[...] = jnp.zeros(wg.shape, F32)
    gain_x[me] = gain_v[...]
    for c in local:
        c.wait()
    arrive(wx)
    wholes = [lambda rows: up_all.at[:, rows, :], lambda rows: gate_all.at[rows, :], lambda rows: down_all.at[:, :, rows, :]]
    wy = [remote(whole(eighth), whole(eighth), wy_send.at[d, i], wy_recv.at[d, i], peer)
          for d, peer in enumerate(y_peers) for i, whole in enumerate(wholes)]
    start(wy)
    start(acts(0)[1::2])
    arrive(gx)
    for t in range(TP):
        pad_s[2, t * NZ:t * NZ + DEGS, 0:SLICE] = gain_x[t]
    cols = pad_s[2].T
    for t in range(TP):
        for degree in range(DEGS):
            col = t * NZ + degree
            gain_b[degree, t * SLICE:(t + 1) * SLICE, :] = jnp.broadcast_to(cols[0:SLICE, col:col + 1], (SLICE, BLK))
    arrive(wy)
    side = part(core, CH // 2)
    wc = [remote(whole(side), whole(side), wc_send.at[i], wc_recv.at[i], pair) for i, whole in enumerate(wholes)]
    start(wc)
    arrive(wc)
    for degree in range(DEGS):
        wup_t[degree] = up_all[degree].T
        wdown_t[degree] = down_all[degree].reshape(HID, CH).T
    wgate_t[...] = gate_all[...].T

    def gain_of(coef):
        return gain_b[0 if coef == 0 else (1 if coef < TP else 2)]

    def norm(b, lanes):
        x0 = x_all[0, :, lanes].astype(F32)
        mean_s = jnp.sum(x0, axis=0, keepdims=True) * (1.0 / CH)
        cen = x0 - mean_s
        inv_s = lax.rsqrt(jnp.sum(cen * cen, axis=0, keepdims=True) * (1.0 / CH) + NORM_EPS)
        n_s[0] = ((cen * inv_s) * gain_of(0)).astype(BF16)
        acc = jnp.zeros((CH, BLK), F32)
        for coef in range(1, COEFS):
            xk = x_all[coef, :, lanes].astype(F32)
            acc = acc + xk * xk
        inv_v = lax.rsqrt(jnp.sum(acc, axis=0, keepdims=True) * VEC_SCALE + NORM_EPS)
        for coef in range(1, COEFS):
            xk = x_all[coef, :, lanes].astype(F32)
            n_s[coef] = ((xk * inv_v) * gain_of(coef)).astype(BF16)
        for i, stat in enumerate((mean_s, inv_s, inv_v)):
            stat_s[b, i:i + 1, :] = stat

    def up():
        def up_step(i, carry):
            for k in range(DEGS):
                coef = i * DEGS + k
                y_s[coef] = mm(wup_t[degree_of(coef)], n_s[coef]).astype(BF16)
            return carry
        lax.fori_loop(0, DEGS, up_step, 0)

    def hidden_grads(b, lanes):
        def grad_step(i, carry):
            for k in range(DEGS):
                coef = i * DEGS + k
                dm_s[coef] = mm(down_all[degree_of(coef)].reshape(HID, CH), g_all[coef, :, lanes]).astype(BF16)
            return carry
        lax.fori_loop(0, DEGS, grad_step, 0)

        def gate_step(i, carry):
            rows = part(i, CH)
            half = (0.5 * mm(wgate_t[rows, :], n_s[0])).astype(BF16).astype(F32)
            th = jnp.tanh(half)
            plus = 1.0 + th
            val = half * plus
            m_s[0, rows, :] = val.astype(BF16)
            slope = 0.5 * (plus + val * (1.0 - th))
            da_s[b, rows, :] = (dm_s[0, rows, :].astype(F32) * slope).astype(BF16)
            return carry
        lax.fori_loop(0, TP, gate_step, 0)

    def expand(j, s_buf, du_buf):
        rows = part(j, SUB)
        yj = y_s[:, rows, :].reshape(KROWS, BLK)
        dzj = dm_s[1:, rows, :].reshape(CH, BLK)
        for r0 in range(0, GRID_ROWS, CHUNK):
            half = mm(kg[r0:r0 + CHUNK, 0:KROWS], yj).astype(BF16).astype(F32)
            dval = mm(kf[r0:r0 + CHUNK, :], dzj).astype(BF16).astype(F32)
            th = jnp.tanh(half)
            plus = 1.0 + th
            val = half * plus
            s_buf[r0:r0 + CHUNK, :] = val.astype(BF16)
            du_buf[r0:r0 + CHUNK, :] = (dval * (plus + val * (1.0 - th))).astype(BF16)

    def halves(back, last, buf, rows):
        low = mm(last[...], buf[HID:GRID_PAD, :])
        sums = [mm(back[...], buf[h * BLK:(h + 1) * BLK, :]) + low[h * rows:(h + 1) * rows, :] for h in range(2)]
        return jnp.concatenate([v.reshape(rows // NZ, NZ, BLK) for v in sums], axis=1).astype(BF16)

    def contract(b, j, s_buf, du_buf):
        rows = part(j, SUB)
        m_s[1:, rows, :] = halves(kft, kftl, s_buf, ZROWS)
        dy_s[b, :, rows, :] = halves(kgt, kgtl, du_buf, YROWS)

    def grid_step(i, b):
        expand(2 * i + 1, sb1, db1)
        contract(b, 2 * i, sb0, db0)
        expand(jnp.minimum(2 * i + 2, GROUPS - 1), sb0, db0)
        contract(b, 2 * i + 1, sb1, db1)
        return b

    def weight_grads(b, t, lanes):
        rows = part(t, CH)

        for degree in range(DEGS):
            coefs = range(degree * degree, (degree + 1) * (degree + 1))
            wg[t, degree * CH:(degree + 1) * CH, :] += sum(mm_nt(n_s[c], dy_s[b, c, rows, :]) for c in coefs)
            wg[t, (degree + TP) * CH:(degree + TP + 1) * CH, :] += sum(mm_nt(m_s[c, rows, :], g_all[c, :, lanes]) for c in coefs)
        wg[t, DEGS * CH:TP * CH, :] += mm_nt(n_s[0], da_s[b, rows, :])

    def down(lanes):
        def down_step(i, carry):
            for k in range(DEGS):
                coef = i * DEGS + k
                xk = x_all[coef, :, lanes].astype(F32)
                out_all[coef, :, lanes] = (xk + mm(wdown_t[degree_of(coef)], m_s[coef])).astype(BF16)
            return carry
        lax.fori_loop(0, DEGS, down_step, 0)

    def norm_grads(b):
        def norm_grad_step(i, carry):
            for k in range(DEGS):
                coef = i * DEGS + k
                dn_s[coef] = mm(up_all[degree_of(coef)], dy_s[b, coef])
            return carry
        lax.fori_loop(0, DEGS, norm_grad_step, 0)
        dn_s[0] += mm(gate_all[...], da_s[b])

    def norm_back(i, carry):
        b = 1 - i
        norm_grads(b)
        lanes = part(b, BLK)
        mean_s, inv_s, inv_v = [stat_s[b, k:k + 1, :] for k in range(DEGS)]
        hat = (x_all[0, :, lanes].astype(F32) - mean_s) * inv_s
        dh = dn_s[0].astype(BF16).astype(F32) * gain_of(0)
        m1 = jnp.sum(dh, axis=0, keepdims=True) * (1.0 / CH)
        m2 = jnp.sum(dh * hat, axis=0, keepdims=True) * (1.0 / CH)
        dx_all[0, :, lanes] = (inv_s * (dh - m1 - hat * m2) + g_all[0, :, lanes].astype(F32)).astype(BF16)
        acc = jnp.zeros((CH, BLK), F32)
        for coef in range(1, COEFS):
            xk = x_all[coef, :, lanes].astype(F32)
            acc = acc + (dn_s[coef].astype(BF16).astype(F32) * gain_of(coef)) * (xk * inv_v)
        mv = jnp.sum(acc, axis=0, keepdims=True) * VEC_SCALE
        for coef in range(1, COEFS):
            xk = x_all[coef, :, lanes].astype(F32)
            dh = dn_s[coef].astype(BF16).astype(F32) * gain_of(coef)
            dx_all[coef, :, lanes] = (inv_v * (dh - (xk * inv_v) * mv) + g_all[coef, :, lanes].astype(F32)).astype(BF16)
        return carry

    outs = ((out_all, out_loc), (dx_all, dx_loc))

    def out_copies(b, i, third):
        src, dst = outs[i]
        coefs = slice(third * DEGS, (third + 1) * DEGS)
        cols = part(me * BLOCKS + b, BLK)
        return [remote(src.at[coefs, part(lax.rem(me + d, TP), SLICE), part(b, BLK)], dst.at[coefs, :, cols],
                       o_send.at[b, i, third, d - 1], o_recv.at[b, i, third, d - 1], x_peers[d - 1]) for d in x_dist]

    def out_local(b, i):
        src, dst = outs[i]
        return pltpu.make_async_copy(src.at[:, part(me, SLICE), part(b, BLK)], dst.at[:, :, part(me * BLOCKS + b, BLK)], oloc_sem.at[b, i])

    sent = [[[out_copies(b, i, third) for third in range(DEGS)] for i in range(2)] for b in range(BLOCKS)]
    kept = [[out_local(b, i) for i in range(2)] for b in range(BLOCKS)]

    def send_out(b, i):
        for third in range(DEGS):
            start(sent[b][i][third])
        kept[b][i].start()

    half_rows = ROWS // 2

    def c1(t):
        return remote(wg.at[t, part(1 - core, half_rows), :], r1.at[t], s1.at[t], q1.at[t], pair)

    def c2(t):
        return [remote(a1.at[t, part(lax.rem(y + d, TP), EIGHTH), :], r2.at[t, d - 1], s2.at[t, d - 1], q2.at[t, d - 1], y_peers[d - 1]) for d in x_dist]

    def c3(t):
        return [remote(a2.at[t, part(lax.rem(lax.rem(z + d, NZ), NZ - 1), TILE), :], r3.at[t, d - 1], s3.at[t, d - 1], q3.at[t, d - 1], z_peers[d - 1])
                for d in range(1, NZ)]

    def c4(t):
        return [remote(a3.at[t], r4.at[t, d - 1], s4.at[t, d - 1], q4.at[t, d - 1], x_peers[d - 1]) for d in x_dist]

    c5 = [remote(fin, r5.at[part(z, TILE), :], s5.at[d - 1], q5.at[d - 1], z_peers[d - 1]) for d in range(1, NZ)]

    def sum_core(t):
        c1(t).wait_recv()
        a1[t] = wg[t, part(core, half_rows), :] + r1[t]
        start(c2(t))

    def sum_y(t):
        arrive(c2(t))
        a2[t] = (a1[t, part(y, EIGHTH), :] + r2[t, 0]) + (r2[t, 1] + r2[t, 2])
        start(c3(t))

    def sum_z(t):
        arrive(c3(t))
        own = a2[t, part(lax.rem(z, NZ - 1), TILE), :]
        a3[t] = ((own + r3[t, 0]) + (r3[t, 1] + r3[t, 2])) + ((r3[t, 3] + r3[t, 4]) + (r3[t, 5] + r3[t, 6]))
        start(c4(t))

    def sum_x(t):
        arrive(c4(t))

        @pl.when(me == t)
        def _():
            fin[...] = ((a3[t] + r4[t, 0]) + (r4[t, 1] + r4[t, 2])).astype(BF16)
            start(c5)
            r5[part(z, TILE), :] = fin[...]

    for c in acts(0):
        c.wait_send()
    start(acts(1))
    per = GROUPS // 2 // TP

    def block_step(b, carry):
        lanes = part(b, BLK)
        arrive(acts(b)[0::2])
        norm(b, lanes)
        up()
        arrive(acts(b)[1::2])
        hidden_grads(b, lanes)
        expand(0, sb0, db0)

        def quarter_step(t, inner):
            lax.fori_loop(t * per, (t + 1) * per, grid_step, b)

            @pl.when((b == 1) & (t > 0))
            def _():
                sum_core(t - 1)

            @pl.when((b == 1) & (t == TP - 1))
            def _():
                sum_y(0)
            weight_grads(b, t, lanes)

            @pl.when(b == 1)
            def _():
                c1(t).start()
            return inner
        lax.fori_loop(0, TP, quarter_step, 0)

        @pl.when(b == 0)
        def _():
            down(lanes)
            send_out(0, 0)
        return carry
    lax.fori_loop(0, BLOCKS, block_step, 0)
    down(pl.ds(BLK, BLK))
    sum_core(TP - 1)
    send_out(1, 0)
    sum_y(1)
    norm_back(0, 0)
    sum_y(2)
    sum_z(0)
    sum_y(3)
    send_out(1, 1)
    norm_back(1, 0)
    sum_z(1)
    sum_z(2)
    sum_z(3)
    send_out(0, 1)
    for t in range(TP):
        sum_x(t)
    arrive(c5)
    slot = part(core * TP + y, EIGHTH)
    c6 = [remote(r5.at[0:EIGHTH, :], r7.at[slot, :], s6.at[i], q6.at[i], yc_peers[i]) for i in range(len(group))]
    start(c6)
    own = pltpu.make_async_copy(r5.at[0:EIGHTH, :], r7.at[slot, :], small_sem.at[0])
    own.start()
    arrive(c6)
    own.wait()
    finished = wx + gx + wy + wc + c5 + c6 + acts(1)
    for t in range(TP):
        finished = finished + [c1(t)] + c2(t) + c3(t) + c4(t)
    for b in range(BLOCKS):
        for i in range(2):
            kept[b][i].wait()
            for third in range(DEGS):
                arrive(sent[b][i][third])
                finished = finished + sent[b][i][third]
    for c in finished:
        c.wait_send()


def step_call(x, g, gain, up, gate, down, tog, frg):
    hbm = pl.BlockSpec(memory_space=pl.ANY)
    dma = pltpu.SemaphoreType.DMA
    v = pltpu.VMEM
    sds = jax.ShapeDtypeStruct
    atoms = x.shape[2] // TP
    act = (COEFS, CH, atoms)
    hid = (COEFS, HID, BLK)
    peers = TP - 1
    zs = NZ - 1
    return pl.pallas_call(
        step_kernel,
        out_shape=[sds(x.shape, BF16), sds(x.shape, BF16), sds((ROWS, CH), BF16)],
        in_specs=[hbm] * 8, out_specs=[hbm] * 3,
        scratch_shapes=[
            v(act, BF16), v(act, BF16), v((TP, DEGS, SLICE), F32), v((DEGS, CH, HID), BF16), v((CH, HID), BF16), v((DEGS, TP, CH, CH), BF16),
            v(act, BF16), v(act, BF16), v((TP, ROWS, CH), F32), v((DEGS, CH, CH), F32), v((DEGS, CH, BLK), F32),
            v((DEGS, HID, CH), BF16), v((HID, CH), BF16), v((DEGS, CH, HID), BF16),
            v((GRID_ROWS, BLK), BF16), v((GRID_ROWS, CH), BF16), v((ZROWS, BLK), BF16), v((YROWS, BLK), BF16), v((2 * ZROWS, CH), BF16), v((2 * YROWS, CH), BF16),
            v((COEFS, CH, BLK), BF16), v(hid, BF16), v(hid, BF16), v(hid, BF16), v((BLOCKS,) + hid, BF16), v((BLOCKS, HID, BLK), BF16), v((COEFS, CH, BLK), F32), v((BLOCKS, NZ, BLK), F32),
            v((GRID_PAD, BLK), BF16), v((GRID_PAD, BLK), BF16), v((GRID_PAD, BLK), BF16), v((GRID_PAD, BLK), BF16),
            v((TP, ROWS // 2, CH), F32), v((TP, ROWS // 2, CH), F32), v((TP, peers, EIGHTH, CH), F32), v((TP, EIGHTH, CH), F32),
            v((TP, zs, TILE, CH), F32), v((TP, TILE, CH), F32), v((TP, peers, TILE, CH), F32), v((TILE, CH), BF16),
            v((NZ * TILE, CH), BF16), v((DEGS, SLICE), F32), v((COEFS, PTS), F32), v((COEFS - 1, PTS), F32), dma((3,)),
            dma((BLOCKS, peers, 2)), dma((BLOCKS, peers, 2)), dma((peers, 3)), dma((peers, 3)), dma((peers, 3)), dma((peers, 3)), dma((3,)), dma((3,)),
            dma((peers,)), dma((peers,)), dma((5,)),
            dma((BLOCKS, 2, DEGS, peers)), dma((BLOCKS, 2, DEGS, peers)), dma((BLOCKS, 2)),
            dma((TP,)), dma((TP,)), dma((TP, peers)), dma((TP, peers)), dma((TP, zs)), dma((TP, zs)), dma((TP, peers)), dma((TP, peers)),
            dma((zs,)), dma((zs,)), dma((zs,)), dma((zs,))],
        compiler_params=pltpu.CompilerParams(collective_id=0, has_side_effects=True, vmem_limit_bytes=VMEM_LIMIT), name="step",
    )(x, g, gain, up, gate, down, tog, frg)


def store_kernel(out_in, dx_in, w_in, out, dx, d_up, d_gate, d_down, out_v, dx_v, w_v, in_sem, out_sem):
    thirds = [pl.ds(i * DEGS, DEGS) for i in range(DEGS)]
    moves = [((w_in, w_v), [(w_v.at[part(i, CH), :], d_up.at[i]) for i in range(DEGS)] + [(w_v.at[part(DEGS, CH), :], d_gate)]
              + [(w_v.at[part(TP + i, CH), :], d_down.at[i]) for i in range(DEGS)])]
    for src, buf, dst in ((out_in, out_v, out), (dx_in, dx_v, dx)):
        moves = moves + [((src.at[k], buf.at[k]), [(buf.at[k], dst.at[k])]) for k in thirds]
    loads = [pltpu.make_async_copy(*load, in_sem.at[i]) for i, (load, _) in enumerate(moves)]
    start(loads)
    stores = []
    for load, (_, pairs) in zip(loads, moves):
        load.wait()
        for pair in pairs:
            stores.append(pltpu.make_async_copy(*pair, out_sem.at[len(stores)]))
            stores[-1].start()
    for store in stores:
        store.wait()


def store_call(out, dx, w):
    hbm = pl.BlockSpec(memory_space=pl.ANY)
    sds = jax.ShapeDtypeStruct
    mats = sds((DEGS, CH, CH), BF16)
    v = pltpu.VMEM
    return pl.pallas_call(
        store_kernel, out_shape=[sds(out.shape, BF16), sds(dx.shape, BF16), mats, sds((CH, CH), BF16), mats], in_specs=[hbm] * 3, out_specs=[hbm] * 5,
        scratch_shapes=[v(out.shape, BF16), v(dx.shape, BF16), v(w.shape, BF16), pltpu.SemaphoreType.DMA((7,)), pltpu.SemaphoreType.DMA((13,))],
        compiler_params=pltpu.CompilerParams(vmem_limit_bytes=VMEM_LIMIT), name="store",
    )(out, dx, w)


def solution(mesh):
    act = P('dp', None, 'tp')
    in_specs = (act, P(None, 'tp'), P(None, None, 'tp'), P(None, 'tp'), P(None, 'tp', None), P(None, None), P(None, None), act)
    out_specs = (act, act, P(None, None, 'tp'), P(None, 'tp'), P(None, 'tp', None))

    def local_step(x, gain, up, gate, down, tog, frg, g):
        out, dx, d_up, d_gate, d_down = store_call(*step_call(x.transpose(1, 2, 0), g.transpose(1, 2, 0), gain, up, gate, down, tog, frg.T))
        return out.transpose(2, 0, 1), dx.transpose(2, 0, 1), d_up, d_gate, d_down

    return jax.shard_map(local_step, mesh=mesh, in_specs=in_specs, out_specs=out_specs, check_vma=False)
```

```python
import jax
import jax.numpy as jnp
from jax import lax
from jax.experimental import pallas as pl
from jax.experimental.pallas import tpu as pltpu
from jax.sharding import PartitionSpec as P

NORM_EPS = 1e-5
COEFS = 9
CH = 128
HID = 512
SUB = 16
BLK = 256
GRID_ROWS = 576
GRID_PAD = 640
SLAB = 56
ROWS = 896
TILE = 16
EIGHTH = 112
NZ = 8
DEGS = 3
TP = 4
SLICE = 32
PTS = 36
VEC_SCALE = 1.0 / 1024
VMEM_LIMIT = 60 * 2**20
F32 = jnp.float32
BF16 = jnp.bfloat16


def iota(shape, axis):
    return lax.broadcasted_iota(jnp.int32, shape, axis)


def mm(a, b):
    return jnp.dot(a, b, preferred_element_type=F32)


def mm_nt(a, b):
    return lax.dot_general(a, b, (((1,), (1,)), ((), ())), preferred_element_type=F32)


def one_hot(shape, row_div, col_div):
    return jnp.where(iota(shape, 0) // row_div == iota(shape, 1) // col_div, 1.0, 0.0).astype(BF16)


def point_of(row):
    main = row < HID
    point = jnp.where(main, (row % BLK) // NZ, SLICE + (row % SLICE) // NZ)
    half = jnp.where(main, row // BLK, (row % 64) // SLICE)
    return point, half


def spread_out(table_t, cols):
    point, half = point_of(iota((GRID_ROWS, CH), 0))
    left = mm(jnp.where(point == iota((GRID_ROWS, CH), 1), 1.0, 0.0).astype(BF16), table_t).astype(BF16)
    full = mm(left, one_hot((CH, cols), 1, SUB))
    row = iota((GRID_ROWS, cols), 0)
    same = point_of(row)[1] * NZ + row % NZ == iota((GRID_ROWS, cols), 1) % SUB
    return jnp.where(same, 0.5 * full, 0.0).astype(BF16)


def spread_back(table, rows):
    left = mm(one_hot((rows, CH), NZ, 1), table).astype(BF16)
    full = mm(left, one_hot((CH, BLK), 1, NZ))
    return jnp.where(iota((rows, BLK), 0) % NZ == iota((rows, BLK), 1) % NZ, full, 0.0).astype(BF16)


def spread_last(table, rows):
    row, col = iota((2 * rows, CH), 0), iota((2 * rows, CH), 1)
    r2, c2 = iota((2 * rows, CH), 0), iota((2 * rows, CH), 1)
    left = mm(jnp.where((r2 % rows) // NZ == c2, 1.0, 0.0).astype(BF16), table).astype(BF16)
    pick = jnp.where(iota((CH, CH), 0) == SLICE + (iota((CH, CH), 1) % SLICE) // NZ, 1.0, 0.0).astype(BF16)
    full = mm(left, pick)
    same = (row % NZ == col % NZ) & (row // rows == col // SLICE)
    return jnp.where(same, full, 0.0).astype(BF16)


def degree_of(coef):
    return jnp.where(coef >= 4, 2, jnp.where(coef >= 1, 1, 0))


MESH = pl.DeviceIdType.MESH


def places():
    dp = lax.axis_index("dp")
    return lax.axis_index("tp"), dp // NZ, (dp // 2) % TP, dp % 2


def dp_index(z, y, core):
    return (z * TP + y) * 2 + core


def remote(src, dst, send_sem, recv_sem, peer):
    return pltpu.make_async_remote_copy(src_ref=src, dst_ref=dst, send_sem=send_sem, recv_sem=recv_sem,
                                        device_id=peer, device_id_type=MESH)


def part(i, size):
    return pl.ds(pl.multiple_of(i * size, size), size)


def start(copies):
    for c in copies:
        c.start()


def arrive(copies):
    for c in copies:
        c.wait_recv()


CHUNK = 288
KROWS = 144
UNROLL = 4
ZROWS = 64
YROWS = 72
GROUPS = HID // SUB
BLOCKS = 2


def step_kernel(x_loc, g_loc, gain_loc, up_loc, gate_loc, down_loc, tog_ref, frg_ref,
                out_loc, dx_loc, r7,
                x_all, g_all, gain_x, up_all, gate_all, down_all, out_all, dx_all, wg, pad_s, gain_b,
                wup_t, wgate_t, wdown_t, kg, kf, kft, kgt, kftl, kgtl, n_s, y_s, dm_s, m_s, dy_s, da_s, dn_s, stat_s, sb0, sb1, db0, db1,
                r1, a1, r2, a2, r3, a3, r4, fin, r5, gain_v, tog_v, frg_v, small_sem,
                act_send, act_recv, wx_send, wx_recv, wy_send, wy_recv, wc_send, wc_recv, gain_send, gain_recv, loc_sem,
                o_send, o_recv, oloc_sem, s1, q1, s2, q2, s3, q3, s4, q4, s5, q5, s6, q6):
    me, z, y, core = places()
    atoms = x_all.shape[2]
    small = [pltpu.make_async_copy(src, dst, small_sem.at[i]) for i, (src, dst) in enumerate(((gain_loc, gain_v), (tog_ref, tog_v), (frg_ref, frg_v)))]
    start(small)
    pair = {"dp": dp_index(z, y, 1 - core)}
    x_dist = list(range(1, TP))
    x_peers = [{"tp": lax.rem(me + d, TP)} for d in x_dist]
    y_peers = [{"dp": dp_index(z, lax.rem(y + d, TP), core)} for d in x_dist]
    z_peers = [{"dp": dp_index(lax.rem(z + d, NZ), y, core)} for d in range(1, NZ)]
    group = [(dy, dc) for dc in range(2) for dy in range(TP) if dy + dc > 0]
    yc_peers = [{"dp": dp_index(z, lax.rem(y + dy, TP), lax.rem(core + dc, 2))} for dy, dc in group]
    barrier = pltpu.get_barrier_semaphore()
    meeting = x_peers + z_peers + yc_peers
    for peer in meeting:
        pl.semaphore_signal(barrier, inc=1, device_id=peer, device_id_type=MESH)
    pl.semaphore_wait(barrier, len(meeting))

    eighth = part(core * TP + y, TILE)
    mine = part(me, CH)
    pieces = [(up_loc.at[:, eighth, :], up_all.at[:, eighth, mine]),
              (gate_loc.at[eighth, :], gate_all.at[eighth, mine]),
              (down_loc.at[:, eighth, :], down_all.at[:, me, eighth, :])]
    wx = [remote(src, dst, wx_send.at[d, i], wx_recv.at[d, i], peer)
          for d, peer in enumerate(x_peers) for i, (src, dst) in enumerate(pieces)]
    gx = [remote(gain_loc, gain_x.at[me], gain_send.at[d], gain_recv.at[d], peer) for d, peer in enumerate(x_peers)]
    start(wx + gx)
    def acts(b):
        copies = []
        for d, peer in enumerate(x_peers):
            cols = part(lax.rem(me + d + 1, TP) * BLOCKS + b, BLK)
            for i, (src, dst) in enumerate(((x_loc, x_all), (g_loc, g_all))):
                copies.append(remote(src.at[:, :, cols], dst.at[:, part(me, SLICE), part(b, BLK)], act_send.at[b, d, i], act_recv.at[b, d, i], peer))
        return copies

    start(acts(0)[0::2])
    local = [pltpu.make_async_copy(src, dst, loc_sem.at[i]) for i, (src, dst) in enumerate(
        pieces + [(x_loc.at[:, :, part(me, atoms)], x_all.at[:, part(me, SLICE), :]), (g_loc.at[:, :, part(me, atoms)], g_all.at[:, part(me, SLICE), :])])]
    start(local)

    pad_s[...] = jnp.zeros(pad_s.shape, F32)
    for c in small:
        c.wait()
    pad_s[0, 0:COEFS, 0:PTS] = tog_v[...]
    pad_s[1, 0:COEFS - 1, 0:PTS] = frg_v[...]
    tog, tog_t = pad_s[0].astype(BF16), pad_s[0].T.astype(BF16)
    frg_t, frg = pad_s[1].astype(BF16), pad_s[1].T.astype(BF16)
    kg[...] = spread_out(tog_t, BLK)
    kf[...] = spread_out(frg, CH)
    kft[...] = spread_back(frg_t, ZROWS)
    kgt[...] = spread_back(tog, YROWS)
    kftl[...] = spread_last(frg_t, ZROWS)
    kgtl[...] = spread_last(tog, YROWS)
    for buf in (sb0, sb1, db0, db1):
        buf[GRID_ROWS:GRID_PAD, :] = jnp.zeros((GRID_PAD - GRID_ROWS, BLK), BF16)
    wg[...] = jnp.zeros(wg.shape, F32)
    gain_x[me] = gain_v[...]
    for c in local:
        c.wait()
    arrive(wx)
    wholes = [lambda rows: up_all.at[:, rows, :], lambda rows: gate_all.at[rows, :], lambda rows: down_all.at[:, :, rows, :]]
    wy = [remote(whole(eighth), whole(eighth), wy_send.at[d, i], wy_recv.at[d, i], peer)
          for d, peer in enumerate(y_peers) for i, whole in enumerate(wholes)]
    start(wy)
    start(acts(0)[1::2])
    arrive(gx)
    for t in range(TP):
        pad_s[2, t * NZ:t * NZ + DEGS, 0:SLICE] = gain_x[t]
    cols = pad_s[2].T
    for t in range(TP):
        for degree in range(DEGS):
            col = t * NZ + degree
            gain_b[degree, t * SLICE:(t + 1) * SLICE, :] = jnp.broadcast_to(cols[0:SLICE, col:col + 1], (SLICE, BLK))
    arrive(wy)
    side = part(core, CH // 2)
    wc = [remote(whole(side), whole(side), wc_send.at[i], wc_recv.at[i], pair) for i, whole in enumerate(wholes)]
    start(wc)
    arrive(wc)
    for degree in range(DEGS):
        wup_t[degree] = up_all[degree].T
        wdown_t[degree] = down_all[degree].reshape(HID, CH).T
    wgate_t[...] = gate_all[...].T

    def gain_of(coef):
        return gain_b[0 if coef == 0 else (1 if coef < TP else 2)]

    def norm(b, lanes):
        x0 = x_all[0, :, lanes].astype(F32)
        mean_s = jnp.sum(x0, axis=0, keepdims=True) * (1.0 / CH)
        cen = x0 - mean_s
        inv_s = lax.rsqrt(jnp.sum(cen * cen, axis=0, keepdims=True) * (1.0 / CH) + NORM_EPS)
        n_s[0] = ((cen * inv_s) * gain_of(0)).astype(BF16)
        acc = jnp.zeros((CH, BLK), F32)
        for coef in range(1, COEFS):
            xk = x_all[coef, :, lanes].astype(F32)
            acc = acc + xk * xk
        inv_v = lax.rsqrt(jnp.sum(acc, axis=0, keepdims=True) * VEC_SCALE + NORM_EPS)
        for coef in range(1, COEFS):
            xk = x_all[coef, :, lanes].astype(F32)
            n_s[coef] = ((xk * inv_v) * gain_of(coef)).astype(BF16)
        for i, stat in enumerate((mean_s, inv_s, inv_v)):
            stat_s[b, i:i + 1, :] = stat

    def up():
        def up_step(i, carry):
            for k in range(DEGS):
                coef = i * DEGS + k
                y_s[coef] = mm(wup_t[degree_of(coef)], n_s[coef]).astype(BF16)
            return carry
        lax.fori_loop(0, DEGS, up_step, 0)

    def hidden_grads(b, lanes):
        def grad_step(i, carry):
            for k in range(DEGS):
                coef = i * DEGS + k
                dm_s[coef] = mm(down_all[degree_of(coef)].reshape(HID, CH), g_all[coef, :, lanes]).astype(BF16)
            return carry
        lax.fori_loop(0, DEGS, grad_step, 0)

        def gate_step(i, carry):
            rows = part(i, CH)
            half = (0.5 * mm(wgate_t[rows, :], n_s[0])).astype(BF16).astype(F32)
            th = jnp.tanh(half)
            plus = 1.0 + th
            val = half * plus
            m_s[0, rows, :] = val.astype(BF16)
            slope = 0.5 * (plus + val * (1.0 - th))
            da_s[b, rows, :] = (dm_s[0, rows, :].astype(F32) * slope).astype(BF16)
            return carry
        for i in range(TP):
            gate_step(i, 0)

    def expand(j, s_buf, du_buf):
        rows = part(j, SUB)
        yj = y_s[:, rows, :].reshape(KROWS, BLK)
        dzj = dm_s[1:, rows, :].reshape(CH, BLK)
        for r0 in range(0, GRID_ROWS, CHUNK):
            half = mm(kg[r0:r0 + CHUNK, 0:KROWS], yj).astype(BF16).astype(F32)
            dval = mm(kf[r0:r0 + CHUNK, :], dzj).astype(BF16).astype(F32)
            th = jnp.tanh(half)
            plus = 1.0 + th
            val = half * plus
            s_buf[r0:r0 + CHUNK, :] = val.astype(BF16)
            du_buf[r0:r0 + CHUNK, :] = (dval * (plus + val * (1.0 - th))).astype(BF16)

    def halves(back, last, buf, rows):
        low = mm(last[...], buf[HID:GRID_PAD, :])
        sums = [mm(back[...], buf[h * BLK:(h + 1) * BLK, :]) + low[h * rows:(h + 1) * rows, :] for h in range(2)]
        return jnp.concatenate([v.reshape(rows // NZ, NZ, BLK) for v in sums], axis=1).astype(BF16)

    def contract(b, j, s_buf, du_buf):
        rows = part(j, SUB)
        m_s[1:, rows, :] = halves(kft, kftl, s_buf, ZROWS)
        dy_s[b, :, rows, :] = halves(kgt, kgtl, du_buf, YROWS)

    bufs = ((sb0, db0), (sb1, db1))

    def grid_step(i, b):
        for k in range(UNROLL):
            j = UNROLL * i + k
            expand(jnp.minimum(j + 1, GROUPS - 1), *bufs[(k + 1) % 2])
            contract(b, j, *bufs[k % 2])
        return b

    def weight_grads(b, t, lanes):
        rows = part(t, CH)

        for degree in range(DEGS):
            coefs = range(degree * degree, (degree + 1) * (degree + 1))
            wg[t, degree * CH:(degree + 1) * CH, :] += sum(mm_nt(n_s[c], dy_s[b, c, rows, :]) for c in coefs)
            wg[t, (degree + TP) * CH:(degree + TP + 1) * CH, :] += sum(mm_nt(m_s[c, rows, :], g_all[c, :, lanes]) for c in coefs)
        wg[t, DEGS * CH:TP * CH, :] += mm_nt(n_s[0], da_s[b, rows, :])

    def down(lanes):
        def down_step(i, carry):
            for k in range(DEGS):
                coef = i * DEGS + k
                xk = x_all[coef, :, lanes].astype(F32)
                out_all[coef, :, lanes] = (xk + mm(wdown_t[degree_of(coef)], m_s[coef])).astype(BF16)
            return carry
        lax.fori_loop(0, DEGS, down_step, 0)

    def norm_grads(b):
        def norm_grad_step(i, carry):
            for k in range(DEGS):
                coef = i * DEGS + k
                dn_s[coef] = mm(up_all[degree_of(coef)], dy_s[b, coef])
            return carry
        lax.fori_loop(0, DEGS, norm_grad_step, 0)
        dn_s[0] += mm(gate_all[...], da_s[b])

    def norm_back(i, carry):
        b = 1 - i
        norm_grads(b)
        lanes = part(b, BLK)
        mean_s, inv_s, inv_v = [stat_s[b, k:k + 1, :] for k in range(DEGS)]
        hat = (x_all[0, :, lanes].astype(F32) - mean_s) * inv_s
        dh = dn_s[0].astype(BF16).astype(F32) * gain_of(0)
        m1 = jnp.sum(dh, axis=0, keepdims=True) * (1.0 / CH)
        m2 = jnp.sum(dh * hat, axis=0, keepdims=True) * (1.0 / CH)
        dx_all[0, :, lanes] = (inv_s * (dh - m1 - hat * m2) + g_all[0, :, lanes].astype(F32)).astype(BF16)
        acc = jnp.zeros((CH, BLK), F32)
        for coef in range(1, COEFS):
            xk = x_all[coef, :, lanes].astype(F32)
            acc = acc + (dn_s[coef].astype(BF16).astype(F32) * gain_of(coef)) * (xk * inv_v)
        mv = jnp.sum(acc, axis=0, keepdims=True) * VEC_SCALE
        for coef in range(1, COEFS):
            xk = x_all[coef, :, lanes].astype(F32)
            dh = dn_s[coef].astype(BF16).astype(F32) * gain_of(coef)
            dx_all[coef, :, lanes] = (inv_v * (dh - (xk * inv_v) * mv) + g_all[coef, :, lanes].astype(F32)).astype(BF16)
        return carry

    outs = ((out_all, out_loc), (dx_all, dx_loc))

    def out_copies(b, i, third):
        src, dst = outs[i]
        coefs = slice(third * DEGS, (third + 1) * DEGS)
        cols = part(me * BLOCKS + b, BLK)
        return [remote(src.at[coefs, part(lax.rem(me + d, TP), SLICE), part(b, BLK)], dst.at[coefs, :, cols],
                       o_send.at[b, i, third, d - 1], o_recv.at[b, i, third, d - 1], x_peers[d - 1]) for d in x_dist]

    def out_local(b, i):
        src, dst = outs[i]
        return pltpu.make_async_copy(src.at[:, part(me, SLICE), part(b, BLK)], dst.at[:, :, part(me * BLOCKS + b, BLK)], oloc_sem.at[b, i])

    sent = [[[out_copies(b, i, third) for third in range(DEGS)] for i in range(2)] for b in range(BLOCKS)]
    kept = [[out_local(b, i) for i in range(2)] for b in range(BLOCKS)]

    def send_out(b, i):
        for third in range(DEGS):
            start(sent[b][i][third])
        kept[b][i].start()

    half_rows = ROWS // 2

    def c1(t):
        return remote(wg.at[t, part(1 - core, half_rows), :], r1.at[t], s1.at[t], q1.at[t], pair)

    def c2(t):
        return [remote(a1.at[t, part(lax.rem(y + d, TP), EIGHTH), :], r2.at[t, d - 1], s2.at[t, d - 1], q2.at[t, d - 1], y_peers[d - 1]) for d in x_dist]

    def c3(t):
        return [remote(a2.at[t, part(lax.rem(lax.rem(z + d, NZ), NZ - 1), TILE), :], r3.at[t, d - 1], s3.at[t, d - 1], q3.at[t, d - 1], z_peers[d - 1])
                for d in range(1, NZ)]

    def c4(t):
        return [remote(a3.at[t], r4.at[t, d - 1], s4.at[t, d - 1], q4.at[t, d - 1], x_peers[d - 1]) for d in x_dist]

    c5 = [remote(fin, r5.at[part(z, TILE), :], s5.at[d - 1], q5.at[d - 1], z_peers[d - 1]) for d in range(1, NZ)]

    def sum_core(t):
        c1(t).wait_recv()
        a1[t] = wg[t, part(core, half_rows), :] + r1[t]
        start(c2(t))

    def sum_y(t):
        arrive(c2(t))
        a2[t] = (a1[t, part(y, EIGHTH), :] + r2[t, 0]) + (r2[t, 1] + r2[t, 2])
        start(c3(t))

    def sum_z(t):
        arrive(c3(t))
        own = a2[t, part(lax.rem(z, NZ - 1), TILE), :]
        a3[t] = ((own + r3[t, 0]) + (r3[t, 1] + r3[t, 2])) + ((r3[t, 3] + r3[t, 4]) + (r3[t, 5] + r3[t, 6]))
        start(c4(t))

    def sum_x(t):
        arrive(c4(t))

        @pl.when(me == t)
        def _():
            fin[...] = ((a3[t] + r4[t, 0]) + (r4[t, 1] + r4[t, 2])).astype(BF16)
            start(c5)
            r5[part(z, TILE), :] = fin[...]

    for c in acts(0):
        c.wait_send()
    start(acts(1))
    per = GROUPS // UNROLL // TP

    def block_step(b, carry):
        lanes = part(b, BLK)
        arrive(acts(b)[0::2])
        norm(b, lanes)
        up()
        arrive(acts(b)[1::2])
        hidden_grads(b, lanes)
        expand(0, sb0, db0)

        def quarter_step(t, inner):
            lax.fori_loop(t * per, (t + 1) * per, grid_step, b)

            @pl.when((b == 1) & (t > 0))
            def _():
                sum_core(t - 1)

            @pl.when((b == 1) & (t == TP - 1))
            def _():
                sum_y(0)
            weight_grads(b, t, lanes)

            @pl.when(b == 1)
            def _():
                c1(t).start()
            return inner
        lax.fori_loop(0, TP, quarter_step, 0)

        @pl.when(b == 0)
        def _():
            down(lanes)
            send_out(0, 0)
        return carry
    lax.fori_loop(0, BLOCKS, block_step, 0)
    down(pl.ds(BLK, BLK))
    sum_core(TP - 1)
    send_out(1, 0)
    sum_y(1)
    norm_back(0, 0)
    sum_y(2)
    sum_z(0)
    sum_y(3)
    send_out(1, 1)
    norm_back(1, 0)
    sum_z(1)
    sum_z(2)
    sum_z(3)
    send_out(0, 1)
    for t in range(TP):
        sum_x(t)
    arrive(c5)
    slot = part(core * TP + y, EIGHTH)
    c6 = [remote(r5.at[0:EIGHTH, :], r7.at[slot, :], s6.at[i], q6.at[i], yc_peers[i]) for i in range(len(group))]
    start(c6)
    own = pltpu.make_async_copy(r5.at[0:EIGHTH, :], r7.at[slot, :], small_sem.at[0])
    own.start()
    arrive(c6)
    own.wait()
    finished = wx + gx + wy + wc + c5 + c6 + acts(1)
    for t in range(TP):
        finished = finished + [c1(t)] + c2(t) + c3(t) + c4(t)
    for b in range(BLOCKS):
        for i in range(2):
            kept[b][i].wait()
            for third in range(DEGS):
                arrive(sent[b][i][third])
                finished = finished + sent[b][i][third]
    for c in finished:
        c.wait_send()


def step_call(x, g, gain, up, gate, down, tog, frg):
    hbm = pl.BlockSpec(memory_space=pl.ANY)
    dma = pltpu.SemaphoreType.DMA
    v = pltpu.VMEM
    sds = jax.ShapeDtypeStruct
    atoms = x.shape[2] // TP
    act = (COEFS, CH, atoms)
    hid = (COEFS, HID, BLK)
    peers = TP - 1
    zs = NZ - 1
    return pl.pallas_call(
        step_kernel,
        out_shape=[sds(x.shape, BF16), sds(x.shape, BF16), sds((ROWS, CH), BF16)],
        in_specs=[hbm] * 8, out_specs=[hbm] * 3,
        scratch_shapes=[
            v(act, BF16), v(act, BF16), v((TP, DEGS, SLICE), F32), v((DEGS, CH, HID), BF16), v((CH, HID), BF16), v((DEGS, TP, CH, CH), BF16),
            v(act, BF16), v(act, BF16), v((TP, ROWS, CH), F32), v((DEGS, CH, CH), F32), v((DEGS, CH, BLK), F32),
            v((DEGS, HID, CH), BF16), v((HID, CH), BF16), v((DEGS, CH, HID), BF16),
            v((GRID_ROWS, BLK), BF16), v((GRID_ROWS, CH), BF16), v((ZROWS, BLK), BF16), v((YROWS, BLK), BF16), v((2 * ZROWS, CH), BF16), v((2 * YROWS, CH), BF16),
            v((COEFS, CH, BLK), BF16), v(hid, BF16), v(hid, BF16), v(hid, BF16), v((BLOCKS,) + hid, BF16), v((BLOCKS, HID, BLK), BF16), v((COEFS, CH, BLK), F32), v((BLOCKS, NZ, BLK), F32),
            v((GRID_PAD, BLK), BF16), v((GRID_PAD, BLK), BF16), v((GRID_PAD, BLK), BF16), v((GRID_PAD, BLK), BF16),
            v((TP, ROWS // 2, CH), F32), v((TP, ROWS // 2, CH), F32), v((TP, peers, EIGHTH, CH), F32), v((TP, EIGHTH, CH), F32),
            v((TP, zs, TILE, CH), F32), v((TP, TILE, CH), F32), v((TP, peers, TILE, CH), F32), v((TILE, CH), BF16),
            v((NZ * TILE, CH), BF16), v((DEGS, SLICE), F32), v((COEFS, PTS), F32), v((COEFS - 1, PTS), F32), dma((3,)),
            dma((BLOCKS, peers, 2)), dma((BLOCKS, peers, 2)), dma((peers, 3)), dma((peers, 3)), dma((peers, 3)), dma((peers, 3)), dma((3,)), dma((3,)),
            dma((peers,)), dma((peers,)), dma((5,)),
            dma((BLOCKS, 2, DEGS, peers)), dma((BLOCKS, 2, DEGS, peers)), dma((BLOCKS, 2)),
            dma((TP,)), dma((TP,)), dma((TP, peers)), dma((TP, peers)), dma((TP, zs)), dma((TP, zs)), dma((TP, peers)), dma((TP, peers)),
            dma((zs,)), dma((zs,)), dma((zs,)), dma((zs,))],
        compiler_params=pltpu.CompilerParams(collective_id=0, has_side_effects=True, vmem_limit_bytes=VMEM_LIMIT), name="step",
    )(x, g, gain, up, gate, down, tog, frg)


def store_kernel(out_in, dx_in, w_in, out, dx, d_up, d_gate, d_down, out_v, dx_v, w_v, in_sem, out_sem):
    thirds = [pl.ds(i * DEGS, DEGS) for i in range(DEGS)]
    moves = [((w_in, w_v), [(w_v.at[part(i, CH), :], d_up.at[i]) for i in range(DEGS)] + [(w_v.at[part(DEGS, CH), :], d_gate)]
              + [(w_v.at[part(TP + i, CH), :], d_down.at[i]) for i in range(DEGS)])]
    for src, buf, dst in ((out_in, out_v, out), (dx_in, dx_v, dx)):
        moves = moves + [((src.at[k], buf.at[k]), [(buf.at[k], dst.at[k])]) for k in thirds]
    loads = [pltpu.make_async_copy(*load, in_sem.at[i]) for i, (load, _) in enumerate(moves)]
    start(loads)
    stores = []
    for load, (_, pairs) in zip(loads, moves):
        load.wait()
        for pair in pairs:
            stores.append(pltpu.make_async_copy(*pair, out_sem.at[len(stores)]))
            stores[-1].start()
    for store in stores:
        store.wait()


def store_call(out, dx, w):
    hbm = pl.BlockSpec(memory_space=pl.ANY)
    sds = jax.ShapeDtypeStruct
    mats = sds((DEGS, CH, CH), BF16)
    v = pltpu.VMEM
    return pl.pallas_call(
        store_kernel, out_shape=[sds(out.shape, BF16), sds(dx.shape, BF16), mats, sds((CH, CH), BF16), mats], in_specs=[hbm] * 3, out_specs=[hbm] * 5,
        scratch_shapes=[v(out.shape, BF16), v(dx.shape, BF16), v(w.shape, BF16), pltpu.SemaphoreType.DMA((7,)), pltpu.SemaphoreType.DMA((13,))],
        compiler_params=pltpu.CompilerParams(vmem_limit_bytes=VMEM_LIMIT), name="store",
    )(out, dx, w)


def solution(mesh):
    act = P('dp', None, 'tp')
    in_specs = (act, P(None, 'tp'), P(None, None, 'tp'), P(None, 'tp'), P(None, 'tp', None), P(None, None), P(None, None), act)
    out_specs = (act, act, P(None, None, 'tp'), P(None, 'tp'), P(None, 'tp', None))

    def local_step(x, gain, up, gate, down, tog, frg, g):
        out, dx, d_up, d_gate, d_down = store_call(*step_call(x.transpose(1, 2, 0), g.transpose(1, 2, 0), gain, up, gate, down, tog, frg.T))
        return out.transpose(2, 0, 1), dx.transpose(2, 0, 1), d_up, d_gate, d_down

    return jax.shard_map(local_step, mesh=mesh, in_specs=in_specs, out_specs=out_specs, check_vma=False)
```

```python
import jax
import jax.numpy as jnp
from jax import lax
from jax.experimental import pallas as pl
from jax.experimental.pallas import tpu as pltpu
from jax.sharding import PartitionSpec as P

NORM_EPS = 1e-5
COEFS = 9
CH = 128
HID = 512
SUB = 16
BLK = 256
GRID_ROWS = 576
GRID_PAD = 640
SLAB = 56
ROWS = 896
TILE = 16
EIGHTH = 112
NZ = 8
DEGS = 3
TP = 4
SLICE = 32
PTS = 36
VEC_SCALE = 1.0 / 1024
VMEM_LIMIT = 60 * 2**20
F32 = jnp.float32
BF16 = jnp.bfloat16


def iota(shape, axis):
    return lax.broadcasted_iota(jnp.int32, shape, axis)


def mm(a, b):
    return jnp.dot(a, b, preferred_element_type=F32)


def mm_nt(a, b):
    return lax.dot_general(a, b, (((1,), (1,)), ((), ())), preferred_element_type=F32)


def one_hot(shape, row_div, col_div):
    return jnp.where(iota(shape, 0) // row_div == iota(shape, 1) // col_div, 1.0, 0.0).astype(BF16)


def point_of(row):
    main = row < HID
    point = jnp.where(main, (row % BLK) // NZ, SLICE + (row % SLICE) // NZ)
    half = jnp.where(main, row // BLK, (row % 64) // SLICE)
    return point, half


def spread_out(table_t, cols):
    point, half = point_of(iota((GRID_ROWS, CH), 0))
    left = mm(jnp.where(point == iota((GRID_ROWS, CH), 1), 1.0, 0.0).astype(BF16), table_t).astype(BF16)
    full = mm(left, one_hot((CH, cols), 1, SUB))
    row = iota((GRID_ROWS, cols), 0)
    same = point_of(row)[1] * NZ + row % NZ == iota((GRID_ROWS, cols), 1) % SUB
    return jnp.where(same, 0.5 * full, 0.0).astype(BF16)


def spread_back(table, rows):
    left = mm(one_hot((rows, CH), NZ, 1), table).astype(BF16)
    full = mm(left, one_hot((CH, BLK), 1, NZ))
    return jnp.where(iota((rows, BLK), 0) % NZ == iota((rows, BLK), 1) % NZ, full, 0.0).astype(BF16)


def spread_last(table, rows):
    row, col = iota((2 * rows, CH), 0), iota((2 * rows, CH), 1)
    r2, c2 = iota((2 * rows, CH), 0), iota((2 * rows, CH), 1)
    left = mm(jnp.where((r2 % rows) // NZ == c2, 1.0, 0.0).astype(BF16), table).astype(BF16)
    pick = jnp.where(iota((CH, CH), 0) == SLICE + (iota((CH, CH), 1) % SLICE) // NZ, 1.0, 0.0).astype(BF16)
    full = mm(left, pick)
    same = (row % NZ == col % NZ) & (row // rows == col // SLICE)
    return jnp.where(same, full, 0.0).astype(BF16)


def degree_of(coef):
    if isinstance(coef, int):
        return int(coef >= 1) + int(coef >= TP)
    return jnp.where(coef >= 4, 2, jnp.where(coef >= 1, 1, 0))


MESH = pl.DeviceIdType.MESH


def places():
    dp = lax.axis_index("dp")
    return lax.axis_index("tp"), dp // NZ, (dp // 2) % TP, dp % 2


def dp_index(z, y, core):
    return (z * TP + y) * 2 + core


def remote(src, dst, send_sem, recv_sem, peer):
    return pltpu.make_async_remote_copy(src_ref=src, dst_ref=dst, send_sem=send_sem, recv_sem=recv_sem,
                                        device_id=peer, device_id_type=MESH)


def part(i, size):
    return pl.ds(pl.multiple_of(i * size, size), size)


def start(copies):
    for c in copies:
        c.start()


def arrive(copies):
    for c in copies:
        c.wait_recv()


CHUNK = 288
KROWS = 144
UNROLL = 8
ZROWS = 64
YROWS = 72
GROUPS = HID // SUB
BLOCKS = 2


def step_kernel(x_loc, g_loc, gain_loc, up_loc, gate_loc, down_loc, tog_ref, frg_ref,
                out_loc, dx_loc, r7,
                x_all, g_all, gain_x, up_all, gate_all, down_all, out_all, dx_all, wg, pad_s, gain_b,
                wup_t, wgate_t, wdown_t, kg, kf, kft, kgt, kftl, kgtl, n_s, y_s, dm_s, m_s, dy_s, da_s, dn_s, stat_s, sb0, sb1, db0, db1,
                r1, a1, r2, a2, r3, a3, r4, fin, r5, gain_v, tog_v, frg_v, small_sem,
                act_send, act_recv, wx_send, wx_recv, wy_send, wy_recv, wc_send, wc_recv, gain_send, gain_recv, loc_sem,
                o_send, o_recv, oloc_sem, s1, q1, s2, q2, s3, q3, s4, q4, s5, q5, s6, q6):
    me, z, y, core = places()
    atoms = x_all.shape[2]
    small = [pltpu.make_async_copy(src, dst, small_sem.at[i]) for i, (src, dst) in enumerate(((gain_loc, gain_v), (tog_ref, tog_v), (frg_ref, frg_v)))]
    start(small)
    pair = {"dp": dp_index(z, y, 1 - core)}
    x_dist = list(range(1, TP))
    x_peers = [{"tp": lax.rem(me + d, TP)} for d in x_dist]
    y_peers = [{"dp": dp_index(z, lax.rem(y + d, TP), core)} for d in x_dist]
    z_peers = [{"dp": dp_index(lax.rem(z + d, NZ), y, core)} for d in range(1, NZ)]
    group = [(dy, dc) for dc in range(2) for dy in range(TP) if dy + dc > 0]
    yc_peers = [{"dp": dp_index(z, lax.rem(y + dy, TP), lax.rem(core + dc, 2))} for dy, dc in group]
    barrier = pltpu.get_barrier_semaphore()
    meeting = x_peers + z_peers + yc_peers
    for peer in meeting:
        pl.semaphore_signal(barrier, inc=1, device_id=peer, device_id_type=MESH)
    pl.semaphore_wait(barrier, len(meeting))

    eighth = part(core * TP + y, TILE)
    mine = part(me, CH)
    pieces = [(up_loc.at[:, eighth, :], up_all.at[:, eighth, mine]),
              (gate_loc.at[eighth, :], gate_all.at[eighth, mine]),
              (down_loc.at[:, eighth, :], down_all.at[:, me, eighth, :])]
    wx = [remote(src, dst, wx_send.at[d, i], wx_recv.at[d, i], peer)
          for d, peer in enumerate(x_peers) for i, (src, dst) in enumerate(pieces)]
    gx = [remote(gain_loc, gain_x.at[me], gain_send.at[d], gain_recv.at[d], peer) for d, peer in enumerate(x_peers)]
    start(wx + gx)
    def acts(b):
        copies = []
        for d, peer in enumerate(x_peers):
            cols = part(lax.rem(me + d + 1, TP) * BLOCKS + b, BLK)
            for i, (src, dst) in enumerate(((x_loc, x_all), (g_loc, g_all))):
                copies.append(remote(src.at[:, :, cols], dst.at[:, part(me, SLICE), part(b, BLK)], act_send.at[b, d, i], act_recv.at[b, d, i], peer))
        return copies

    start(acts(0)[0::2])
    local = [pltpu.make_async_copy(src, dst, loc_sem.at[i]) for i, (src, dst) in enumerate(
        pieces + [(x_loc.at[:, :, part(me, atoms)], x_all.at[:, part(me, SLICE), :]), (g_loc.at[:, :, part(me, atoms)], g_all.at[:, part(me, SLICE), :])])]
    start(local)

    pad_s[...] = jnp.zeros(pad_s.shape, F32)
    for c in small:
        c.wait()
    pad_s[0, 0:COEFS, 0:PTS] = tog_v[...]
    pad_s[1, 0:COEFS - 1, 0:PTS] = frg_v[...]
    tog, tog_t = pad_s[0].astype(BF16), pad_s[0].T.astype(BF16)
    frg_t, frg = pad_s[1].astype(BF16), pad_s[1].T.astype(BF16)
    kg[...] = spread_out(tog_t, BLK)
    kf[...] = spread_out(frg, CH)
    kft[...] = spread_back(frg_t, ZROWS)
    kgt[...] = spread_back(tog, YROWS)
    kftl[...] = spread_last(frg_t, ZROWS)
    kgtl[...] = spread_last(tog, YROWS)
    for buf in (sb0, sb1, db0, db1):
        buf[GRID_ROWS:GRID_PAD, :] = jnp.zeros((GRID_PAD - GRID_ROWS, BLK), BF16)
    wg[...] = jnp.zeros(wg.shape, F32)
    gain_x[me] = gain_v[...]
    for c in local:
        c.wait()
    arrive(wx)
    wholes = [lambda rows: up_all.at[:, rows, :], lambda rows: gate_all.at[rows, :], lambda rows: down_all.at[:, :, rows, :]]
    wy = [remote(whole(eighth), whole(eighth), wy_send.at[d, i], wy_recv.at[d, i], peer)
          for d, peer in enumerate(y_peers) for i, whole in enumerate(wholes)]
    start(wy)
    start(acts(0)[1::2])
    arrive(gx)
    for t in range(TP):
        pad_s[2, t * NZ:t * NZ + DEGS, 0:SLICE] = gain_x[t]
    cols = pad_s[2].T
    for t in range(TP):
        for degree in range(DEGS):
            col = t * NZ + degree
            gain_b[degree, t * SLICE:(t + 1) * SLICE, :] = jnp.broadcast_to(cols[0:SLICE, col:col + 1], (SLICE, BLK))
    arrive(wy)
    side = part(core, CH // 2)
    wc = [remote(whole(side), whole(side), wc_send.at[i], wc_recv.at[i], pair) for i, whole in enumerate(wholes)]
    start(wc)
    arrive(wc)
    for degree in range(DEGS):
        wup_t[degree] = up_all[degree].T
        wdown_t[degree] = down_all[degree].reshape(HID, CH).T
    wgate_t[...] = gate_all[...].T

    def gain_of(coef):
        return gain_b[0 if coef == 0 else (1 if coef < TP else 2)]

    def norm(b, lanes):
        x0 = x_all[0, :, lanes].astype(F32)
        mean_s = jnp.sum(x0, axis=0, keepdims=True) * (1.0 / CH)
        cen = x0 - mean_s
        inv_s = lax.rsqrt(jnp.sum(cen * cen, axis=0, keepdims=True) * (1.0 / CH) + NORM_EPS)
        n_s[0] = ((cen * inv_s) * gain_of(0)).astype(BF16)
        acc = jnp.zeros((CH, BLK), F32)
        for coef in range(1, COEFS):
            xk = x_all[coef, :, lanes].astype(F32)
            acc = acc + xk * xk
        inv_v = lax.rsqrt(jnp.sum(acc, axis=0, keepdims=True) * VEC_SCALE + NORM_EPS)
        for coef in range(1, COEFS):
            xk = x_all[coef, :, lanes].astype(F32)
            n_s[coef] = ((xk * inv_v) * gain_of(coef)).astype(BF16)
        for i, stat in enumerate((mean_s, inv_s, inv_v)):
            stat_s[b, i:i + 1, :] = stat

    def up():
        def up_step(i, carry):
            for k in range(DEGS):
                coef = i * DEGS + k
                y_s[coef] = mm(wup_t[degree_of(coef)], n_s[coef]).astype(BF16)
            return carry
        for i in range(DEGS):
            up_step(i, 0)

    def hidden_grads(b, lanes):
        def grad_step(i, carry):
            for k in range(DEGS):
                coef = i * DEGS + k
                dm_s[coef] = mm(down_all[degree_of(coef)].reshape(HID, CH), g_all[coef, :, lanes]).astype(BF16)
            return carry
        for i in range(DEGS):
            grad_step(i, 0)

        def gate_step(i, carry):
            rows = part(i, CH)
            half = (0.5 * mm(wgate_t[rows, :], n_s[0])).astype(BF16).astype(F32)
            th = jnp.tanh(half)
            plus = 1.0 + th
            val = half * plus
            m_s[0, rows, :] = val.astype(BF16)
            slope = 0.5 * (plus + val * (1.0 - th))
            da_s[b, rows, :] = (dm_s[0, rows, :].astype(F32) * slope).astype(BF16)
            return carry
        for i in range(TP):
            gate_step(i, 0)

    def expand(j, s_buf, du_buf):
        rows = part(j, SUB)
        yj = y_s[:, rows, :].reshape(KROWS, BLK)
        dzj = dm_s[1:, rows, :].reshape(CH, BLK)
        for r0 in range(0, GRID_ROWS, CHUNK):
            half = mm(kg[r0:r0 + CHUNK, 0:KROWS], yj).astype(BF16).astype(F32)
            dval = mm(kf[r0:r0 + CHUNK, :], dzj).astype(BF16).astype(F32)
            th = jnp.tanh(half)
            plus = 1.0 + th
            val = half * plus
            s_buf[r0:r0 + CHUNK, :] = val.astype(BF16)
            du_buf[r0:r0 + CHUNK, :] = (dval * (plus + val * (1.0 - th))).astype(BF16)

    def halves(back, last, buf, rows):
        low = mm(last[...], buf[HID:GRID_PAD, :])
        sums = [mm(back[...], buf[h * BLK:(h + 1) * BLK, :]) + low[h * rows:(h + 1) * rows, :] for h in range(2)]
        return jnp.concatenate([v.reshape(rows // NZ, NZ, BLK) for v in sums], axis=1).astype(BF16)

    def contract(b, j, s_buf, du_buf):
        rows = part(j, SUB)
        m_s[1:, rows, :] = halves(kft, kftl, s_buf, ZROWS)
        dy_s[b, :, rows, :] = halves(kgt, kgtl, du_buf, YROWS)

    bufs = ((sb0, db0), (sb1, db1))

    def grid_step(i, b):
        for k in range(UNROLL):
            j = UNROLL * i + k
            expand(jnp.minimum(j + 1, GROUPS - 1), *bufs[(k + 1) % 2])
            contract(b, j, *bufs[k % 2])
        return b

    def weight_grads(b, t, lanes):
        rows = part(t, CH)

        for degree in range(DEGS):
            coefs = range(degree * degree, (degree + 1) * (degree + 1))
            wg[t, degree * CH:(degree + 1) * CH, :] += sum(mm_nt(n_s[c], dy_s[b, c, rows, :]) for c in coefs)
            wg[t, (degree + TP) * CH:(degree + TP + 1) * CH, :] += sum(mm_nt(m_s[c, rows, :], g_all[c, :, lanes]) for c in coefs)
        wg[t, DEGS * CH:TP * CH, :] += mm_nt(n_s[0], da_s[b, rows, :])

    def down(lanes):
        def down_step(i, carry):
            for k in range(DEGS):
                coef = i * DEGS + k
                xk = x_all[coef, :, lanes].astype(F32)
                out_all[coef, :, lanes] = (xk + mm(wdown_t[degree_of(coef)], m_s[coef])).astype(BF16)
            return carry
        for i in range(DEGS):
            down_step(i, 0)

    def norm_grads(b):
        def norm_grad_step(i, carry):
            for k in range(DEGS):
                coef = i * DEGS + k
                dn_s[coef] = mm(up_all[degree_of(coef)], dy_s[b, coef])
            return carry
        for i in range(DEGS):
            norm_grad_step(i, 0)
        dn_s[0] += mm(gate_all[...], da_s[b])

    def norm_back(i, carry):
        b = 1 - i
        norm_grads(b)
        lanes = part(b, BLK)
        mean_s, inv_s, inv_v = [stat_s[b, k:k + 1, :] for k in range(DEGS)]
        hat = (x_all[0, :, lanes].astype(F32) - mean_s) * inv_s
        dh = dn_s[0].astype(BF16).astype(F32) * gain_of(0)
        m1 = jnp.sum(dh, axis=0, keepdims=True) * (1.0 / CH)
        m2 = jnp.sum(dh * hat, axis=0, keepdims=True) * (1.0 / CH)
        dx_all[0, :, lanes] = (inv_s * (dh - m1 - hat * m2) + g_all[0, :, lanes].astype(F32)).astype(BF16)
        acc = jnp.zeros((CH, BLK), F32)
        for coef in range(1, COEFS):
            xk = x_all[coef, :, lanes].astype(F32)
            acc = acc + (dn_s[coef].astype(BF16).astype(F32) * gain_of(coef)) * (xk * inv_v)
        mv = jnp.sum(acc, axis=0, keepdims=True) * VEC_SCALE
        for coef in range(1, COEFS):
            xk = x_all[coef, :, lanes].astype(F32)
            dh = dn_s[coef].astype(BF16).astype(F32) * gain_of(coef)
            dx_all[coef, :, lanes] = (inv_v * (dh - (xk * inv_v) * mv) + g_all[coef, :, lanes].astype(F32)).astype(BF16)
        return carry

    outs = ((out_all, out_loc), (dx_all, dx_loc))

    def out_copies(b, i, third):
        src, dst = outs[i]
        coefs = slice(third * DEGS, (third + 1) * DEGS)
        cols = part(me * BLOCKS + b, BLK)
        return [remote(src.at[coefs, part(lax.rem(me + d, TP), SLICE), part(b, BLK)], dst.at[coefs, :, cols],
                       o_send.at[b, i, third, d - 1], o_recv.at[b, i, third, d - 1], x_peers[d - 1]) for d in x_dist]

    def out_local(b, i):
        src, dst = outs[i]
        return pltpu.make_async_copy(src.at[:, part(me, SLICE), part(b, BLK)], dst.at[:, :, part(me * BLOCKS + b, BLK)], oloc_sem.at[b, i])

    sent = [[[out_copies(b, i, third) for third in range(DEGS)] for i in range(2)] for b in range(BLOCKS)]
    kept = [[out_local(b, i) for i in range(2)] for b in range(BLOCKS)]

    def send_out(b, i):
        for third in range(DEGS):
            start(sent[b][i][third])
        kept[b][i].start()

    half_rows = ROWS // 2

    def c1(t):
        return remote(wg.at[t, part(1 - core, half_rows), :], r1.at[t], s1.at[t], q1.at[t], pair)

    def c2(t):
        return [remote(a1.at[t, part(lax.rem(y + d, TP), EIGHTH), :], r2.at[t, d - 1], s2.at[t, d - 1], q2.at[t, d - 1], y_peers[d - 1]) for d in x_dist]

    def c3(t):
        return [remote(a2.at[t, part(lax.rem(lax.rem(z + d, NZ), NZ - 1), TILE), :], r3.at[t, d - 1], s3.at[t, d - 1], q3.at[t, d - 1], z_peers[d - 1])
                for d in range(1, NZ)]

    def c4(t):
        return [remote(a3.at[t], r4.at[t, d - 1], s4.at[t, d - 1], q4.at[t, d - 1], x_peers[d - 1]) for d in x_dist]

    c5 = [remote(fin, r5.at[part(z, TILE), :], s5.at[d - 1], q5.at[d - 1], z_peers[d - 1]) for d in range(1, NZ)]

    def sum_core(t):
        c1(t).wait_recv()
        a1[t] = wg[t, part(core, half_rows), :] + r1[t]
        start(c2(t))

    def sum_y(t):
        arrive(c2(t))
        a2[t] = (a1[t, part(y, EIGHTH), :] + r2[t, 0]) + (r2[t, 1] + r2[t, 2])
        start(c3(t))

    def sum_z(t):
        arrive(c3(t))
        own = a2[t, part(lax.rem(z, NZ - 1), TILE), :]
        a3[t] = ((own + r3[t, 0]) + (r3[t, 1] + r3[t, 2])) + ((r3[t, 3] + r3[t, 4]) + (r3[t, 5] + r3[t, 6]))
        start(c4(t))

    def sum_x(t):
        arrive(c4(t))

        @pl.when(me == t)
        def _():
            fin[...] = ((a3[t] + r4[t, 0]) + (r4[t, 1] + r4[t, 2])).astype(BF16)
            start(c5)
            r5[part(z, TILE), :] = fin[...]

    for c in acts(0):
        c.wait_send()
    start(acts(1))
    per = GROUPS // UNROLL // TP

    def block_step(b, carry):
        lanes = part(b, BLK)
        arrive(acts(b)[0::2])
        norm(b, lanes)
        up()
        arrive(acts(b)[1::2])
        hidden_grads(b, lanes)
        expand(0, sb0, db0)

        def quarter_step(t, inner):
            lax.fori_loop(t * per, (t + 1) * per, grid_step, b)

            @pl.when((b == 1) & (t > 0))
            def _():
                sum_core(t - 1)

            @pl.when((b == 1) & (t == TP - 1))
            def _():
                sum_y(0)
            weight_grads(b, t, lanes)

            @pl.when(b == 1)
            def _():
                c1(t).start()
            return inner
        lax.fori_loop(0, TP, quarter_step, 0)

        @pl.when(b == 0)
        def _():
            down(lanes)
            send_out(0, 0)
        return carry
    lax.fori_loop(0, BLOCKS, block_step, 0)
    down(pl.ds(BLK, BLK))
    sum_core(TP - 1)
    send_out(1, 0)
    sum_y(1)
    norm_back(0, 0)
    sum_y(2)
    sum_z(0)
    sum_y(3)
    send_out(1, 1)
    norm_back(1, 0)
    sum_z(1)
    sum_z(2)
    sum_z(3)
    send_out(0, 1)
    for t in range(TP):
        sum_x(t)
    arrive(c5)
    slot = part(core * TP + y, EIGHTH)
    c6 = [remote(r5.at[0:EIGHTH, :], r7.at[slot, :], s6.at[i], q6.at[i], yc_peers[i]) for i in range(len(group))]
    start(c6)
    own = pltpu.make_async_copy(r5.at[0:EIGHTH, :], r7.at[slot, :], small_sem.at[0])
    own.start()
    arrive(c6)
    own.wait()
    finished = wx + gx + wy + wc + c5 + c6 + acts(1)
    for t in range(TP):
        finished = finished + [c1(t)] + c2(t) + c3(t) + c4(t)
    for b in range(BLOCKS):
        for i in range(2):
            kept[b][i].wait()
            for third in range(DEGS):
                arrive(sent[b][i][third])
                finished = finished + sent[b][i][third]
    for c in finished:
        c.wait_send()


def step_call(x, g, gain, up, gate, down, tog, frg):
    hbm = pl.BlockSpec(memory_space=pl.ANY)
    dma = pltpu.SemaphoreType.DMA
    v = pltpu.VMEM
    sds = jax.ShapeDtypeStruct
    atoms = x.shape[2] // TP
    act = (COEFS, CH, atoms)
    hid = (COEFS, HID, BLK)
    peers = TP - 1
    zs = NZ - 1
    return pl.pallas_call(
        step_kernel,
        out_shape=[sds(x.shape, BF16), sds(x.shape, BF16), sds((ROWS, CH), BF16)],
        in_specs=[hbm] * 8, out_specs=[hbm] * 3,
        scratch_shapes=[
            v(act, BF16), v(act, BF16), v((TP, DEGS, SLICE), F32), v((DEGS, CH, HID), BF16), v((CH, HID), BF16), v((DEGS, TP, CH, CH), BF16),
            v(act, BF16), v(act, BF16), v((TP, ROWS, CH), F32), v((DEGS, CH, CH), F32), v((DEGS, CH, BLK), F32),
            v((DEGS, HID, CH), BF16), v((HID, CH), BF16), v((DEGS, CH, HID), BF16),
            v((GRID_ROWS, BLK), BF16), v((GRID_ROWS, CH), BF16), v((ZROWS, BLK), BF16), v((YROWS, BLK), BF16), v((2 * ZROWS, CH), BF16), v((2 * YROWS, CH), BF16),
            v((COEFS, CH, BLK), BF16), v(hid, BF16), v(hid, BF16), v(hid, BF16), v((BLOCKS,) + hid, BF16), v((BLOCKS, HID, BLK), BF16), v((COEFS, CH, BLK), F32), v((BLOCKS, NZ, BLK), F32),
            v((GRID_PAD, BLK), BF16), v((GRID_PAD, BLK), BF16), v((GRID_PAD, BLK), BF16), v((GRID_PAD, BLK), BF16),
            v((TP, ROWS // 2, CH), F32), v((TP, ROWS // 2, CH), F32), v((TP, peers, EIGHTH, CH), F32), v((TP, EIGHTH, CH), F32),
            v((TP, zs, TILE, CH), F32), v((TP, TILE, CH), F32), v((TP, peers, TILE, CH), F32), v((TILE, CH), BF16),
            v((NZ * TILE, CH), BF16), v((DEGS, SLICE), F32), v((COEFS, PTS), F32), v((COEFS - 1, PTS), F32), dma((3,)),
            dma((BLOCKS, peers, 2)), dma((BLOCKS, peers, 2)), dma((peers, 3)), dma((peers, 3)), dma((peers, 3)), dma((peers, 3)), dma((3,)), dma((3,)),
            dma((peers,)), dma((peers,)), dma((5,)),
            dma((BLOCKS, 2, DEGS, peers)), dma((BLOCKS, 2, DEGS, peers)), dma((BLOCKS, 2)),
            dma((TP,)), dma((TP,)), dma((TP, peers)), dma((TP, peers)), dma((TP, zs)), dma((TP, zs)), dma((TP, peers)), dma((TP, peers)),
            dma((zs,)), dma((zs,)), dma((zs,)), dma((zs,))],
        compiler_params=pltpu.CompilerParams(collective_id=0, has_side_effects=True, vmem_limit_bytes=VMEM_LIMIT), name="step",
    )(x, g, gain, up, gate, down, tog, frg)


def store_kernel(out_in, dx_in, w_in, out, dx, d_up, d_gate, d_down, out_v, dx_v, w_v, in_sem, out_sem):
    thirds = [pl.ds(i * DEGS, DEGS) for i in range(DEGS)]
    moves = [((w_in, w_v), [(w_v.at[part(i, CH), :], d_up.at[i]) for i in range(DEGS)] + [(w_v.at[part(DEGS, CH), :], d_gate)]
              + [(w_v.at[part(TP + i, CH), :], d_down.at[i]) for i in range(DEGS)])]
    for src, buf, dst in ((out_in, out_v, out), (dx_in, dx_v, dx)):
        moves = moves + [((src.at[k], buf.at[k]), [(buf.at[k], dst.at[k])]) for k in thirds]
    loads = [pltpu.make_async_copy(*load, in_sem.at[i]) for i, (load, _) in enumerate(moves)]
    start(loads)
    stores = []
    for load, (_, pairs) in zip(loads, moves):
        load.wait()
        for pair in pairs:
            stores.append(pltpu.make_async_copy(*pair, out_sem.at[len(stores)]))
            stores[-1].start()
    for store in stores:
        store.wait()


def store_call(out, dx, w):
    hbm = pl.BlockSpec(memory_space=pl.ANY)
    sds = jax.ShapeDtypeStruct
    mats = sds((DEGS, CH, CH), BF16)
    v = pltpu.VMEM
    return pl.pallas_call(
        store_kernel, out_shape=[sds(out.shape, BF16), sds(dx.shape, BF16), mats, sds((CH, CH), BF16), mats], in_specs=[hbm] * 3, out_specs=[hbm] * 5,
        scratch_shapes=[v(out.shape, BF16), v(dx.shape, BF16), v(w.shape, BF16), pltpu.SemaphoreType.DMA((7,)), pltpu.SemaphoreType.DMA((13,))],
        compiler_params=pltpu.CompilerParams(vmem_limit_bytes=VMEM_LIMIT), name="store",
    )(out, dx, w)


def solution(mesh):
    act = P('dp', None, 'tp')
    in_specs = (act, P(None, 'tp'), P(None, None, 'tp'), P(None, 'tp'), P(None, 'tp', None), P(None, None), P(None, None), act)
    out_specs = (act, act, P(None, None, 'tp'), P(None, 'tp'), P(None, 'tp', None))

    def local_step(x, gain, up, gate, down, tog, frg, g):
        out, dx, d_up, d_gate, d_down = store_call(*step_call(x.transpose(1, 2, 0), g.transpose(1, 2, 0), gain, up, gate, down, tog, frg.T))
        return out.transpose(2, 0, 1), dx.transpose(2, 0, 1), d_up, d_gate, d_down

    return jax.shard_map(local_step, mesh=mesh, in_specs=in_specs, out_specs=out_specs, check_vma=False)
```

```python
import jax
import jax.numpy as jnp
from jax import lax
from jax.experimental import pallas as pl
from jax.experimental.pallas import tpu as pltpu
from jax.sharding import PartitionSpec as P

NORM_EPS = 1e-5
COEFS = 9
CH = 128
HID = 512
SUB = 16
BLK = 256
GRID_ROWS = 576
GRID_PAD = 640
SLAB = 56
ROWS = 896
TILE = 16
EIGHTH = 112
NZ = 8
DEGS = 3
TP = 4
SLICE = 32
PTS = 36
VEC_SCALE = 1.0 / 1024
VMEM_LIMIT = 60 * 2**20
F32 = jnp.float32
BF16 = jnp.bfloat16


def iota(shape, axis):
    return lax.broadcasted_iota(jnp.int32, shape, axis)


def mm(a, b):
    return jnp.dot(a, b, preferred_element_type=F32)


def mm_nt(a, b):
    return lax.dot_general(a, b, (((1,), (1,)), ((), ())), preferred_element_type=F32)


def one_hot(shape, row_div, col_div):
    return jnp.where(iota(shape, 0) // row_div == iota(shape, 1) // col_div, 1.0, 0.0).astype(BF16)


def point_of(row):
    main = row < HID
    point = jnp.where(main, (row % BLK) // NZ, SLICE + (row % SLICE) // NZ)
    half = jnp.where(main, row // BLK, (row % 64) // SLICE)
    return point, half


def spread_out(table_t, cols):
    point, half = point_of(iota((GRID_ROWS, CH), 0))
    left = mm(jnp.where(point == iota((GRID_ROWS, CH), 1), 1.0, 0.0).astype(BF16), table_t).astype(BF16)
    full = mm(left, one_hot((CH, cols), 1, SUB))
    row = iota((GRID_ROWS, cols), 0)
    same = point_of(row)[1] * NZ + row % NZ == iota((GRID_ROWS, cols), 1) % SUB
    return jnp.where(same, 0.5 * full, 0.0).astype(BF16)


def spread_back(table, rows):
    left = mm(one_hot((rows, CH), NZ, 1), table).astype(BF16)
    full = mm(left, one_hot((CH, BLK), 1, NZ))
    return jnp.where(iota((rows, BLK), 0) % NZ == iota((rows, BLK), 1) % NZ, full, 0.0).astype(BF16)


def spread_last(table, rows):
    row, col = iota((2 * rows, CH), 0), iota((2 * rows, CH), 1)
    r2, c2 = iota((2 * rows, CH), 0), iota((2 * rows, CH), 1)
    left = mm(jnp.where((r2 % rows) // NZ == c2, 1.0, 0.0).astype(BF16), table).astype(BF16)
    pick = jnp.where(iota((CH, CH), 0) == SLICE + (iota((CH, CH), 1) % SLICE) // NZ, 1.0, 0.0).astype(BF16)
    full = mm(left, pick)
    same = (row % NZ == col % NZ) & (row // rows == col // SLICE)
    return jnp.where(same, full, 0.0).astype(BF16)


def degree_of(coef):
    if isinstance(coef, int):
        return int(coef >= 1) + int(coef >= TP)
    return jnp.where(coef >= 4, 2, jnp.where(coef >= 1, 1, 0))


MESH = pl.DeviceIdType.MESH


def places():
    dp = lax.axis_index("dp")
    return lax.axis_index("tp"), dp // NZ, (dp // 2) % TP, dp % 2


def dp_index(z, y, core):
    return (z * TP + y) * 2 + core


def remote(src, dst, send_sem, recv_sem, peer):
    return pltpu.make_async_remote_copy(src_ref=src, dst_ref=dst, send_sem=send_sem, recv_sem=recv_sem,
                                        device_id=peer, device_id_type=MESH)


def part(i, size):
    return pl.ds(pl.multiple_of(i * size, size), size)


def start(copies):
    for c in copies:
        c.start()


def arrive(copies):
    for c in copies:
        c.wait_recv()


CHUNK = 288
KROWS = 144
UNROLL = 8
ZROWS = 64
YROWS = 72
GROUPS = HID // SUB
BLOCKS = 2


def step_kernel(x_loc, g_loc, gain_loc, up_loc, gate_loc, down_loc, tog_ref, frg_ref,
                out_loc, dx_loc, r7,
                x_all, g_all, gain_x, up_all, gate_all, down_all, out_all, dx_all, wg, pad_s, gain_b,
                wup_t, wgate_t, wdown_t, kg, kf, kft, kgt, kftl, kgtl, n_s, y_s, dm_s, m_s, dy_s, da_s, dn_s, stat_s, sb0, sb1, db0, db1,
                r1, a1, r2, a2, r3, a3, r4, fin, r5, gain_v, tog_v, frg_v, small_sem,
                act_send, act_recv, wx_send, wx_recv, wy_send, wy_recv, wc_send, wc_recv, gain_send, gain_recv, loc_sem,
                o_send, o_recv, oloc_sem, s1, q1, s2, q2, s3, q3, s4, q4, s5, q5, s6, q6):
    me, z, y, core = places()
    atoms = x_all.shape[2]
    small = [pltpu.make_async_copy(src, dst, small_sem.at[i]) for i, (src, dst) in enumerate(((gain_loc, gain_v), (tog_ref, tog_v), (frg_ref, frg_v)))]
    start(small)
    pair = {"dp": dp_index(z, y, 1 - core)}
    x_dist = list(range(1, TP))
    x_peers = [{"tp": lax.rem(me + d, TP)} for d in x_dist]
    y_peers = [{"dp": dp_index(z, lax.rem(y + d, TP), core)} for d in x_dist]
    z_peers = [{"dp": dp_index(lax.rem(z + d, NZ), y, core)} for d in range(1, NZ)]
    group = [(dy, dc) for dc in range(2) for dy in range(TP) if dy + dc > 0]
    yc_peers = [{"dp": dp_index(z, lax.rem(y + dy, TP), lax.rem(core + dc, 2))} for dy, dc in group]
    barrier = pltpu.get_barrier_semaphore()
    meeting = x_peers + z_peers + yc_peers
    for peer in meeting:
        pl.semaphore_signal(barrier, inc=1, device_id=peer, device_id_type=MESH)
    pl.semaphore_wait(barrier, len(meeting))

    eighth = part(core * TP + y, TILE)
    mine = part(me, CH)
    pieces = [(up_loc.at[:, eighth, :], up_all.at[:, eighth, mine]),
              (gate_loc.at[eighth, :], gate_all.at[eighth, mine]),
              (down_loc.at[:, eighth, :], down_all.at[:, me, eighth, :])]
    wx = [remote(src, dst, wx_send.at[d, i], wx_recv.at[d, i], peer)
          for d, peer in enumerate(x_peers) for i, (src, dst) in enumerate(pieces)]
    gx = [remote(gain_loc, gain_x.at[me], gain_send.at[d], gain_recv.at[d], peer) for d, peer in enumerate(x_peers)]
    start(wx + gx)
    def acts(b):
        copies = []
        for d, peer in enumerate(x_peers):
            cols = part(lax.rem(me + d + 1, TP) * BLOCKS + b, BLK)
            for i, (src, dst) in enumerate(((x_loc, x_all), (g_loc, g_all))):
                copies.append(remote(src.at[:, :, cols], dst.at[:, part(me, SLICE), part(b, BLK)], act_send.at[b, d, i], act_recv.at[b, d, i], peer))
        return copies

    start(acts(0)[0::2])
    local = [pltpu.make_async_copy(src, dst, loc_sem.at[i]) for i, (src, dst) in enumerate(
        pieces + [(x_loc.at[:, :, part(me, atoms)], x_all.at[:, part(me, SLICE), :]), (g_loc.at[:, :, part(me, atoms)], g_all.at[:, part(me, SLICE), :])])]
    start(local)

    pad_s[...] = jnp.zeros(pad_s.shape, F32)
    for c in small:
        c.wait()
    pad_s[0, 0:COEFS, 0:PTS] = tog_v[...]
    pad_s[1, 0:COEFS - 1, 0:PTS] = frg_v[...]
    tog, tog_t = pad_s[0].astype(BF16), pad_s[0].T.astype(BF16)
    frg_t, frg = pad_s[1].astype(BF16), pad_s[1].T.astype(BF16)
    kg[...] = spread_out(tog_t, BLK)
    kf[...] = spread_out(frg, CH)
    kft[...] = spread_back(frg_t, ZROWS)
    kgt[...] = spread_back(tog, YROWS)
    kftl[...] = spread_last(frg_t, ZROWS)
    kgtl[...] = spread_last(tog, YROWS)
    for buf in (sb0, sb1, db0, db1):
        buf[GRID_ROWS:GRID_PAD, :] = jnp.zeros((GRID_PAD - GRID_ROWS, BLK), BF16)
    wg[...] = jnp.zeros(wg.shape, F32)
    gain_x[me] = gain_v[...]
    for c in local:
        c.wait()
    arrive(wx)
    wholes = [lambda rows: up_all.at[:, rows, :], lambda rows: gate_all.at[rows, :], lambda rows: down_all.at[:, :, rows, :]]
    wy = [remote(whole(eighth), whole(eighth), wy_send.at[d, i], wy_recv.at[d, i], peer)
          for d, peer in enumerate(y_peers) for i, whole in enumerate(wholes)]
    start(wy)
    start(acts(0)[1::2])
    arrive(gx)
    for t in range(TP):
        pad_s[2, t * NZ:t * NZ + DEGS, 0:SLICE] = gain_x[t]
    cols = pad_s[2].T
    for t in range(TP):
        for degree in range(DEGS):
            col = t * NZ + degree
            gain_b[degree, t * SLICE:(t + 1) * SLICE, :] = jnp.broadcast_to(cols[0:SLICE, col:col + 1], (SLICE, BLK))
    arrive(wy)
    side = part(core, CH // 2)
    wc = [remote(whole(side), whole(side), wc_send.at[i], wc_recv.at[i], pair) for i, whole in enumerate(wholes)]
    start(wc)
    arrive(wc)
    for degree in range(DEGS):
        wup_t[degree] = up_all[degree].T
        wdown_t[degree] = down_all[degree].reshape(HID, CH).T
    wgate_t[...] = gate_all[...].T

    def gain_of(coef):
        return gain_b[0 if coef == 0 else (1 if coef < TP else 2)]

    def norm(b, lanes):
        x0 = x_all[0, :, lanes].astype(F32)
        mean_s = jnp.sum(x0, axis=0, keepdims=True) * (1.0 / CH)
        cen = x0 - mean_s
        inv_s = lax.rsqrt(jnp.sum(cen * cen, axis=0, keepdims=True) * (1.0 / CH) + NORM_EPS)
        n_s[0] = ((cen * inv_s) * gain_of(0)).astype(BF16)
        acc = jnp.zeros((CH, BLK), F32)
        for coef in range(1, COEFS):
            xk = x_all[coef, :, lanes].astype(F32)
            acc = acc + xk * xk
        inv_v = lax.rsqrt(jnp.sum(acc, axis=0, keepdims=True) * VEC_SCALE + NORM_EPS)
        for coef in range(1, COEFS):
            xk = x_all[coef, :, lanes].astype(F32)
            n_s[coef] = ((xk * inv_v) * gain_of(coef)).astype(BF16)
        for i, stat in enumerate((mean_s, inv_s, inv_v)):
            stat_s[b, i:i + 1, :] = stat

    def up():
        def up_step(i, carry):
            for k in range(DEGS):
                coef = i * DEGS + k
                y_s[coef] = mm(wup_t[degree_of(coef)], n_s[coef]).astype(BF16)
            return carry
        for i in range(DEGS):
            up_step(i, 0)

    def hidden_grads(b, lanes):
        def grad_step(i, carry):
            for k in range(DEGS):
                coef = i * DEGS + k
                dm_s[coef] = mm(down_all[degree_of(coef)].reshape(HID, CH), g_all[coef, :, lanes]).astype(BF16)
            return carry
        for i in range(DEGS):
            grad_step(i, 0)

        def gate_step(i, carry):
            rows = part(i, CH)
            half = (0.5 * mm(wgate_t[rows, :], n_s[0])).astype(BF16).astype(F32)
            th = jnp.tanh(half)
            plus = 1.0 + th
            val = half * plus
            m_s[0, rows, :] = val.astype(BF16)
            slope = 0.5 * (plus + val * (1.0 - th))
            da_s[b, rows, :] = (dm_s[0, rows, :].astype(F32) * slope).astype(BF16)
            return carry
        for i in range(TP):
            gate_step(i, 0)

    def expand(j, s_buf, du_buf):
        rows = part(j, SUB)
        yj = y_s[:, rows, :].reshape(KROWS, BLK)
        dzj = dm_s[1:, rows, :].reshape(CH, BLK)
        for r0 in range(0, GRID_ROWS, CHUNK):
            half = mm(kg[r0:r0 + CHUNK, 0:KROWS], yj).astype(BF16).astype(F32)
            dval = mm(kf[r0:r0 + CHUNK, :], dzj).astype(BF16).astype(F32)
            th = jnp.tanh(half)
            plus = 1.0 + th
            val = half * plus
            s_buf[r0:r0 + CHUNK, :] = val.astype(BF16)
            du_buf[r0:r0 + CHUNK, :] = (dval * (plus + val * (1.0 - th))).astype(BF16)

    def halves(back, last, buf, rows):
        low = mm(last[...], buf[HID:GRID_PAD, :])
        sums = [mm(back[...], buf[h * BLK:(h + 1) * BLK, :]) + low[h * rows:(h + 1) * rows, :] for h in range(2)]
        return jnp.concatenate([v.reshape(rows // NZ, NZ, BLK) for v in sums], axis=1).astype(BF16)

    def contract(b, j, s_buf, du_buf):
        rows = part(j, SUB)
        m_s[1:, rows, :] = halves(kft, kftl, s_buf, ZROWS)
        dy_s[b, :, rows, :] = halves(kgt, kgtl, du_buf, YROWS)

    bufs = ((sb0, db0), (sb1, db1))

    def grid_step(i, b):
        for k in range(UNROLL):
            j = UNROLL * i + k
            expand(jnp.minimum(j + 1, GROUPS - 1), *bufs[(k + 1) % 2])
            contract(b, j, *bufs[k % 2])
        return b

    def weight_grads(b, t, lanes):
        rows = part(t, CH)

        for degree in range(DEGS):
            coefs = range(degree * degree, (degree + 1) * (degree + 1))
            wg[t, degree * CH:(degree + 1) * CH, :] += sum(mm_nt(n_s[c], dy_s[b, c, rows, :]) for c in coefs)
            wg[t, (degree + TP) * CH:(degree + TP + 1) * CH, :] += sum(mm_nt(m_s[c, rows, :], g_all[c, :, lanes]) for c in coefs)
        wg[t, DEGS * CH:TP * CH, :] += mm_nt(n_s[0], da_s[b, rows, :])

    def down(lanes):
        def down_step(i, carry):
            for k in range(DEGS):
                coef = i * DEGS + k
                xk = x_all[coef, :, lanes].astype(F32)
                out_all[coef, :, lanes] = (xk + mm(wdown_t[degree_of(coef)], m_s[coef])).astype(BF16)
            return carry
        for i in range(DEGS):
            down_step(i, 0)

    def norm_grads(b):
        def norm_grad_step(i, carry):
            for k in range(DEGS):
                coef = i * DEGS + k
                dn_s[coef] = mm(up_all[degree_of(coef)], dy_s[b, coef])
            return carry
        for i in range(DEGS):
            norm_grad_step(i, 0)
        dn_s[0] += mm(gate_all[...], da_s[b])

    def norm_back(i, carry):
        b = 1 - i
        norm_grads(b)
        lanes = part(b, BLK)
        mean_s, inv_s, inv_v = [stat_s[b, k:k + 1, :] for k in range(DEGS)]
        hat = (x_all[0, :, lanes].astype(F32) - mean_s) * inv_s
        dh = dn_s[0].astype(BF16).astype(F32) * gain_of(0)
        m1 = jnp.sum(dh, axis=0, keepdims=True) * (1.0 / CH)
        m2 = jnp.sum(dh * hat, axis=0, keepdims=True) * (1.0 / CH)
        dx_all[0, :, lanes] = (inv_s * (dh - m1 - hat * m2) + g_all[0, :, lanes].astype(F32)).astype(BF16)
        acc = jnp.zeros((CH, BLK), F32)
        for coef in range(1, COEFS):
            xk = x_all[coef, :, lanes].astype(F32)
            acc = acc + (dn_s[coef].astype(BF16).astype(F32) * gain_of(coef)) * (xk * inv_v)
        mv = jnp.sum(acc, axis=0, keepdims=True) * VEC_SCALE
        for coef in range(1, COEFS):
            xk = x_all[coef, :, lanes].astype(F32)
            dh = dn_s[coef].astype(BF16).astype(F32) * gain_of(coef)
            dx_all[coef, :, lanes] = (inv_v * (dh - (xk * inv_v) * mv) + g_all[coef, :, lanes].astype(F32)).astype(BF16)
        return carry

    outs = ((out_all, out_loc), (dx_all, dx_loc))

    def out_copies(b, i, third):
        src, dst = outs[i]
        coefs = slice(third * DEGS, (third + 1) * DEGS)
        cols = part(me * BLOCKS + b, BLK)
        return [remote(src.at[coefs, part(lax.rem(me + d, TP), SLICE), part(b, BLK)], dst.at[coefs, :, cols],
                       o_send.at[b, i, third, d - 1], o_recv.at[b, i, third, d - 1], x_peers[d - 1]) for d in x_dist]

    def out_local(b, i):
        src, dst = outs[i]
        return pltpu.make_async_copy(src.at[:, part(me, SLICE), part(b, BLK)], dst.at[:, :, part(me * BLOCKS + b, BLK)], oloc_sem.at[b, i])

    sent = [[[out_copies(b, i, third) for third in range(DEGS)] for i in range(2)] for b in range(BLOCKS)]
    kept = [[out_local(b, i) for i in range(2)] for b in range(BLOCKS)]

    def send_out(b, i):
        for third in range(DEGS):
            start(sent[b][i][third])
        kept[b][i].start()

    half_rows = ROWS // 2

    def c1(t):
        return remote(wg.at[t, part(1 - core, half_rows), :], r1.at[t], s1.at[t], q1.at[t], pair)

    def c2(t):
        return [remote(a1.at[t, part(lax.rem(y + d, TP), EIGHTH), :], r2.at[t, d - 1], s2.at[t, d - 1], q2.at[t, d - 1], y_peers[d - 1]) for d in x_dist]

    def c3(t):
        return [remote(a2.at[t, part(lax.rem(lax.rem(z + d, NZ), NZ - 1), TILE), :], r3.at[t, d - 1], s3.at[t, d - 1], q3.at[t, d - 1], z_peers[d - 1])
                for d in range(1, NZ)]

    def c4(t):
        return [remote(a3.at[t], r4.at[t, d - 1], s4.at[t, d - 1], q4.at[t, d - 1], x_peers[d - 1]) for d in x_dist]

    c5 = [remote(fin, r5.at[part(z, TILE), :], s5.at[d - 1], q5.at[d - 1], z_peers[d - 1]) for d in range(1, NZ)]

    def sum_core(t):
        c1(t).wait_recv()
        a1[t] = wg[t, part(core, half_rows), :] + r1[t]
        start(c2(t))

    def sum_y(t):
        arrive(c2(t))
        a2[t] = (a1[t, part(y, EIGHTH), :] + r2[t, 0]) + (r2[t, 1] + r2[t, 2])
        start(c3(t))

    def sum_z(t):
        arrive(c3(t))
        own = a2[t, part(lax.rem(z, NZ - 1), TILE), :]
        a3[t] = ((own + r3[t, 0]) + (r3[t, 1] + r3[t, 2])) + ((r3[t, 3] + r3[t, 4]) + (r3[t, 5] + r3[t, 6]))
        start(c4(t))

    def sum_x(t):
        arrive(c4(t))

        @pl.when(me == t)
        def _():
            fin[...] = ((a3[t] + r4[t, 0]) + (r4[t, 1] + r4[t, 2])).astype(BF16)
            start(c5)
            r5[part(z, TILE), :] = fin[...]

    for c in acts(0):
        c.wait_send()
    start(acts(1))

    def block_step(b, carry):
        lanes = part(b, BLK)
        arrive(acts(b)[0::2])
        norm(b, lanes)
        up()
        arrive(acts(b)[1::2])
        hidden_grads(b, lanes)
        expand(0, sb0, db0)

        def quarter_step(t, inner):
            grid_step(t, b)
            weight_grads(b, t, lanes)

            @pl.when(b == 1)
            def _():
                c1(t).start()

            @pl.when((b == 1) & (t > 0))
            def _():
                sum_core(t - 1)

            @pl.when((b == 1) & (t == TP - 1))
            def _():
                sum_y(0)
            return inner
        lax.fori_loop(0, TP, quarter_step, 0)

        @pl.when(b == 0)
        def _():
            down(lanes)
            send_out(0, 0)
        return carry
    lax.fori_loop(0, BLOCKS, block_step, 0)
    down(pl.ds(BLK, BLK))
    sum_core(TP - 1)
    send_out(1, 0)
    sum_y(1)
    norm_back(0, 0)
    sum_y(2)
    sum_z(0)
    sum_y(3)
    send_out(1, 1)
    norm_back(1, 0)
    sum_z(1)
    sum_z(2)
    sum_z(3)
    send_out(0, 1)
    for t in range(TP):
        sum_x(t)
    arrive(c5)
    slot = part(core * TP + y, EIGHTH)
    c6 = [remote(r5.at[0:EIGHTH, :], r7.at[slot, :], s6.at[i], q6.at[i], yc_peers[i]) for i in range(len(group))]
    start(c6)
    own = pltpu.make_async_copy(r5.at[0:EIGHTH, :], r7.at[slot, :], small_sem.at[0])
    own.start()
    arrive(c6)
    own.wait()
    finished = wx + gx + wy + wc + c5 + c6 + acts(1)
    for t in range(TP):
        finished = finished + [c1(t)] + c2(t) + c3(t) + c4(t)
    for b in range(BLOCKS):
        for i in range(2):
            kept[b][i].wait()
            for third in range(DEGS):
                arrive(sent[b][i][third])
                finished = finished + sent[b][i][third]
    for c in finished:
        c.wait_send()


def step_call(x, g, gain, up, gate, down, tog, frg):
    hbm = pl.BlockSpec(memory_space=pl.ANY)
    dma = pltpu.SemaphoreType.DMA
    v = pltpu.VMEM
    sds = jax.ShapeDtypeStruct
    atoms = x.shape[2] // TP
    act = (COEFS, CH, atoms)
    hid = (COEFS, HID, BLK)
    peers = TP - 1
    zs = NZ - 1
    return pl.pallas_call(
        step_kernel,
        out_shape=[sds(x.shape, BF16), sds(x.shape, BF16), sds((ROWS, CH), BF16)],
        in_specs=[hbm] * 8, out_specs=[hbm] * 3,
        scratch_shapes=[
            v(act, BF16), v(act, BF16), v((TP, DEGS, SLICE), F32), v((DEGS, CH, HID), BF16), v((CH, HID), BF16), v((DEGS, TP, CH, CH), BF16),
            v(act, BF16), v(act, BF16), v((TP, ROWS, CH), F32), v((DEGS, CH, CH), F32), v((DEGS, CH, BLK), F32),
            v((DEGS, HID, CH), BF16), v((HID, CH), BF16), v((DEGS, CH, HID), BF16),
            v((GRID_ROWS, BLK), BF16), v((GRID_ROWS, CH), BF16), v((ZROWS, BLK), BF16), v((YROWS, BLK), BF16), v((2 * ZROWS, CH), BF16), v((2 * YROWS, CH), BF16),
            v((COEFS, CH, BLK), BF16), v(hid, BF16), v(hid, BF16), v(hid, BF16), v((BLOCKS,) + hid, BF16), v((BLOCKS, HID, BLK), BF16), v((COEFS, CH, BLK), F32), v((BLOCKS, NZ, BLK), F32),
            v((GRID_PAD, BLK), BF16), v((GRID_PAD, BLK), BF16), v((GRID_PAD, BLK), BF16), v((GRID_PAD, BLK), BF16),
            v((TP, ROWS // 2, CH), F32), v((TP, ROWS // 2, CH), F32), v((TP, peers, EIGHTH, CH), F32), v((TP, EIGHTH, CH), F32),
            v((TP, zs, TILE, CH), F32), v((TP, TILE, CH), F32), v((TP, peers, TILE, CH), F32), v((TILE, CH), BF16),
            v((NZ * TILE, CH), BF16), v((DEGS, SLICE), F32), v((COEFS, PTS), F32), v((COEFS - 1, PTS), F32), dma((3,)),
            dma((BLOCKS, peers, 2)), dma((BLOCKS, peers, 2)), dma((peers, 3)), dma((peers, 3)), dma((peers, 3)), dma((peers, 3)), dma((3,)), dma((3,)),
            dma((peers,)), dma((peers,)), dma((5,)),
            dma((BLOCKS, 2, DEGS, peers)), dma((BLOCKS, 2, DEGS, peers)), dma((BLOCKS, 2)),
            dma((TP,)), dma((TP,)), dma((TP, peers)), dma((TP, peers)), dma((TP, zs)), dma((TP, zs)), dma((TP, peers)), dma((TP, peers)),
            dma((zs,)), dma((zs,)), dma((zs,)), dma((zs,))],
        compiler_params=pltpu.CompilerParams(collective_id=0, has_side_effects=True, vmem_limit_bytes=VMEM_LIMIT), name="step",
    )(x, g, gain, up, gate, down, tog, frg)


def store_kernel(out_in, dx_in, w_in, out, dx, d_up, d_gate, d_down, out_v, dx_v, w_v, in_sem, out_sem):
    thirds = [pl.ds(i * DEGS, DEGS) for i in range(DEGS)]
    moves = [((w_in, w_v), [(w_v.at[part(i, CH), :], d_up.at[i]) for i in range(DEGS)] + [(w_v.at[part(DEGS, CH), :], d_gate)]
              + [(w_v.at[part(TP + i, CH), :], d_down.at[i]) for i in range(DEGS)])]
    for src, buf, dst in ((out_in, out_v, out), (dx_in, dx_v, dx)):
        moves = moves + [((src.at[k], buf.at[k]), [(buf.at[k], dst.at[k])]) for k in thirds]
    loads = [pltpu.make_async_copy(*load, in_sem.at[i]) for i, (load, _) in enumerate(moves)]
    start(loads)
    stores = []
    for load, (_, pairs) in zip(loads, moves):
        load.wait()
        for pair in pairs:
            stores.append(pltpu.make_async_copy(*pair, out_sem.at[len(stores)]))
            stores[-1].start()
    for store in stores:
        store.wait()


def store_call(out, dx, w):
    hbm = pl.BlockSpec(memory_space=pl.ANY)
    sds = jax.ShapeDtypeStruct
    mats = sds((DEGS, CH, CH), BF16)
    v = pltpu.VMEM
    return pl.pallas_call(
        store_kernel, out_shape=[sds(out.shape, BF16), sds(dx.shape, BF16), mats, sds((CH, CH), BF16), mats], in_specs=[hbm] * 3, out_specs=[hbm] * 5,
        scratch_shapes=[v(out.shape, BF16), v(dx.shape, BF16), v(w.shape, BF16), pltpu.SemaphoreType.DMA((7,)), pltpu.SemaphoreType.DMA((13,))],
        compiler_params=pltpu.CompilerParams(vmem_limit_bytes=VMEM_LIMIT), name="store",
    )(out, dx, w)


def solution(mesh):
    act = P('dp', None, 'tp')
    in_specs = (act, P(None, 'tp'), P(None, None, 'tp'), P(None, 'tp'), P(None, 'tp', None), P(None, None), P(None, None), act)
    out_specs = (act, act, P(None, None, 'tp'), P(None, 'tp'), P(None, 'tp', None))

    def local_step(x, gain, up, gate, down, tog, frg, g):
        out, dx, d_up, d_gate, d_down = store_call(*step_call(x.transpose(1, 2, 0), g.transpose(1, 2, 0), gain, up, gate, down, tog, frg.T))
        return out.transpose(2, 0, 1), dx.transpose(2, 0, 1), d_up, d_gate, d_down

    return jax.shard_map(local_step, mesh=mesh, in_specs=in_specs, out_specs=out_specs, check_vma=False)
```
